32 devices in a mesh: rep: 8 (over z, x), tp: 4 (over y, core).
Axes of the slice: x: 2, y: 2, z: 4, core: 2. Of those that a mesh axis runs over, the one named last changes fastest.
Arguments:
- tokens: bfloat16 [64, 4096], P(('rep', 'tp')), may hold values from -6 to 6
- conv_state: bfloat16 [3, 64, 8192], P(None, 'rep', 'tp'), may hold values from -6 to 6
- ssm_state: float32 [64, 16, 8192], P('rep', None, 'tp'), may hold values from -6 to 6
- norm_gains: bfloat16 [2, 4096], P(None, ('rep', 'tp')), may hold values from 0.5 to 1.5
- conv_weight: bfloat16 [4, 8192], P(None, ('rep', 'tp')), may hold values from -3 to 3
- conv_skip: bfloat16 [2, 8192], P(None, ('rep', 'tp')), may hold values from -3 to 3
- step_bias: bfloat16 [8192], P(('rep', 'tp')), may hold values from -5 to -1
- decay_log: bfloat16 [16, 8192], P(None, ('rep', 'tp')), may hold values from 0 to 2.796875
- input_proj: bfloat16 [4096, 2, 8192], P(('rep', 'tp')), may hold values from -0.09375 to 0.09375
- select_proj: bfloat16 [8192, 288], P('tp', 'rep'), may hold values from -0.0625 to 0.0625
- step_proj: bfloat16 [256, 8192], P(('rep', 'tp')), may hold values from -0.375 to 0.375
- output_proj: bfloat16 [8192, 4096], P(None, ('rep', 'tp')), may hold values from -0.0625 to 0.0625
- router: bfloat16 [4096, 16], P(('rep', 'tp')), may hold values from -0.09375 to 0.09375
- expert_proj: bfloat16 [4096, 2, 2, 12288], P(('rep', 'tp')), may hold values from -0.09375 to 0.09375
- expert_ids: int32 [64, 2], P(('rep', 'tp')), may hold values from 0 to 15, as said below
Outputs:
- mamba_out: bfloat16 [64, 4096], P(('rep', 'tp'))
- conv_next: bfloat16 [3, 64, 8192], P(None, 'rep', 'tp')
- ssm_next: float32 [64, 16, 8192], P('rep', None, 'tp')
- expert_hidden: bfloat16 [128, 12288], P('rep', 'tp')
The draws below stay inside these ranges and needn't reach their ends.
Inputs may be any that keep to these rules, and one draw needn't show every extreme that they name: `expert_ids`: each row names two different experts. Within each aligned block of 2 rows (the rows of one device) each expert e < 2 is named by at most 2 rows.
All inputs are finite; a program needn't handle non-finite values.
Results may differ from the reference program's by a relative error of at most 0.04.
Values may be sent and summed in bfloat16 or wider, within the bound.
A program may use at most 192 MiB of HBM per device.

```python
import jax
import jax.numpy as jnp
from jax import lax

D = 4096
INNER = 8192
STEP_RANK = 256
STATE = 16
TAPS = 4
FF = 12288
EXPERTS = 16
EXP_WIN = 2
CAPACITY = 2
TOK_DEV = 2
REQ = 8
TOKENS = 64
SLOTS = 128
N_REP = 8
N_TP = 4


def draw_expert_ids(key, part):
    blocks = TOKENS // TOK_DEV
    per_replica = REQ // TOK_DEV
    subkeys = jax.random.split(jax.random.fold_in(key, 17), 6)
    counts = jax.random.randint(subkeys[0], (blocks, EXP_WIN), 1, CAPACITY + 1)
    full_replica = jax.random.randint(subkeys[1], (), 0, blocks // per_replica)
    replica_of = jnp.arange(blocks, dtype=jnp.int32) // per_replica
    counts = jnp.where((replica_of == full_replica)[:, None], CAPACITY, counts)
    scores = jax.random.randint(subkeys[2], (blocks, TOK_DEV, EXP_WIN), 0, 1 << 20) * TOK_DEV + jnp.arange(TOK_DEV, dtype=jnp.int32)[None, :, None]
    ordering = jnp.argsort(scores, axis=1)
    order_rank = jnp.argsort(ordering, axis=1)
    member = order_rank < counts[:, None, :]
    in_first = member[:, :, 0]
    in_second = member[:, :, 1]
    spare = EXPERTS - EXP_WIN
    spare_one = EXP_WIN + jax.random.randint(subkeys[3], (blocks, TOK_DEV), 0, spare)
    spare_two = EXP_WIN + (spare_one - EXP_WIN + jax.random.randint(subkeys[4], (blocks, TOK_DEV), 1, spare)) % spare
    first_pick = jnp.where(in_first, 0, jnp.where(in_second, 1, spare_one))
    second_pick = jnp.where(in_first & in_second, 1, jnp.where(in_first | in_second, spare_one, spare_two))
    swapped = jax.random.randint(subkeys[5], (blocks, TOK_DEV), 0, 2) == 1
    column_one = jnp.where(swapped, second_pick, first_pick)
    column_two = jnp.where(swapped, first_pick, second_pick)
    return jnp.stack([column_one, column_two], axis=-1).reshape(TOKENS, 2).astype(jnp.int32)


def shard_levels(key, extent, cuts, least, top_value):
    def one(axis_at, blocks):
        draws = jax.random.uniform(jax.random.fold_in(jax.random.fold_in(key, 6), axis_at), (blocks,), jnp.float32, least / len(cuts), top_value / len(cuts))
        return jnp.repeat(jnp.exp(draws), extent[axis_at] // blocks).reshape((-1,) + (1,) * (len(extent) - axis_at - 1))

    level = one(*cuts[0])
    for cut in cuts[1:]:
        level = level * one(*cut)
    return level


def normal_values(own_key, dims, scale, bound, cuts=(), held_as=jnp.bfloat16):
    level = shard_levels(own_key, dims, cuts, -0.22, 0.18) if cuts else 1.0
    array = jax.random.normal(own_key, dims, jnp.float32) * scale * level
    return jnp.minimum(jnp.maximum(array, -bound), bound).astype(held_as)


def setup_inputs(seed: int = 0) -> dict:
    splits = jax.random.split(jax.random.key(seed), 16)
    return {
        "tokens": normal_values(splits[0], (TOKENS, D), 1.0, 6.0, ((0, 32),)),
        "conv_state": normal_values(splits[1], (TAPS - 1, TOKENS, INNER), 1.0, 6.0, ((1, 8), (2, 4))),
        "ssm_state": normal_values(splits[2], (TOKENS, STATE, INNER), 1.0, 6.0, ((0, 8), (2, 4)), jnp.float32),
        "norm_gains": jnp.clip(1.0 + 0.1 * jax.random.normal(splits[3], (2, D), jnp.float32), 0.5, 1.5).astype(jnp.bfloat16),
        "conv_weight": normal_values(splits[4], (TAPS, INNER), 0.5, 3.0, ((1, 32),)),
        "conv_skip": normal_values(splits[5], (2, INNER), 0.5, 3.0, ((1, 32),)),
        "step_bias": jnp.clip(-5.0 + 4.0 * jax.random.uniform(splits[6], (INNER,), jnp.float32) ** shard_levels(splits[6], (INNER,), ((0, 32),), -0.2, 0.2), -5.0, -1.0).astype(jnp.bfloat16),
        "decay_log": jnp.clip(2.796875 * jax.random.uniform(splits[7], (STATE, INNER), jnp.float32) ** shard_levels(splits[7], (STATE, INNER), ((1, 32),), -0.2, 0.2), 0.0, 2.796875).astype(jnp.bfloat16),
        "input_proj": normal_values(splits[8], (D, 2, INNER), D ** -0.5, 0.09375, ((0, 32),)),
        "select_proj": normal_values(splits[9], (INNER, STEP_RANK + 2 * STATE), INNER ** -0.5, 0.0625, ((0, 4), (1, 8))),
        "step_proj": normal_values(splits[10], (STEP_RANK, INNER), STEP_RANK ** -0.5, 0.375, ((0, 32),)),
        "output_proj": normal_values(splits[11], (INNER, D), INNER ** -0.5, 0.0625, ((1, 32),)),
        "router": normal_values(splits[12], (D, EXPERTS), D ** -0.5, 0.09375, ((0, 32),)),
        "expert_proj": normal_values(splits[13], (D, EXP_WIN, 2, FF), D ** -0.5, 0.09375, ((0, 32),)),
        "expert_ids": draw_expert_ids(jax.random.fold_in(splits[15], 71), 0),
    }


epsilon = 1e-05

def norm_scale(values, gain):
    mean_square = lax.optimization_barrier(jnp.mean(values * values, axis=-1, keepdims=True))
    return values * lax.rsqrt(mean_square + epsilon) * gain.astype(jnp.float32)

def ssm_block(block_args):
    state, step_size, activated, input_map, output_map, decay_rate = block_args
    factor = jnp.exp(step_size[:, None, :] * decay_rate[None])
    state_next = factor * state + (step_size * activated)[:, None, :] * input_map[:, :, None]
    readout = lax.optimization_barrier(jnp.sum(state_next * output_map[:, :, None], axis=1))
    return (state_next, readout)

def reference(tokens, conv_state, ssm_state, norm_gains, conv_weight, conv_skip, step_bias, decay_log, input_proj, select_proj, step_proj, output_proj, router, expert_proj, expert_ids):
    residual_in = tokens.astype(jnp.float32)
    normed = norm_scale(residual_in, norm_gains[0]).astype(jnp.bfloat16)
    projected = jnp.dot(normed, input_proj.reshape(D, 2 * INNER), preferred_element_type=jnp.float32)
    conv_input = projected[:, :INNER]
    gate_z = projected[:, INNER:]
    conv_taps = conv_weight.astype(jnp.float32)
    history = conv_state.astype(jnp.float32)
    conv_mix = lax.optimization_barrier(jnp.sum(conv_taps[:-1, None, :] * history, axis=0)) + conv_taps[-1] * conv_input + conv_skip[0].astype(jnp.float32)
    conv_next = jnp.concatenate([conv_state[1:], conv_input.astype(jnp.bfloat16)[None]], axis=0)
    activated = jax.nn.silu(conv_mix)
    selected = jnp.dot(activated.astype(jnp.bfloat16), select_proj, preferred_element_type=jnp.float32)
    step_low = selected[:, :STEP_RANK].astype(jnp.bfloat16)
    input_map = selected[:, STEP_RANK:STEP_RANK + STATE]
    output_map = selected[:, STEP_RANK + STATE:]
    step_size = jax.nn.softplus(jnp.dot(step_low, step_proj, preferred_element_type=jnp.float32) + step_bias.astype(jnp.float32))
    decay_rate = -jnp.exp(decay_log.astype(jnp.float32))
    replicas = TOKENS // REQ
    state_next, readout = lax.map(lambda block_args: ssm_block(block_args + (decay_rate,)), (ssm_state.reshape(replicas, REQ, STATE, INNER), step_size.reshape(replicas, REQ, INNER), activated.reshape(replicas, REQ, INNER), input_map.reshape(replicas, REQ, STATE), output_map.reshape(replicas, REQ, STATE)))
    ssm_next = state_next.reshape(TOKENS, STATE, INNER)
    readout = readout.reshape(TOKENS, INNER) + conv_skip[1].astype(jnp.float32) * activated
    gated_out = (readout * jax.nn.silu(gate_z)).astype(jnp.bfloat16)
    inner_block = INNER // N_TP
    mixer_out = jnp.zeros((TOKENS, D), jnp.float32)
    for block_index in range(N_TP):
        lower = block_index * inner_block
        partial_out = jnp.dot(gated_out[:, lower:lower + inner_block], output_proj[lower:lower + inner_block], preferred_element_type=jnp.float32)
        mixer_out = mixer_out + lax.optimization_barrier(partial_out.astype(jnp.bfloat16)).astype(jnp.float32)
    residual = residual_in + mixer_out
    mamba_out = residual.astype(jnp.bfloat16)
    moe_in = norm_scale(residual, norm_gains[1]).astype(jnp.bfloat16)
    logits = jnp.dot(moe_in, router, preferred_element_type=jnp.float32)
    choose = (expert_ids[:, :, None] == jnp.arange(EXPERTS, dtype=jnp.int32)[None, None, :]).astype(jnp.float32)
    picked = lax.optimization_barrier(jnp.sum(choose * logits[:, None, :], axis=2))
    first_gate = jax.nn.sigmoid(picked[:, 0] - picked[:, 1])
    second_gate = jax.nn.sigmoid(picked[:, 1] - picked[:, 0])
    window = jnp.arange(EXP_WIN, dtype=jnp.int32)
    names_first = expert_ids[:, 0:1] == window[None, :]
    names_second = expert_ids[:, 1:2] == window[None, :]
    zero = jnp.zeros((), jnp.float32)
    gate_w = jnp.where(names_first, first_gate[:, None], zero) + jnp.where(names_second, second_gate[:, None], zero)
    routed = (names_first | names_second).astype(jnp.int32)
    blocks = TOKENS // TOK_DEV
    routed_blocks = routed.reshape(blocks, TOK_DEV, EXP_WIN)
    position = jnp.cumsum(routed_blocks, axis=1) - routed_blocks
    slot_of = ((position[..., None] == jnp.arange(CAPACITY, dtype=jnp.int32)) & (routed_blocks[..., None] > 0)).astype(jnp.float32)
    slot_x = jnp.einsum('btec,btd->becd', slot_of, moe_in.reshape(blocks, TOK_DEV, D).astype(jnp.float32)).astype(jnp.bfloat16)
    slot_gate = jnp.einsum('btec,bte->bec', slot_of, gate_w.reshape(blocks, TOK_DEV, EXP_WIN)).astype(jnp.bfloat16)
    feature_block = D // N_REP
    hidden_list = []
    for expert in range(EXP_WIN):
        slot_rows = slot_x[:, expert].reshape(blocks * CAPACITY, D)
        gate_up = jnp.zeros((blocks * CAPACITY, 2 * FF), jnp.float32)
        for block_index in range(N_REP):
            lower = block_index * feature_block
            partial_up = jnp.dot(slot_rows[:, lower:lower + feature_block], expert_proj[lower:lower + feature_block, expert].reshape(feature_block, 2 * FF), preferred_element_type=jnp.float32)
            gate_up = gate_up + lax.optimization_barrier(partial_up.astype(jnp.bfloat16)).astype(jnp.float32)
        slot_scale = slot_gate[:, expert].reshape(blocks * CAPACITY).astype(jnp.float32)
        hidden = slot_scale[:, None] * jax.nn.silu(gate_up[:, :FF]) * gate_up[:, FF:]
        hidden_list.append(hidden.reshape(blocks, CAPACITY, FF))
    expert_hidden = jnp.stack(hidden_list, axis=1).reshape(SLOTS, FF).astype(jnp.bfloat16)
    return (mamba_out, conv_next, ssm_next, expert_hidden)
```

```python
import functools

import jax
import jax.numpy as jnp
from jax import lax
from jax.experimental import pallas as pl
from jax.experimental.pallas import tpu as pltpu
from jax.sharding import PartitionSpec as P

CAPACITY = 2
LANES = 128


epsilon = 1e-05
MESH = pl.DeviceIdType.MESH


def send_kernel(plan, *refs):
    arrays = len(plan)
    sources, targets, sems = refs[:arrays], refs[arrays : 2 * arrays], refs[2 * arrays :]
    barrier = pltpu.get_barrier_semaphore()
    greeted = 0
    for axis, count in dict((axis, count) for axis, count, _ in plan).items():
        me = lax.axis_index(axis)
        for step in range(1, count):
            pl.semaphore_signal(
                barrier, inc=1, device_id={axis: lax.rem(me + step, count)}, device_id_type=MESH
            )
        greeted += count - 1
    pl.semaphore_wait(barrier, greeted)
    copies = []
    for which, (axis, count, mode) in enumerate(plan):
        me = lax.axis_index(axis)
        for step in range(1, count):
            peer = lax.rem(me + step, count)
            source = sources[which]
            if mode == "lanes":
                lanes = source.shape[-1] // count
                source = source.at[:, pl.ds(pl.multiple_of(peer * lanes, lanes), lanes)]
            elif mode == "lead":
                source = source.at[peer]
            copy = pltpu.make_async_remote_copy(
                src_ref=source,
                dst_ref=targets[which].at[me],
                send_sem=sems[2 * which].at[step - 1],
                recv_sem=sems[2 * which + 1].at[step - 1],
                device_id={axis: peer},
                device_id_type=MESH,
            )
            copy.start()
            copies.append(copy)
    for copy in copies:
        copy.wait()


def send(items, collective_id):
    shapes, plan, scratch = [], [], []
    for x, axis, mode in items:
        count = lax.axis_size(axis)
        if mode == "lanes":
            piece = x.shape[:-1] + (x.shape[-1] // count,)
        elif mode == "lead":
            piece = x.shape[1:]
        else:
            piece = x.shape
        shapes.append(jax.ShapeDtypeStruct((count,) + piece, x.dtype))
        plan.append((axis, count, mode))
        scratch += [pltpu.SemaphoreType.DMA((count - 1,))] * 2
    return pl.pallas_call(
        functools.partial(send_kernel, tuple(plan)),
        out_shape=shapes,
        in_specs=[pl.BlockSpec(memory_space=pl.ANY)] * len(items),
        out_specs=[pl.BlockSpec(memory_space=pl.ANY)] * len(items),
        scratch_shapes=scratch,
        compiler_params=pltpu.CompilerParams(collective_id=collective_id, has_side_effects=True),
    )(*[x for x, _, _ in items])


def own_piece(x, axis, mode):
    me = lax.axis_index(axis)
    if mode == "lanes":
        lanes = x.shape[-1] // lax.axis_size(axis)
        return lax.dynamic_slice_in_dim(x, me * lanes, lanes, x.ndim - 1)
    if mode == "lead":
        return lax.dynamic_index_in_dim(x, me, 0, keepdims=False)
    return x


def sum_of(item, got):
    total = own_piece(*item).astype(jnp.float32)
    me = lax.axis_index(item[1])
    for sender in range(got.shape[0]):
        total += jnp.where(me == sender, 0.0, got[sender].astype(jnp.float32))
    return total


def all_of(item, got):
    return lax.dynamic_update_index_in_dim(got, own_piece(*item), lax.axis_index(item[1]), 0)


def gather(x, axis, collective_id):
    item = (x, axis, "whole")
    return all_of(item, send([item], collective_id)[0])


CORES = 2
LANE_PAIR = 2
ROOM = 40 * 2**20


def split_of(rep_count, tp_count):
    return rep_count // CORES, CORES, tp_count // CORES, CORES


def start_all(copies):
    for copy in copies:
        copy.start()


class Reduce:
    def __init__(self, rep_count, tp_count, rows, dev_cols, total_chunks):
        self.z, self.x, self.y, self.c = split_of(rep_count, tp_count)
        self.rows = rows
        self.half = 2 * LANES if dev_cols % (4 * LANES) == 0 else LANES
        self.per = dev_cols // (2 * self.half)
        self.dev_cols = dev_cols
        self.chunks = total_chunks
        self.blocks = self.z * self.x * self.y

    def chunk_bytes(self):
        return self.c * 2 * self.blocks * self.rows * self.half * 2 * 2

    def scratch(self, depth):
        n, z, x, y, rows, half = self.chunks, self.z, self.x, self.y, self.rows, self.half
        bf16 = jnp.bfloat16
        groups = self.c * y * 2 * (half // LANES)
        dma = pltpu.SemaphoreType.DMA
        buffers = dict(
            w=pltpu.VMEM((n, groups, depth // 2, 2, LANES), bf16),
            b0=pltpu.VMEM((n, self.c, 2, self.blocks, rows, half), bf16),
            r0=pltpu.VMEM((n, 2, self.blocks, rows, half), bf16),
            r1a=pltpu.VMEM((n, y - 1, x * z, rows, half), bf16),
            r1b=pltpu.VMEM((n, x - 1, y * z, rows, half), bf16),
            r2a=pltpu.VMEM((n, x - 1, z, rows, half), bf16),
            r2b=pltpu.VMEM((n, y - 1, z, rows, half), bf16),
            b3=pltpu.VMEM((n, z, 2, rows, half), bf16),
            r3=pltpu.VMEM((n, z - 1, 2, rows, half), bf16),
            ws=dma((n,)),
            s0=dma((2, n)),
            s1a=dma((2, n, y - 1)),
            s1b=dma((2, n, x - 1)),
            s2a=dma((2, n, x - 1)),
            s2b=dma((2, n, y - 1)),
            s3=dma((2, n, z - 1)),
        )
        return buffers

    def place(self):
        rep, tp = lax.axis_index("rep"), lax.axis_index("tp")
        self.rep, self.tp = rep, tp
        self.mz, self.mx = lax.div(rep, self.x), lax.rem(rep, self.x)
        self.my, self.mc = lax.div(tp, self.c), lax.rem(tp, self.c)

    def peer_z(self, to):
        return {"rep": to * self.x + self.mx}

    def peer_x(self, to):
        return {"rep": self.mz * self.x + to}

    def peer_y(self, to):
        return {"tp": to * self.c + self.mc}

    def peer_c(self):
        return {"tp": self.my * self.c + 1 - self.mc}

    def peers(self):
        out = [self.peer_c()]
        out += [self.peer_y(lax.rem(self.my + s, self.y)) for s in range(1, self.y)]
        out += [self.peer_x(lax.rem(self.mx + s, self.x)) for s in range(1, self.x)]
        out += [self.peer_z(lax.rem(self.mz + s, self.z)) for s in range(1, self.z)]
        return out

    def exchange(self, source, count, me, size, target, sems, i, peer):
        copies = []
        for step in range(1, count):
            to = lax.rem(me + step, count)
            copies.append(
                pltpu.make_async_remote_copy(
                    src_ref=source.at[pl.ds(to * size, size)],
                    dst_ref=target.at[i, step - 1],
                    send_sem=sems.at[0, i, step - 1],
                    recv_sem=sems.at[1, i, step - 1],
                    device_id=peer(to),
                    device_id_type=MESH,
                )
            )
        return copies

    def copies(self, s, i, stage):
        z, x, y = self.z, self.x, self.y
        if stage == 0:
            return [
                pltpu.make_async_remote_copy(
                    src_ref=s["b0"].at[i, 1 - self.mc],
                    dst_ref=s["r0"].at[i],
                    send_sem=s["s0"].at[0, i],
                    recv_sem=s["s0"].at[1, i],
                    device_id=self.peer_c(),
                    device_id_type=MESH,
                )
            ]
        if stage == 1:
            return self.exchange(
                s["r0"].at[i, 0], y, self.my, x * z, s["r1a"], s["s1a"], i, self.peer_y
            ) + self.exchange(
                s["r0"].at[i, 1], x, self.mx, y * z, s["r1b"], s["s1b"], i, self.peer_x
            )
        if stage == 2:
            return self.exchange(
                s["r1a"].at[i, 0], x, self.mx, z, s["r2a"], s["s2a"], i, self.peer_x
            ) + self.exchange(
                s["r1b"].at[i, 0], y, self.my, z, s["r2b"], s["s2b"], i, self.peer_y
            )
        third = []
        for step in range(1, z):
            to = lax.rem(self.mz + step, z)
            third.append(
                pltpu.make_async_remote_copy(
                    src_ref=s["b3"].at[i, to],
                    dst_ref=s["r3"].at[i, step - 1],
                    send_sem=s["s3"].at[0, i, step - 1],
                    recv_sem=s["s3"].at[1, i, step - 1],
                    device_id=self.peer_z(to),
                    device_id_type=MESH,
                )
            )
        return third

    def fetch(self, s, w_ref, i, column, pick):
        wide = 2 * self.half
        for y in range(self.y):
            for c in range(self.c):
                for k in range(wide // LANES):
                    at = (y * self.c + c) * self.dev_cols + column + k * LANES
                    at = pl.ds(pl.multiple_of(at, LANES), LANES)
                    pltpu.make_async_copy(
                        pick(w_ref, at),
                        s["w"].at[i, (y * self.c + c) * (wide // LANES) + k],
                        s["ws"].at[i],
                    ).start()

    def multiply(self, s, i, left):
        w = s["w"]
        pltpu.make_async_copy(w.at[i], w.at[i], s["ws"].at[i]).wait()
        depth = w.shape[2] * 2
        pieces = self.half // LANES
        for y in range(self.y):
            for c in range(self.c):
                for h in range(2):
                    first = ((y * self.c + c) * 2 + h) * pieces
                    right = [
                        w.at[i, first + k].reshape(depth, LANES)[...] for k in range(pieces)
                    ]
                    right = jnp.concatenate(right, axis=1) if pieces > 1 else right[0]
                    got = jnp.dot(left, right, preferred_element_type=jnp.float32)
                    got = got.astype(jnp.bfloat16)
                    got = got.reshape(self.z, self.x, self.rows, self.half)
                    for x in range(self.x):
                        at = (y * self.x + x) if h == 0 else (x * self.y + y)
                        s["b0"][i, c, h, at * self.z : (at + 1) * self.z] = got[:, x]
        start_all(self.copies(s, i, 0))

    def add(self, target, others):
        def piece(k, _):
            total = target[k].astype(jnp.float32)
            for other in others:
                total += other[k].astype(jnp.float32)
            target[k] = total.astype(jnp.bfloat16)
            return 0

        lax.fori_loop(0, target.shape[0], piece, 0, unroll=min(4, target.shape[0]))

    def after_core(self, s, i):
        for copy in self.copies(s, i, 0):
            copy.wait_recv()
        for h in range(2):
            self.add(s["r0"].at[i, h], [s["b0"].at[i, self.mc, h]])
        start_all(self.copies(s, i, 1))

    def after_first(self, s, i):
        for copy in self.copies(s, i, 1):
            copy.wait_recv()
        z = self.z
        for h, name, me, size, count in (
            (0, "r1a", self.my, self.x * z, self.y),
            (1, "r1b", self.mx, self.y * z, self.x),
        ):
            others = [s[name].at[i, k] for k in range(1, count - 1)]
            others.append(s["r0"].at[i, h, pl.ds(me * size, size)])
            self.add(s[name].at[i, 0], others)
        start_all(self.copies(s, i, 2))

    def after_second(self, s, i):
        for copy in self.copies(s, i, 2):
            copy.wait_recv()
        for h, name, came, me, count in (
            (0, "r2a", "r1a", self.mx, self.x),
            (1, "r2b", "r1b", self.my, self.y),
        ):
            for k in range(self.z):
                total = s[came][i, 0, me * self.z + k].astype(jnp.float32)
                for j in range(count - 1):
                    total += s[name][i, j, k].astype(jnp.float32)
                s["b3"][i, k, h] = total.astype(jnp.bfloat16)
        start_all(self.copies(s, i, 3))

    def after_third(self, s, i, store):
        for copy in self.copies(s, i, 3):
            copy.wait_recv()
        for h in range(2):
            total = s["b3"][i, self.mz, h].astype(jnp.float32)
            for k in range(self.z - 1):
                total += s["r3"][i, k, h].astype(jnp.float32)
            store(i, h, total)

    def finish(self, s):
        def one(i, _):
            for stage in range(4):
                for copy in self.copies(s, i, stage):
                    copy.wait_send()
            return 0

        lax.fori_loop(0, self.chunks, one, 0)

    def run(self, s, left_of, store, lags, extras=()):
        n = self.chunks
        stages = (
            (lags[3], lambda i: self.after_third(s, i, store)),
            (lags[2], lambda i: self.after_second(s, i)),
            (lags[1], lambda i: self.after_first(s, i)),
            (lags[0], lambda i: self.after_core(s, i)),
            (0, lambda i: self.multiply(s, i, left_of(i))),
        )

        def step(t, _):
            for lag, work in stages:
                @pl.when((t >= lag) & (t < n + lag))
                def _(lag=lag, work=work):
                    work(t - lag)
            for when, work in extras:
                pl.when(t == when)(work)
            return 0

        lax.fori_loop(0, n + lags[3], step, 0)
        self.finish(s)


def spread(rows, per, pairs):
    count, depth = rows.shape
    lane = lax.broadcasted_iota(jnp.int32, (depth, depth * pairs), 1)
    source = lax.broadcasted_iota(jnp.int32, (depth, depth * pairs), 0)
    parts = []
    for j in range(pairs):
        moves = (lane == source * pairs + j).astype(jnp.bfloat16)
        part = jnp.dot(rows, moves, preferred_element_type=jnp.float32)
        parts.append(part.reshape(count // per, 1, per, depth * pairs))
    wide = jnp.concatenate(parts, axis=1)
    return wide.reshape(count * pairs, depth * pairs).astype(jnp.bfloat16)


def greet(ids):
    barrier = pltpu.get_barrier_semaphore()
    for device in ids:
        pl.semaphore_signal(barrier, inc=1, device_id=device, device_id_type=MESH)
    pl.semaphore_wait(barrier, len(ids))


def device_of(index, tp_count):
    return {"rep": lax.div(index, tp_count), "tp": lax.rem(index, tp_count)}


def greet_all(count, me, tp_count):
    barrier = pltpu.get_barrier_semaphore()

    def one(step, _):
        to = device_of(lax.rem(me + step, count), tp_count)
        pl.semaphore_signal(barrier, inc=1, device_id=to, device_id_type=MESH)
        return 0

    lax.fori_loop(1, count, one, 0)
    pl.semaphore_wait(barrier, count - 1)


def scatter_start(source, target, sems, count, me, tp_count):
    whole = len(source.shape) == len(target.shape) - 1

    def one(step, _):
        to = lax.rem(me + step, count)
        pltpu.make_async_remote_copy(
            src_ref=source if whole else source.at[to],
            dst_ref=target.at[me],
            send_sem=sems.at[0],
            recv_sem=sems.at[1],
            device_id=device_of(to, tp_count),
            device_id_type=MESH,
        ).start()
        return 0

    lax.fori_loop(1, count, one, 0)


def scatter_wait(target, sems, which, count):
    part = target.at[pl.ds(0, count - 1)]
    pltpu.make_async_copy(part, part, sems.at[which]).wait()


def first_kernel(
    red, names, tok_ref, ids_ref, gain_ref, packed_ref, step_ref, sel_ref, w_ref,
    proj_ref, tokall_ref, idsall_ref, packall_ref, stepall_ref, selall_ref, *scratch
):
    s = dict(zip(names, scratch))
    red.place()
    tp_count, rep_count = red.y * red.c, red.z * red.x
    count = tp_count * rep_count
    rep, tp = red.rep, red.tp
    me = rep * tp_count + tp
    inner_dev = red.dev_cols
    for i in range(red.chunks):
        red.fetch(s, w_ref, i, i * 2 * red.half, lambda w, at: w.at[:, :, at])
    tok = tok_ref[...].astype(jnp.float32)
    width = tok.shape[0] * tok.shape[2]
    square = jnp.sum(jnp.sum(tok * tok, axis=0), axis=-1, keepdims=True)
    s["scale"][...] = jnp.broadcast_to(
        lax.rsqrt(square / width + epsilon), s["scale"].shape
    )
    greet_all(count, me, tp_count)
    scatter_start(tok_ref, tokall_ref, s["toks"], count, me, tp_count)
    scatter_start(ids_ref, idsall_ref, s["idss"], count, me, tp_count)
    tokall_ref[me] = tok_ref[me]
    idsall_ref[me] = ids_ref[...]
    peers = [lax.rem(tp + step, tp_count) for step in range(1, tp_count)]
    scale_copies, step_copies = [], []
    for k, to in enumerate(peers):
        scale_copies.append(
            pltpu.make_async_remote_copy(
                src_ref=s["scale"],
                dst_ref=s["scales"].at[tp],
                send_sem=s["scs"].at[0, k],
                recv_sem=s["scs"].at[1, k],
                device_id={"tp": to},
                device_id_type=MESH,
            )
        )
        columns = pl.ds(pl.multiple_of(to * inner_dev, LANES), inner_dev)
        step_copies.append(
            pltpu.make_async_remote_copy(
                src_ref=step_ref.at[:, columns],
                dst_ref=stepall_ref.at[rep, tp],
                send_sem=s["sts"].at[0, k],
                recv_sem=s["sts"].at[1, k],
                device_id={"tp": to},
                device_id_type=MESH,
            )
        )
    start_all(scale_copies)
    s["scales"][tp] = s["scale"][...]
    start_all(step_copies)
    columns = pl.ds(pl.multiple_of(tp * inner_dev, LANES), inner_dev)
    own_step = pltpu.make_async_copy(step_ref.at[:, columns], stepall_ref.at[rep, tp], s["own"].at[0])
    own_sel = pltpu.make_async_copy(sel_ref, selall_ref.at[rep], s["own"].at[1])
    own_step.start()
    own_sel.start()
    to_x = {"rep": red.mz * red.x + lax.rem(red.mx + 1, red.x)}
    slot = lax.rem(me, rep_count)
    home_tp = lax.div(me, rep_count)

    def pack_copy(to_rep):
        return pltpu.make_async_remote_copy(
            src_ref=packed_ref,
            dst_ref=packall_ref.at[slot],
            send_sem=s["pks"].at[0, to_rep],
            recv_sem=s["pks"].at[1, slot],
            device_id={"rep": to_rep, "tp": home_tp},
            device_id_type=MESH,
        )

    def is_me(to_rep):
        return (to_rep == rep) & (home_tp == tp)

    def pack_start(to_rep, _):
        @pl.when(is_me(to_rep))
        def _():
            packall_ref[slot] = packed_ref[...]

        @pl.when(jnp.logical_not(is_me(to_rep)))
        def _():
            pack_copy(to_rep).start()

        return 0

    def relay(ref, sems, source_rep, device, which):
        return pltpu.make_async_remote_copy(
            src_ref=ref.at[source_rep],
            dst_ref=ref.at[source_rep],
            send_sem=sems.at[0, which],
            recv_sem=sems.at[1, which],
            device_id=device,
            device_id_type=MESH,
        )

    z, x, mz, mx = red.z, red.x, red.mz, red.mx

    def up(ref, sems, k, sx, base):
        return relay(ref, sems, (mz - k + 1) * x + sx, {"rep": (mz + 1) * x + mx}, base + k - 1)

    def down(ref, sems, k, sx, base):
        return relay(ref, sems, (mz + k - 1) * x + sx, {"rep": (mz - 1) * x + mx}, base + k - 1)

    def up_came(ref, sems, k, sx, base):
        return relay(ref, sems, (mz - k) * x + sx, to_x, base + k - 1)

    def down_came(ref, sems, k, sx, base):
        return relay(ref, sems, (mz + k) * x + sx, to_x, base + k - 1)

    def round_start(ref, sems, k, columns):
        for n, sx in enumerate(columns):
            base = n * 2 * (z - 1)

            @pl.when((mz - k + 1 >= 0) & (mz + 1 < z))
            def _():
                up(ref, sems, k, sx, base).start()

            @pl.when((mz + k - 1 < z) & (mz - 1 >= 0))
            def _():
                down(ref, sems, k, sx, base + z - 1).start()

    def round_wait(ref, sems, k, columns, sent):
        for n, sx in enumerate(columns):
            base = n * 2 * (z - 1)

            if sent:
                @pl.when((mz - k + 1 >= 0) & (mz + 1 < z))
                def _():
                    up(ref, sems, k, sx, base).wait_send()

                @pl.when((mz + k - 1 < z) & (mz - 1 >= 0))
                def _():
                    down(ref, sems, k, sx, base + z - 1).wait_send()
            else:
                @pl.when(mz - k >= 0)
                def _():
                    up_came(ref, sems, k, sx, base).wait_recv()

                @pl.when(mz + k < z)
                def _():
                    down_came(ref, sems, k, sx, base + z - 1).wait_recv()

    both = list(range(x))
    mine = [mx]
    own_sel.wait()
    sel_x = relay(selall_ref, s["sxs"], rep, to_x, 0)
    sel_x.start()
    lax.fori_loop(0, rep_count, pack_start, 0)

    scatter_wait(tokall_ref, s["toks"], 1, count)
    tok_all = tokall_ref.reshape(count * tok_ref.shape[1], tok_ref.shape[2])[...]
    x_rows = (tok_all.astype(jnp.float32) * gain_ref[...].astype(jnp.float32)).astype(jnp.bfloat16)
    s["left"][...] = spread(x_rows, red.rows // 2, 2)
    for copy in scale_copies:
        copy.wait_recv()
    came = s["scales"].reshape(red.rows // 2, LANES)[:, :1]
    came = jnp.concatenate([came, came], axis=0)

    def store(i, h, total):
        at = pl.multiple_of(i * 2 * red.half + h * red.half, LANES)
        proj_ref[:, pl.ds(at, red.half)] = total * came

    def sel_first():
        relay(selall_ref, s["sxs"], red.mz * red.x + lax.rem(red.mx + 1, red.x), to_x, 0).wait_recv()
        round_start(selall_ref, s["szs"], 1, both)

    def step_first():
        own_step.wait()
        for copy in step_copies:
            copy.wait_recv()
        round_start(stepall_ref, s["tzs"], 1, mine)

    def next_round(ref, sems, k, columns):
        def work():
            round_wait(ref, sems, k - 1, columns, False)
            round_start(ref, sems, k, columns)
        return work

    sel_first()
    step_first()
    n = red.chunks
    extras = []
    lags = (1, 2, 3, 4)
    last = n + lags[3] - 1
    for k in range(2, z):
        extras.append((min(last, 2 * (k - 1)), next_round(stepall_ref, s["tzs"], k, mine)))
        extras.append((min(last, 2 * (k - 1) + 1), next_round(selall_ref, s["szs"], k, both)))
    red.run(s, lambda i: s["left"][...], store, lags, extras)
    round_wait(stepall_ref, s["tzs"], z - 1, mine, False)

    def step_x(source_z):
        return pltpu.make_async_remote_copy(
            src_ref=stepall_ref.at[source_z * x + mx],
            dst_ref=stepall_ref.at[source_z * x + mx],
            send_sem=s["txs"].at[0, source_z],
            recv_sem=s["txs"].at[1, source_z],
            device_id=to_x,
            device_id_type=MESH,
        )

    for k in range(z):
        step_x(k).start()
    round_wait(selall_ref, s["szs"], z - 1, both, False)
    for k in range(1, z):
        round_wait(selall_ref, s["szs"], k, both, True)
        round_wait(stepall_ref, s["tzs"], k, mine, True)
    for k in range(z):
        step_x(k).wait()
    sel_x.wait_send()
    for copy in step_copies + scale_copies:
        copy.wait_send()

    def pack_wait(k, _):
        @pl.when(jnp.logical_not(is_me(k)))
        def _():
            pack_copy(k).wait_send()

        @pl.when(tp * rep_count + k != me)
        def _():
            pltpu.make_async_copy(
                packall_ref.at[k], packall_ref.at[k], s["pks"].at[1, k]
            ).wait()

        return 0

    lax.fori_loop(0, rep_count, pack_wait, 0)
    scatter_wait(idsall_ref, s["idss"], 1, count)
    scatter_wait(idsall_ref, s["idss"], 0, count)
    scatter_wait(tokall_ref, s["toks"], 0, count)


def in_vmem(count):
    return [pl.BlockSpec(memory_space=pltpu.VMEM)] * count


def first_stage(tok, ids, gain, packed, step_proj, sel, w, rep_count, tp_count, inner_dev):
    f32, bf16 = jnp.float32, jnp.bfloat16
    count, tok_dev, slice_dev = tok.shape
    rows = 2 * tok_dev * tp_count
    red = Reduce(rep_count, tp_count, rows, inner_dev, 0)
    red.chunks = red.per
    dma = pltpu.SemaphoreType.DMA
    z, x = red.z, red.x
    scratch = red.scratch(2 * slice_dev)
    scratch.update(
        left=pltpu.VMEM((rep_count * rows, 2 * slice_dev), bf16),
        scale=pltpu.VMEM((tok_dev, LANES), f32),
        scales=pltpu.VMEM((tp_count, tok_dev, LANES), f32),
        toks=dma((2,)),
        idss=dma((2,)),
        scs=dma((2, tp_count - 1)),
        sts=dma((2, tp_count - 1)),
        pks=dma((2, rep_count)),
        own=dma((2,)),
        sxs=dma((2, 1)),
        txs=dma((2, z)),
        szs=dma((2, 2 * x * (z - 1))),
        tzs=dma((2, 2 * (z - 1))),
    )
    shape = jax.ShapeDtypeStruct
    return pl.pallas_call(
        functools.partial(first_kernel, red, tuple(scratch)),
        out_shape=[
            shape((rows, inner_dev), f32),
            shape((count, tok_dev, slice_dev), bf16),
            shape((count,) + ids.shape, bf16),
            shape((rep_count,) + packed.shape, bf16),
            shape((rep_count, tp_count, step_proj.shape[0], inner_dev), bf16),
            shape((rep_count,) + sel.shape, bf16),
        ],
        in_specs=in_vmem(4) + [pl.BlockSpec(memory_space=pl.ANY)] * 3,
        out_specs=in_vmem(6),
        scratch_shapes=list(scratch.values()),
        compiler_params=pltpu.CompilerParams(
            collective_id=0, has_side_effects=True, vmem_limit_bytes=62 * 2**20
        ),
        name="first_stage",
    )(tok, ids, gain, packed, step_proj, sel, w)


def last_kernel(
    red, names, begin, extra, x_ref, home_ref, stat_ref, w_ref, up_ref, *refs
):
    outs = 2 if extra else 0
    s = dict(zip(names, refs[outs:]))
    red.place()
    tp_count, rep_count = red.y * red.c, red.z * red.x
    count = tp_count * rep_count
    rep, tp = red.rep, red.tp
    me = rep * tp_count + tp
    wide = 2 * red.half
    for i in range(red.chunks):
        expert, column = divmod(begin + i, red.per)
        red.fetch(
            s, w_ref, i, column * wide, lambda w, at, expert=expert: w.at[:, expert, :, at]
        )
    for expert in range(x_ref.shape[0]):
        s["left"][expert] = spread(x_ref[expert], red.rows // 2, 2)
    if extra:
        homes_ref, stats_ref = refs[:2]
        greet_all(count, me, tp_count)
    else:
        greet(red.peers())

    def left_of(i):
        return s["left"][lax.div(begin + i, red.per)]

    def store(i, h, total):
        expert = lax.div(begin + i, red.per)
        column = lax.rem(begin + i, red.per) * wide + h * red.half
        up_ref[expert, :, pl.ds(pl.multiple_of(column, LANES), red.half)] = total

    def send_extra():
        scatter_start(home_ref, homes_ref, s["hos"], count, me, tp_count)
        homes_ref[me] = home_ref[me]

        def one(step, _):
            to = lax.rem(me + step, count)
            pltpu.make_async_remote_copy(
                src_ref=stat_ref.at[lax.div(to, tp_count)],
                dst_ref=stats_ref.at[me],
                send_sem=s["sas"].at[0],
                recv_sem=s["sas"].at[1],
                device_id=device_of(to, tp_count),
                device_id_type=MESH,
            ).start()
            return 0

        lax.fori_loop(1, count, one, 0)
        stats_ref[me] = stat_ref[rep]

    extras = [(2, send_extra)] if extra else []
    red.run(s, left_of, store, (1, 3, 5, 7), extras)
    if extra:
        for name, ref in (("hos", homes_ref), ("sas", stats_ref)):
            for which in range(2):
                scatter_wait(ref, s[name], which, count)


def last_stage(slots, home, stat, w, rep_count, tp_count, hidden_dev):
    f32, bf16 = jnp.float32, jnp.bfloat16
    experts, total_rows, slice_dev = slots.shape
    rows = 2 * total_rows // rep_count
    shape = jax.ShapeDtypeStruct
    dma = pltpu.SemaphoreType.DMA
    full = Reduce(rep_count, tp_count, rows, hidden_dev, 0)
    total = full.per * experts
    weights = w.size // experts // full.per * experts * 2 // experts
    most = max(1, ROOM // (full.chunk_bytes() + weights))
    begin, ups = 0, None
    while begin < total:
        red = Reduce(rep_count, tp_count, rows, hidden_dev, min(most, total - begin))
        extra = begin == 0
        scratch = red.scratch(2 * slice_dev)
        scratch["left"] = pltpu.VMEM((experts, rep_count * rows, 2 * slice_dev), bf16)
        outs = [shape((experts, rows, hidden_dev), f32)]
        if extra:
            scratch["hos"] = dma((2,))
            scratch["sas"] = dma((2,))
            count = rep_count * tp_count
            outs += [shape(home.shape, bf16), shape((count,) + stat.shape[1:], f32)]
        got = pl.pallas_call(
            functools.partial(last_kernel, red, tuple(scratch), begin, extra),
            out_shape=outs,
            in_specs=in_vmem(3) + [pl.BlockSpec(memory_space=pl.ANY)],
            out_specs=in_vmem(len(outs)),
            scratch_shapes=list(scratch.values()),
            compiler_params=pltpu.CompilerParams(
                collective_id=10 + begin, has_side_effects=True, vmem_limit_bytes=62 * 2**20
            ),
            name="last_stage",
        )(slots, home, stat, w)
        if extra:
            ups, homes, stats = got
        else:
            edge = begin // full.per
            column = (begin % full.per) * 2 * full.half
            at = lax.broadcasted_iota(jnp.int32, (experts, 1, hidden_dev), 2)
            order = lax.broadcasted_iota(jnp.int32, (experts, 1, hidden_dev), 0)
            older = (order < edge) | ((order == edge) & (at < column))
            ups = jnp.where(older, ups, got[0])
        begin += red.chunks
    return ups, homes, stats


def shards(
    tokens,
    conv_state,
    ssm_state,
    norm_gains,
    conv_weight,
    conv_skip,
    step_bias,
    decay_log,
    input_proj,
    select_proj,
    step_proj,
    output_proj,
    router,
    expert_proj,
    expert_ids,
):
    f32, bf16 = jnp.float32, jnp.bfloat16
    tp_count = lax.axis_size("tp")
    rep_count = lax.axis_size("rep")
    count = tp_count * rep_count
    rep_index = lax.axis_index("rep")
    tok_dev, width = tokens.shape
    slice_dev = width // count
    token_count = tok_dev * count
    req = tok_dev * tp_count
    inner_all = input_proj.shape[2]
    inner_dev = ssm_state.shape[2]
    state_count = ssm_state.shape[1]
    step_rank = step_proj.shape[0] * count
    expert_total = router.shape[1]
    window_count = expert_proj.shape[1]

    pieces = tokens.reshape(tok_dev, count, slice_dev).transpose(1, 0, 2)
    ids = jnp.pad(expert_ids.astype(bf16), ((0, 0), (0, LANES - 2)))
    packed = jnp.concatenate([conv_weight, conv_skip, step_bias[None], decay_log], axis=0)
    packed_rows = packed.shape[0]
    packed = jnp.pad(packed, ((0, -packed_rows % 16), (0, 0)))
    proj, tok_all, ids_all, packed, step_rows, select_rows = first_stage(
        pieces, ids, norm_gains[:1], packed, step_proj, select_proj.T, input_proj,
        rep_count, tp_count, inner_dev,
    )
    conv_input, gate_z = proj[:req], proj[req:]
    tok_slice = tok_all.reshape(token_count, slice_dev).astype(f32)
    ids_all = ids_all.reshape(token_count, LANES)[:, :2].astype(jnp.int32)
    select_rows = select_rows.reshape(-1, inner_dev)
    step_rows = step_rows.reshape(step_rank, inner_dev)
    packed = packed.transpose(1, 0, 2).reshape(-1, inner_dev)[:packed_rows].astype(f32)
    gains = norm_gains.astype(f32)

    window = jnp.arange(window_count, dtype=jnp.int32)
    names_first = ids_all[:, 0:1] == window[None, :]
    names_second = ids_all[:, 1:2] == window[None, :]
    routed = (names_first | names_second).astype(jnp.int32)
    routed = routed.reshape(count, tok_dev, window_count)
    position = jnp.cumsum(routed, axis=1) - routed
    slot_of = (position[..., None] == jnp.arange(CAPACITY, dtype=jnp.int32)) & (
        routed[..., None] > 0
    )
    slot_of = slot_of.astype(f32)
    slot_of, ids_all, tok_slice, packed = lax.optimization_barrier(
        (slot_of, ids_all, tok_slice, packed)
    )

    taps = conv_weight.shape[0]
    conv_taps = packed[:taps]
    skip_rows = packed[taps : taps + 2]
    shift_dev = packed[taps + 2]
    decay_dev = packed[taps + 3 :]
    history = conv_state.astype(f32)
    conv_mix = (
        jnp.sum(conv_taps[:-1, None, :] * history, axis=0)
        + conv_taps[-1] * conv_input
        + skip_rows[0]
    )
    conv_next = jnp.concatenate([conv_state[1:], conv_input.astype(bf16)[None]], axis=0)
    activated = jax.nn.silu(conv_mix)
    select_part = lax.dot_general(
        activated.astype(bf16), select_rows, (((1,), (1,)), ((), ())), preferred_element_type=f32
    )
    selected = jnp.sum(gather(select_part, "tp", 1), axis=0)
    step_low = selected[:, :step_rank].astype(bf16)
    input_map = selected[:, step_rank : step_rank + state_count]
    output_map = selected[:, step_rank + state_count :]
    step_size = jax.nn.softplus(
        jnp.dot(step_low, step_rows, preferred_element_type=f32) + shift_dev
    )
    decay_rate = -jnp.exp(decay_dev)
    factor = jnp.exp(step_size[:, None, :] * decay_rate[None])
    ssm_next = factor * ssm_state + (step_size * activated)[:, None, :] * input_map[:, :, None]
    readout = jnp.sum(ssm_next * output_map[:, :, None], axis=1) + skip_rows[1] * activated
    gated_out = (readout * jax.nn.silu(gate_z)).astype(bf16)

    gated_all = gather(gated_out, "rep", 2).reshape(token_count, inner_dev)
    gated_all = gather(gated_all, "tp", 3)
    gated_all = gated_all.transpose(1, 0, 2).reshape(token_count, inner_all)
    mixer_out = jnp.dot(gated_all, output_proj, preferred_element_type=f32)
    residual = tok_slice + mixer_out
    home = residual.astype(bf16).reshape(count, tok_dev, slice_dev)

    gained = residual * gains[1]
    logit_part = jnp.dot(
        gained, router.astype(f32), preferred_element_type=f32, precision=lax.Precision.HIGHEST
    )
    square_part = jnp.sum(residual * residual, axis=1, keepdims=True)
    stat = jnp.concatenate([logit_part, square_part], axis=1)
    stat = jnp.pad(stat, ((0, 0), (0, LANES - stat.shape[1]))).reshape(rep_count, req, LANES)
    blocks_x = gained.astype(bf16).reshape(count, tok_dev, slice_dev).astype(f32)
    slot_x = jnp.sum(slot_of[..., None] * blocks_x[:, :, None, None, :], axis=1).astype(bf16)
    rows_of = slot_x.transpose(1, 0, 2, 3).reshape(window_count, count * CAPACITY, slice_dev)
    hidden_dev = expert_proj.shape[3] // tp_count
    gate_up, home, stats = last_stage(
        rows_of, home, stat, expert_proj, rep_count, tp_count, hidden_dev
    )
    mamba_out = home.transpose(1, 0, 2).reshape(tok_dev, width)

    summed = jnp.sum(stats, axis=0)
    scale_two = lax.rsqrt(summed[:, expert_total : expert_total + 1] / width + epsilon)
    logits = summed[:, :expert_total] * scale_two
    ids_own = lax.dynamic_slice_in_dim(ids_all, rep_index * req, req, 0)
    choose = (
        ids_own[:, :, None] == jnp.arange(expert_total, dtype=jnp.int32)[None, None, :]
    ).astype(f32)
    picked = jnp.sum(choose * logits[:, None, :], axis=2)
    first_gate = jax.nn.sigmoid(picked[:, 0] - picked[:, 1])
    second_gate = jax.nn.sigmoid(picked[:, 1] - picked[:, 0])
    zero = jnp.zeros((), f32)
    gate_w = jnp.where(ids_own[:, 0:1] == window[None, :], first_gate[:, None], zero) + jnp.where(
        ids_own[:, 1:2] == window[None, :], second_gate[:, None], zero
    )
    slot_own = lax.dynamic_slice_in_dim(slot_of, rep_index * tp_count, tp_count, 0)
    gate_own = jnp.sum(
        slot_own * gate_w.reshape(tp_count, tok_dev, window_count)[..., None], axis=1
    ).astype(bf16).astype(f32)
    scale_own = jnp.sum(slot_own * scale_two.reshape(tp_count, tok_dev, 1, 1), axis=1)
    own = tp_count * CAPACITY
    gate_up = gate_up.reshape(window_count, 2, own, hidden_dev)
    scale_own = scale_own.transpose(1, 0, 2).reshape(window_count, own, 1)
    gate_own = gate_own.transpose(1, 0, 2).reshape(window_count, own, 1)
    hidden = gate_own * jax.nn.silu(gate_up[:, 0] * scale_own) * (gate_up[:, 1] * scale_own)
    hidden = hidden.astype(bf16).reshape(window_count, tp_count, CAPACITY, hidden_dev)
    expert_hidden = hidden.transpose(1, 0, 2, 3).reshape(window_count * own, hidden_dev)
    return (mamba_out, conv_next, ssm_next, expert_hidden)


def solution(mesh):
    in_specs = (
        P(("rep", "tp"), None),
        P(None, "rep", "tp"),
        P("rep", None, "tp"),
        P(None, ("rep", "tp")),
        P(None, ("rep", "tp")),
        P(None, ("rep", "tp")),
        P(("rep", "tp")),
        P(None, ("rep", "tp")),
        P(("rep", "tp"), None, None),
        P("tp", "rep"),
        P(("rep", "tp"), None),
        P(None, ("rep", "tp")),
        P(("rep", "tp"), None),
        P(("rep", "tp"), None, None, None),
        P(("rep", "tp"), None),
    )
    out_specs = (P(("rep", "tp"), None), P(None, "rep", "tp"), P("rep", None, "tp"), P("rep", "tp"))
    return jax.shard_map(shards, mesh=mesh, in_specs=in_specs, out_specs=out_specs, check_vma=False)
```

```python
import functools

import jax
import jax.numpy as jnp
from jax import lax
from jax.experimental import pallas as pl
from jax.experimental.pallas import tpu as pltpu
from jax.sharding import PartitionSpec as P

CAPACITY = 2
LANES = 128


epsilon = 1e-05
MESH = pl.DeviceIdType.MESH


CORES = 2
LANE_PAIR = 2
ROOM = 40 * 2**20


def split_of(rep_count, tp_count):
    return rep_count // CORES, CORES, tp_count // CORES, CORES


def start_all(copies):
    for copy in copies:
        copy.start()


class Reduce:
    def __init__(self, rep_count, tp_count, rows, dev_cols, total_chunks):
        self.z, self.x, self.y, self.c = split_of(rep_count, tp_count)
        self.rows = rows
        self.half = 2 * LANES if dev_cols % (4 * LANES) == 0 else LANES
        self.per = dev_cols // (2 * self.half)
        self.dev_cols = dev_cols
        self.chunks = total_chunks
        self.blocks = self.z * self.x * self.y

    def chunk_bytes(self):
        return self.c * 2 * self.blocks * self.rows * self.half * 2 * 2

    def scratch(self, depth):
        n, z, x, y, rows, half = self.chunks, self.z, self.x, self.y, self.rows, self.half
        bf16 = jnp.bfloat16
        groups = self.c * y * 2 * (half // LANES)
        dma = pltpu.SemaphoreType.DMA
        buffers = dict(
            w=pltpu.VMEM((n, groups, depth // 2, 2, LANES), bf16),
            b0=pltpu.VMEM((n, self.c, 2, self.blocks, rows, half), bf16),
            r0=pltpu.VMEM((n, 2, self.blocks, rows, half), bf16),
            r1a=pltpu.VMEM((n, y - 1, x * z, rows, half), bf16),
            r1b=pltpu.VMEM((n, x - 1, y * z, rows, half), bf16),
            r2a=pltpu.VMEM((n, x - 1, z, rows, half), bf16),
            r2b=pltpu.VMEM((n, y - 1, z, rows, half), bf16),
            b3=pltpu.VMEM((n, z, 2, rows, half), bf16),
            r3=pltpu.VMEM((n, z - 1, 2, rows, half), bf16),
            ws=dma((n,)),
            s0=dma((2, n)),
            s1a=dma((2, n, y - 1)),
            s1b=dma((2, n, x - 1)),
            s2a=dma((2, n, x - 1)),
            s2b=dma((2, n, y - 1)),
            s3=dma((2, n, z - 1)),
        )
        return buffers

    def place(self):
        rep, tp = lax.axis_index("rep"), lax.axis_index("tp")
        self.rep, self.tp = rep, tp
        self.mz, self.mx = lax.div(rep, self.x), lax.rem(rep, self.x)
        self.my, self.mc = lax.div(tp, self.c), lax.rem(tp, self.c)

    def peer_z(self, to):
        return {"rep": to * self.x + self.mx}

    def peer_x(self, to):
        return {"rep": self.mz * self.x + to}

    def peer_y(self, to):
        return {"tp": to * self.c + self.mc}

    def peer_c(self):
        return {"tp": self.my * self.c + 1 - self.mc}

    def peers(self):
        out = [self.peer_c()]
        out += [self.peer_y(lax.rem(self.my + s, self.y)) for s in range(1, self.y)]
        out += [self.peer_x(lax.rem(self.mx + s, self.x)) for s in range(1, self.x)]
        out += [self.peer_z(lax.rem(self.mz + s, self.z)) for s in range(1, self.z)]
        return out

    def exchange(self, source, count, me, size, target, sems, i, peer):
        copies = []
        for step in range(1, count):
            to = lax.rem(me + step, count)
            copies.append(
                pltpu.make_async_remote_copy(
                    src_ref=source.at[pl.ds(to * size, size)],
                    dst_ref=target.at[i, step - 1],
                    send_sem=sems.at[0, i, step - 1],
                    recv_sem=sems.at[1, i, step - 1],
                    device_id=peer(to),
                    device_id_type=MESH,
                )
            )
        return copies

    def copies(self, s, i, stage):
        z, x, y = self.z, self.x, self.y
        if stage == 0:
            return [
                pltpu.make_async_remote_copy(
                    src_ref=s["b0"].at[i, 1 - self.mc],
                    dst_ref=s["r0"].at[i],
                    send_sem=s["s0"].at[0, i],
                    recv_sem=s["s0"].at[1, i],
                    device_id=self.peer_c(),
                    device_id_type=MESH,
                )
            ]
        if stage == 1:
            return self.exchange(
                s["r0"].at[i, 0], y, self.my, x * z, s["r1a"], s["s1a"], i, self.peer_y
            ) + self.exchange(
                s["r0"].at[i, 1], x, self.mx, y * z, s["r1b"], s["s1b"], i, self.peer_x
            )
        if stage == 2:
            return self.exchange(
                s["r1a"].at[i, 0], x, self.mx, z, s["r2a"], s["s2a"], i, self.peer_x
            ) + self.exchange(
                s["r1b"].at[i, 0], y, self.my, z, s["r2b"], s["s2b"], i, self.peer_y
            )
        third = []
        for step in range(1, z):
            to = lax.rem(self.mz + step, z)
            third.append(
                pltpu.make_async_remote_copy(
                    src_ref=s["b3"].at[i, to],
                    dst_ref=s["r3"].at[i, step - 1],
                    send_sem=s["s3"].at[0, i, step - 1],
                    recv_sem=s["s3"].at[1, i, step - 1],
                    device_id=self.peer_z(to),
                    device_id_type=MESH,
                )
            )
        return third

    def fetch(self, s, w_ref, i, column, pick):
        wide = 2 * self.half
        for y in range(self.y):
            for c in range(self.c):
                for k in range(wide // LANES):
                    at = (y * self.c + c) * self.dev_cols + column + k * LANES
                    at = pl.ds(pl.multiple_of(at, LANES), LANES)
                    pltpu.make_async_copy(
                        pick(w_ref, at),
                        s["w"].at[i, (y * self.c + c) * (wide // LANES) + k],
                        s["ws"].at[i],
                    ).start()

    def multiply(self, s, i, left):
        w = s["w"]
        pltpu.make_async_copy(w.at[i], w.at[i], s["ws"].at[i]).wait()
        depth = w.shape[2] * 2
        pieces = self.half // LANES
        for y in range(self.y):
            for c in range(self.c):
                for h in range(2):
                    first = ((y * self.c + c) * 2 + h) * pieces
                    right = [
                        w.at[i, first + k].reshape(depth, LANES)[...] for k in range(pieces)
                    ]
                    right = jnp.concatenate(right, axis=1) if pieces > 1 else right[0]
                    got = jnp.dot(left, right, preferred_element_type=jnp.float32)
                    got = got.astype(jnp.bfloat16)
                    got = got.reshape(self.z, self.x, self.rows, self.half)
                    for x in range(self.x):
                        at = (y * self.x + x) if h == 0 else (x * self.y + y)
                        s["b0"][i, c, h, at * self.z : (at + 1) * self.z] = got[:, x]
        start_all(self.copies(s, i, 0))

    def add(self, target, others):
        def piece(k, _):
            total = target[k].astype(jnp.float32)
            for other in others:
                total += other[k].astype(jnp.float32)
            target[k] = total.astype(jnp.bfloat16)
            return 0

        lax.fori_loop(0, target.shape[0], piece, 0, unroll=min(4, target.shape[0]))

    def after_core(self, s, i):
        for copy in self.copies(s, i, 0):
            copy.wait_recv()
        for h in range(2):
            self.add(s["r0"].at[i, h], [s["b0"].at[i, self.mc, h]])
        start_all(self.copies(s, i, 1))

    def after_first(self, s, i):
        for copy in self.copies(s, i, 1):
            copy.wait_recv()
        z = self.z
        for h, name, me, size, count in (
            (0, "r1a", self.my, self.x * z, self.y),
            (1, "r1b", self.mx, self.y * z, self.x),
        ):
            others = [s[name].at[i, k] for k in range(1, count - 1)]
            others.append(s["r0"].at[i, h, pl.ds(me * size, size)])
            self.add(s[name].at[i, 0], others)
        start_all(self.copies(s, i, 2))

    def after_second(self, s, i):
        for copy in self.copies(s, i, 2):
            copy.wait_recv()
        for h, name, came, me, count in (
            (0, "r2a", "r1a", self.mx, self.x),
            (1, "r2b", "r1b", self.my, self.y),
        ):
            for k in range(self.z):
                total = s[came][i, 0, me * self.z + k].astype(jnp.float32)
                for j in range(count - 1):
                    total += s[name][i, j, k].astype(jnp.float32)
                s["b3"][i, k, h] = total.astype(jnp.bfloat16)
        start_all(self.copies(s, i, 3))

    def after_third(self, s, i, store, done):
        for copy in self.copies(s, i, 3):
            copy.wait_recv()
        for h in range(2):
            total = s["b3"][i, self.mz, h].astype(jnp.float32)
            for k in range(self.z - 1):
                total += s["r3"][i, k, h].astype(jnp.float32)
            store(i, h, total)
        done(i)

    def finish(self, s):
        def one(i, _):
            for stage in range(4):
                for copy in self.copies(s, i, stage):
                    copy.wait_send()
            return 0

        lax.fori_loop(0, self.chunks, one, 0)

    def run(self, s, left_of, store, lags, extras=(), done=lambda i: None):
        n = self.chunks
        stages = (
            (lags[3], lambda i: self.after_third(s, i, store, done)),
            (lags[2], lambda i: self.after_second(s, i)),
            (lags[1], lambda i: self.after_first(s, i)),
            (lags[0], lambda i: self.after_core(s, i)),
            (0, lambda i: self.multiply(s, i, left_of(i))),
        )

        def step(t, _):
            for lag, work in stages:
                @pl.when((t >= lag) & (t < n + lag))
                def _(lag=lag, work=work):
                    work(t - lag)
            for when, work in extras:
                pl.when(t == when)(work)
            return 0

        lax.fori_loop(0, n + lags[3], step, 0)
        self.finish(s)


def spread(rows, per, pairs):
    count, depth = rows.shape
    lane = lax.broadcasted_iota(jnp.int32, (depth, depth * pairs), 1)
    source = lax.broadcasted_iota(jnp.int32, (depth, depth * pairs), 0)
    parts = []
    for j in range(pairs):
        moves = (lane == source * pairs + j).astype(jnp.bfloat16)
        part = jnp.dot(rows, moves, preferred_element_type=jnp.float32)
        parts.append(part.reshape(count // per, 1, per, depth * pairs))
    wide = jnp.concatenate(parts, axis=1)
    return wide.reshape(count * pairs, depth * pairs).astype(jnp.bfloat16)


def greet(ids):
    barrier = pltpu.get_barrier_semaphore()
    for device in ids:
        pl.semaphore_signal(barrier, inc=1, device_id=device, device_id_type=MESH)
    pl.semaphore_wait(barrier, len(ids))


def device_of(index, tp_count):
    return {"rep": lax.div(index, tp_count), "tp": lax.rem(index, tp_count)}


def greet_all(count, me, tp_count):
    barrier = pltpu.get_barrier_semaphore()

    def one(step, _):
        to = device_of(lax.rem(me + step, count), tp_count)
        pl.semaphore_signal(barrier, inc=1, device_id=to, device_id_type=MESH)
        return 0

    lax.fori_loop(1, count, one, 0)
    pl.semaphore_wait(barrier, count - 1)


def scatter_start(source, target, sems, count, me, tp_count):
    whole = len(source.shape) == len(target.shape) - 1

    def one(step, _):
        to = lax.rem(me + step, count)
        pltpu.make_async_remote_copy(
            src_ref=source if whole else source.at[to],
            dst_ref=target.at[me],
            send_sem=sems.at[0],
            recv_sem=sems.at[1],
            device_id=device_of(to, tp_count),
            device_id_type=MESH,
        ).start()
        return 0

    lax.fori_loop(1, count, one, 0)


def scatter_wait(target, sems, which, count):
    part = target.at[pl.ds(0, count - 1)]
    pltpu.make_async_copy(part, part, sems.at[which]).wait()


def in_vmem(count):
    return [pl.BlockSpec(memory_space=pltpu.VMEM)] * count


def remote(source, target, send_sem, recv_sem, device):
    return pltpu.make_async_remote_copy(
        src_ref=source,
        dst_ref=target,
        send_sem=send_sem,
        recv_sem=recv_sem,
        device_id=device,
        device_id_type=MESH,
    )


def silu(v):
    return v / (1.0 + jnp.exp(-v))


def softplus(v):
    return jnp.maximum(v, 0.0) + jnp.log1p(jnp.exp(-jnp.abs(v)))


def column_iota(shape, axis):
    return lax.broadcasted_iota(jnp.int32, shape, axis)


def named(ids, lane):
    ids = ids.astype(jnp.float32).astype(jnp.int32)
    return ids[:, :1] == lane, ids[:, 1:2] == lane


def slot_maps(ids, experts, tok_dev):
    rows = ids.shape[0]
    first, second = named(ids, column_iota((rows, LANES), 1))
    routed = (first | second).astype(jnp.float32)
    later, earlier = column_iota((rows, rows), 0), column_iota((rows, rows), 1)
    before = (earlier < later) & (lax.div(earlier, tok_dev) == lax.div(later, tok_dev))
    position = jnp.dot(
        before.astype(jnp.bfloat16), routed.astype(jnp.bfloat16), preferred_element_type=jnp.float32
    )
    slots = rows // tok_dev * CAPACITY
    row, slot = column_iota((rows, slots), 0), column_iota((rows, slots), 1)
    block = lax.div(row, tok_dev) == lax.div(slot, CAPACITY)
    seat = lax.rem(slot, CAPACITY).astype(jnp.float32)
    maps = []
    for e in range(experts):
        taken = block & (routed[:, e : e + 1] > 0.5) & (position[:, e : e + 1] == seat)
        maps.append(taken.astype(jnp.float32))
    return maps


def mixer_kernel(
    red, names, experts,
    tok_ref, ids_ref, gains_ref, packed_ref, sel_ref, history_ref, router_ref,
    step_ref, w_ref, state_ref, out_w_ref,
    next_ref, state_out_ref, home_ref, stat_ref, slots_ref, idsall_ref, *scratch
):
    f32, bf16 = jnp.float32, jnp.bfloat16
    s = dict(zip(names, scratch))
    red.place()
    z, x, y, c = red.z, red.x, red.y, red.c
    mz, mx, my, mc = red.mz, red.mx, red.my, red.mc
    tp_count, rep_count = y * c, z * x
    count = tp_count * rep_count
    rep, tp = red.rep, red.tp
    me = rep * tp_count + tp
    inner_dev = red.dev_cols
    req = red.rows // 2
    tok_dev, slice_dev = tok_ref.shape[1:]
    tokall, packall, stepall = s["tokall"], s["packall"], s["stepall"]
    taps = history_ref.shape[0] + 1
    states = state_ref.shape[1]

    state_in = pltpu.make_async_copy(state_ref, s["state"], s["own"].at[1])
    out_in = pltpu.make_async_copy(out_w_ref, s["outw"], s["own"].at[2])
    for i in range(red.chunks):
        red.fetch(s, w_ref, i, i * 2 * red.half, lambda w, at: w.at[:, :, at])
    columns = pl.ds(pl.multiple_of(tp * inner_dev, LANES), inner_dev)
    own_step = pltpu.make_async_copy(step_ref.at[:, columns], stepall.at[rep, tp], s["own"].at[0])
    own_step.start()
    state_in.start()
    out_in.start()
    tok = tok_ref[...].astype(f32)
    width = tok.shape[0] * tok.shape[2]
    square = jnp.sum(jnp.sum(tok * tok, axis=0), axis=-1, keepdims=True)
    s["scale"][...] = jnp.broadcast_to(lax.rsqrt(square / width + epsilon), s["scale"].shape)
    greet_all(count, me, tp_count)
    scatter_start(tok_ref, tokall, s["toks"], count, me, tp_count)
    tokall[me] = tok_ref[me]
    slot = lax.rem(me, rep_count)
    home_tp = lax.div(me, rep_count)

    def pack_copy(to_rep):
        return remote(
            packed_ref, packall.at[slot], s["pks"].at[0, to_rep], s["pks"].at[1, slot],
            {"rep": to_rep, "tp": home_tp},
        )

    def is_me(to_rep):
        return (to_rep == rep) & (home_tp == tp)

    def pack_start(to_rep, _):
        @pl.when(is_me(to_rep))
        def _():
            packall[slot] = packed_ref[...]

        @pl.when(jnp.logical_not(is_me(to_rep)))
        def _():
            pack_copy(to_rep).start()

        return 0

    lax.fori_loop(0, rep_count, pack_start, 0)
    scale_copies, step_copies = [], []
    for k in range(tp_count - 1):
        to = lax.rem(tp + k + 1, tp_count)
        scale_copies.append(
            remote(
                s["scale"], s["scales"].at[tp], s["scs"].at[0, k], s["scs"].at[1, k], {"tp": to}
            )
        )
        columns = pl.ds(pl.multiple_of(to * inner_dev, LANES), inner_dev)
        step_copies.append(
            remote(
                step_ref.at[:, columns], stepall.at[rep, tp],
                s["sts"].at[0, k], s["sts"].at[1, k], {"tp": to},
            )
        )
    start_all(scale_copies)
    s["scales"][tp] = s["scale"][...]
    start_all(step_copies)
    scatter_start(ids_ref, idsall_ref, s["idss"], count, me, tp_count)
    idsall_ref[me] = ids_ref[...]
    to_x = {"rep": mz * x + lax.rem(mx + 1, x)}

    def relay(source_z, device, which):
        block = stepall.at[source_z * x + mx]
        return remote(block, block, s["tzs"].at[0, which], s["tzs"].at[1, which], device)

    def up(k):
        return relay(mz - k + 1, {"rep": (mz + 1) * x + mx}, k - 1)

    def down(k):
        return relay(mz + k - 1, {"rep": (mz - 1) * x + mx}, z - 1 + k - 1)

    def round_start(k):
        @pl.when((mz - k + 1 >= 0) & (mz + 1 < z))
        def _():
            up(k).start()

        @pl.when((mz + k - 1 < z) & (mz - 1 >= 0))
        def _():
            down(k).start()

    def round_sent(k):
        @pl.when((mz - k + 1 >= 0) & (mz + 1 < z))
        def _():
            up(k).wait_send()

        @pl.when((mz + k - 1 < z) & (mz - 1 >= 0))
        def _():
            down(k).wait_send()

    def step_x(source_z):
        return remote(
            stepall.at[source_z * x + mx], stepall.at[source_z * x + mx],
            s["txs"].at[0, source_z], s["txs"].at[1, source_z], to_x,
        )

    def round_came(k):
        @pl.when(mz - k >= 0)
        def _():
            relay(mz - k, to_x, k - 1).wait_recv()
            step_x(mz - k).start()

        @pl.when(mz + k < z)
        def _():
            relay(mz + k, to_x, z - 1 + k - 1).wait_recv()
            step_x(mz + k).start()

    s["sel"][...] = jnp.zeros(s["sel"].shape, bf16)
    part_cols = sel_ref.shape[0]
    s["sel"][:part_cols] = sel_ref[...]
    s["router"][...] = jnp.zeros(s["router"].shape, f32)
    s["router"][:, : router_ref.shape[1]] = router_ref[...].astype(f32)
    next_ref[: taps - 2] = history_ref[1:]

    scatter_wait(tokall, s["toks"], 1, count)
    tok_all = tokall.reshape(count * tok_dev, slice_dev)
    gain = gains_ref[...].astype(f32)
    x_rows = (tok_all[...].astype(f32) * gain[:1]).astype(bf16)
    s["left"][...] = spread(x_rows, req, 2)

    def step_first():
        own_step.wait()
        for copy in step_copies:
            copy.wait_recv()
        round_start(1)
        step_x(mz).start()

    def params():
        for copy in scale_copies:
            copy.wait_recv()

        def pack_came(k, _):
            @pl.when(tp * rep_count + k != me)
            def _():
                pltpu.make_async_copy(packall.at[k], packall.at[k], s["pks"].at[1, k]).wait()

            return 0

        lax.fori_loop(0, rep_count, pack_came, 0)
        own = packed_ref.shape[1]
        for k in range(rep_count):
            s["par"][:, k * own : (k + 1) * own] = packall[k].astype(f32)

    def maps():
        scatter_wait(idsall_ref, s["idss"], 1, count)
        ids = idsall_ref.reshape(count * tok_dev, LANES)[...]
        for e, taken in enumerate(slot_maps(ids, experts, tok_dev)):
            s["maps"][e] = taken.astype(bf16)

    def next_round(k):
        def work():
            round_came(k - 1)
            round_start(k)

        return work

    def store(i, h, total):
        at = pl.ds(pl.multiple_of(i * 2 * red.half + h * red.half, LANES), red.half)
        scale = s["scales"].reshape(req, LANES)[:, :1]
        conv_input = total[:req] * scale
        s["gate"][:, at] = total[req:] * scale
        next_ref[taps - 2, :, at] = conv_input.astype(bf16)
        par = s["par"]
        mix = par[taps - 1 : taps, at] * conv_input + par[taps : taps + 1, at]
        for k in range(taps - 1):
            mix += par[k : k + 1, at] * history_ref[k, :, at].astype(f32)
        act = silu(mix)
        s["act"][:, at] = act
        s["actall"][rep, :, at] = act.astype(bf16)

    def act_copies(i):
        at = pl.ds(pl.multiple_of(i * 2 * red.half, LANES), 2 * red.half)
        block = s["actall"].at[rep, :, at]
        return [
            remote(
                block, block, s["acs"].at[0, i, k], s["acs"].at[1, i, k],
                {"rep": lax.rem(rep + k + 1, rep_count)},
            )
            for k in range(rep_count - 1)
        ]

    lags = (1, 2, 3, 4)
    last = red.chunks + lags[3] - 1
    extras = [(0, step_first), (1, params), (2, maps)]
    for k in range(2, z):
        extras.append((min(last, 2 * k - 1), next_round(k)))
    red.run(
        s, lambda i: s["left"][...], store, lags, extras, lambda i: start_all(act_copies(i))
    )
    round_came(z - 1)

    def act_came(i, _):
        for copy in act_copies(i):
            copy.wait_recv()
        return 0

    lax.fori_loop(0, red.chunks, act_came, 0)
    every = s["actall"].reshape(rep_count * req, inner_dev)[...]
    part = lax.dot_general(
        every, s["sel"][...], (((1,), (1,)), ((), ())), preferred_element_type=f32
    )
    s["part"][...] = part.astype(bf16).reshape(rep_count, req, LANES)

    def part_start(step, _):
        to = lax.rem(me + step, count)
        remote(
            s["part"].at[lax.div(to, tp_count)], s["parts"].at[me],
            s["pts"].at[0], s["pts"].at[1], device_of(to, tp_count),
        ).start()
        return 0

    lax.fori_loop(1, count, part_start, 0)
    s["parts"][me] = s["part"][rep]
    scatter_wait(s["parts"], s["pts"], 1, count)
    total_cols = part_cols * rep_count
    tiles = [jnp.zeros((req, LANES), f32) for _ in range(-(-total_cols // LANES))]
    lane = column_iota((req, LANES), 1)
    for r in range(rep_count):
        cols = s["parts"][r * tp_count].astype(f32)
        for p in range(1, tp_count):
            cols += s["parts"][r * tp_count + p].astype(f32)
        tile, shift = divmod(r * part_cols, LANES)
        if shift:
            cols = pltpu.roll(cols, shift, 1)
        tiles[tile] += jnp.where(lane >= shift, cols, 0.0)
        if shift + part_cols > LANES:
            tiles[tile + 1] += jnp.where(lane < shift + part_cols - LANES, cols, 0.0)
    rank = total_cols - 2 * states
    low_tiles = rank // LANES
    low = jnp.concatenate(tiles[:low_tiles], axis=1).astype(bf16)
    both_maps = jnp.concatenate(
        [tiles[low_tiles], jnp.zeros((LANES - req, LANES), f32)], axis=0
    ).T
    s["bc"][...] = both_maps
    for k in range(z):
        step_x(k).wait_recv()
    if step_ref.shape[0] % 8 == 0:
        step_rows = stepall.reshape(rank, inner_dev)[...]
    else:
        step_rows = stepall[...].reshape(rank, inner_dev)
    step_pre = jnp.dot(low, step_rows, preferred_element_type=f32)
    s["step"][...] = softplus(step_pre + s["par"][taps + 2 : taps + 3])
    state_in.wait()
    wide = 2 * LANES
    ways = CORES
    piece = inner_dev // ways
    gall = s["gall"]

    def scan_block(b, _):
        at = pl.ds(pl.multiple_of(b * wide, LANES), wide)
        decay = -jnp.exp(s["par"][taps + 3 : taps + 3 + states, at])
        step, act = s["step"][:, at], s["act"][:, at]
        for t in range(req):
            row = step[t : t + 1]
            now = jnp.exp(row * decay) * s["state"][t, :, at]
            now += (row * act[t : t + 1]) * s["bc"][:states, t : t + 1]
            s["state"][t, :, at] = now
            s["read"][t : t + 1, at] = jnp.sum(
                now * s["bc"][states : 2 * states, t : t + 1], axis=0, keepdims=True
            )
        read = s["read"][:, at] + s["par"][taps + 1 : taps + 2, at] * act
        gall[my, mc, mz, mx, :, at] = (read * silu(s["gate"][:, at])).astype(bf16)
        return 0

    def along_z(h):
        at = pl.ds(h * piece, piece)
        block = gall.at[my, mc, mz, mx, :, at]
        return [
            remote(
                block, block, s["gzs"].at[0, h, k], s["gzs"].at[1, h, k],
                red.peer_z(lax.rem(mz + k + 1, z)),
            )
            for k in range(z - 1)
        ]

    def along_xy(h):
        at = pl.ds(h * piece, piece)
        block = gall.at[my, mc, :, mx, :, at]
        out = []
        for k in range(1, x * y):
            dx, dy = k % x, k // x
            device = {
                "rep": mz * x + lax.rem(mx + dx, x),
                "tp": lax.rem(my + dy, y) * c + mc,
            }
            out.append(
                remote(block, block, s["gxs"].at[0, h, k - 1], s["gxs"].at[1, h, k - 1], device)
            )
        return out

    def along_core(h):
        block = gall.at[:, mc, :, :, :, pl.ds(h * piece, piece)]
        return remote(block, block, s["gcs"].at[0, h], s["gcs"].at[1, h], red.peer_c())

    blocks = piece // wide
    for h in range(ways):
        lax.fori_loop(h * blocks, (h + 1) * blocks, scan_block, 0)
        start_all(along_z(h))
    state_out = pltpu.make_async_copy(s["state"], state_out_ref, s["own"].at[3])
    state_out.start()
    for h in range(ways):
        for copy in along_z(h):
            copy.wait_recv()
        start_all(along_xy(h))
    for h in range(ways):
        for copy in along_xy(h):
            copy.wait_recv()
        along_core(h).start()
    out_in.wait()

    def product(core):
        total = jnp.zeros((rep_count * req, slice_dev), f32)
        for k in range(y):
            rows = gall.at[k, core].reshape(rep_count * req, inner_dev)[...]
            at = pl.multiple_of((k * c + core) * inner_dev, LANES)
            total += jnp.dot(rows, s["outw"][pl.ds(at, inner_dev)], preferred_element_type=f32)
        return total

    mixed = product(mc)
    for h in range(ways):
        along_core(h).wait_recv()
    residual = tok_all[...].astype(f32) + mixed + product(1 - mc)
    home_ref.reshape(count * tok_dev, slice_dev)[...] = residual.astype(bf16)
    gained = residual * gain[1:2]
    stat = jnp.dot(
        gained, s["router"][...], preferred_element_type=f32, precision=lax.Precision.HIGHEST
    )
    squares = jnp.sum(residual * residual, axis=1, keepdims=True)
    lane = column_iota(stat.shape, 1)
    stat = jnp.where(lane == router_ref.shape[1], squares, stat)
    stat_ref[...] = stat.reshape(rep_count, req, LANES)
    for e in range(experts):
        slots_ref[e] = lax.dot_general(
            s["maps"][e], gained.astype(bf16), (((0,), (0,)), ((), ())), preferred_element_type=f32
        ).astype(bf16)

    for k in range(1, z):
        round_sent(k)
    for k in range(z):
        step_x(k).wait_send()
    for copy in step_copies + scale_copies:
        copy.wait_send()

    def pack_sent(k, _):
        @pl.when(jnp.logical_not(is_me(k)))
        def _():
            pack_copy(k).wait_send()

        return 0

    lax.fori_loop(0, rep_count, pack_sent, 0)

    def act_sent(i, _):
        for copy in act_copies(i):
            copy.wait_send()
        return 0

    lax.fori_loop(0, red.chunks, act_sent, 0)
    for h in range(ways):
        for copy in along_z(h) + along_xy(h) + [along_core(h)]:
            copy.wait_send()
    scatter_wait(idsall_ref, s["idss"], 0, count)
    scatter_wait(tokall, s["toks"], 0, count)
    scatter_wait(s["parts"], s["pts"], 0, count)
    state_out.wait()


def mixer(args, rep_count, tp_count, experts):
    tok, ids, gains, packed, sel, history, router, step_proj, w, state, out_w = args
    f32, bf16 = jnp.float32, jnp.bfloat16
    count, tok_dev, slice_dev = tok.shape
    req, states, inner_dev = state.shape
    red = Reduce(rep_count, tp_count, 2 * req, inner_dev, 0)
    n = red.chunks = red.per
    dma = pltpu.SemaphoreType.DMA
    vmem = pltpu.VMEM
    z, x, y, c = red.z, red.x, red.y, red.c
    tokens = count * tok_dev
    scratch = red.scratch(2 * slice_dev)
    scratch.update(
        left=vmem((2 * tokens, 2 * slice_dev), bf16),
        scale=vmem((tok_dev, LANES), f32),
        scales=vmem((tp_count, tok_dev, LANES), f32),
        tokall=vmem(tok.shape, bf16),
        packall=vmem((rep_count,) + packed.shape, bf16),
        par=vmem((packed.shape[0], inner_dev), f32),
        stepall=vmem((rep_count, tp_count, step_proj.shape[0], inner_dev), bf16),
        sel=vmem((LANES, inner_dev), bf16),
        router=vmem((slice_dev, LANES), f32),
        maps=vmem((experts, tokens, count * CAPACITY), bf16),
        gate=vmem((req, inner_dev), f32),
        act=vmem((req, inner_dev), f32),
        actall=vmem((rep_count, req, inner_dev), bf16),
        part=vmem((rep_count, req, LANES), bf16),
        parts=vmem((count, req, LANES), bf16),
        bc=vmem((LANES, LANES), f32),
        step=vmem((req, inner_dev), f32),
        read=vmem((req, inner_dev), f32),
        state=vmem(state.shape, f32),
        outw=vmem(out_w.shape, bf16),
        gall=vmem((y, c, z, x, req, inner_dev), bf16),
        toks=dma((2,)),
        idss=dma((2,)),
        pts=dma((2,)),
        scs=dma((2, tp_count - 1)),
        sts=dma((2, tp_count - 1)),
        pks=dma((2, rep_count)),
        own=dma((4,)),
        txs=dma((2, z)),
        tzs=dma((2, 2 * (z - 1))),
        acs=dma((2, n, rep_count - 1)),
        gzs=dma((2, CORES, z - 1)),
        gxs=dma((2, CORES, x * y - 1)),
        gcs=dma((2, CORES)),
    )
    shape = jax.ShapeDtypeStruct
    anywhere = pl.BlockSpec(memory_space=pl.ANY)
    return pl.pallas_call(
        functools.partial(mixer_kernel, red, tuple(scratch), experts),
        out_shape=[
            shape(history.shape, bf16),
            shape(state.shape, f32),
            shape(tok.shape, bf16),
            shape((rep_count, req, LANES), f32),
            shape((experts, count * CAPACITY, slice_dev), bf16),
            shape((count,) + ids.shape, bf16),
        ],
        in_specs=in_vmem(7) + [anywhere] * 4,
        out_specs=in_vmem(1) + [anywhere] + in_vmem(4),
        scratch_shapes=list(scratch.values()),
        compiler_params=pltpu.CompilerParams(
            collective_id=0, has_side_effects=True, vmem_limit_bytes=62 * 2**20
        ),
        name="mixer",
    )(*args)


def last_kernel(
    red, names, begin, extra, experts_all, width, x_ref, home_ref, stat_ref, ids_ref, w_ref, hid_ref, *refs
):
    outs = 1 if extra else 0
    s = dict(zip(names, refs[outs:]))
    red.place()
    tp_count, rep_count = red.y * red.c, red.z * red.x
    count = tp_count * rep_count
    rep, tp = red.rep, red.tp
    me = rep * tp_count + tp
    wide = 2 * red.half
    for i in range(red.chunks):
        expert, column = divmod(begin + i, red.per)
        red.fetch(
            s, w_ref, i, column * wide, lambda w, at, expert=expert: w.at[:, expert, :, at]
        )
    for expert in range(x_ref.shape[0]):
        s["left"][expert] = spread(x_ref[expert], red.rows // 2, 2)
    if extra:
        homes_ref = refs[0]
    greet_all(count, me, tp_count)

    def left_of(i):
        return s["left"][lax.div(begin + i, red.per)]

    req = red.rows // 2
    stats_ref = s["stats"]
    tok_dev = home_ref.shape[1]
    experts = x_ref.shape[0]

    def gates():
        for which in range(2):
            scatter_wait(stats_ref, s["sas"], which, count)
        summed = stats_ref[0]
        for k in range(1, count):
            summed += stats_ref[k]
        tokens = tp_count * tok_dev
        ids = ids_ref[pl.ds(pl.multiple_of(rep * tokens, 8), tokens)]
        lane = lax.broadcasted_iota(jnp.int32, (tokens, LANES), 1)
        first, second = named(ids, lane)
        scale = lax.rsqrt(summed[:, experts_all : experts_all + 1] / width + epsilon)
        logits = summed * scale
        one = jnp.sum(jnp.where(first, logits, 0.0), axis=1, keepdims=True)
        two = jnp.sum(jnp.where(second, logits, 0.0), axis=1, keepdims=True)
        gate = jnp.where(first, 1.0 / (1.0 + jnp.exp(two - one)), 0.0)
        gate += jnp.where(second, 1.0 / (1.0 + jnp.exp(one - two)), 0.0)
        gate = jnp.where(lane == LANES - 1, scale, gate)
        for e, taken in enumerate(slot_maps(ids, experts, tok_dev)):
            row = lax.dot_general(
                taken, gate, (((0,), (0,)), ((), ())), preferred_element_type=jnp.float32,
                precision=lax.Precision.HIGHEST,
            )
            seat = row[:, e : e + 1].astype(jnp.bfloat16).astype(jnp.float32)
            s["seat"][e] = jnp.broadcast_to(seat, s["seat"].shape[1:])
            s["size"][e] = jnp.broadcast_to(row[:, LANES - 1 :], s["size"].shape[1:])

    def store(i, h, total):
        expert = lax.div(begin + i, red.per)
        column = lax.rem(begin + i, red.per) * wide + h * red.half
        size = s["size"][expert][:, :1]
        up = total[req:] * size
        hidden = s["seat"][expert][:, :1] * silu(total[:req] * size) * up
        at = pl.ds(pl.multiple_of(column, LANES), red.half)
        hid_ref[expert, :, at] = hidden.astype(jnp.bfloat16)

    def send_home():
        scatter_start(home_ref, homes_ref, s["hos"], count, me, tp_count)
        homes_ref[me] = home_ref[me]

    def send_stats():

        def one(step, _):
            to = lax.rem(me + step, count)
            pltpu.make_async_remote_copy(
                src_ref=stat_ref.at[lax.div(to, tp_count)],
                dst_ref=stats_ref.at[me],
                send_sem=s["sas"].at[0],
                recv_sem=s["sas"].at[1],
                device_id=device_of(to, tp_count),
                device_id_type=MESH,
            ).start()
            return 0

        lax.fori_loop(1, count, one, 0)
        stats_ref[me] = stat_ref[rep]

    lags = (1, 3, 5, 7)
    extras = [(0, send_stats), (lags[3] - 1, gates)]
    if extra:
        extras.append((2, send_home))
    red.run(s, left_of, store, lags, extras)
    if extra:
        for which in range(2):
            scatter_wait(homes_ref, s["hos"], which, count)


def last_stage(slots, home, stat, ids, w, experts_all, width, rep_count, tp_count, hidden_dev):
    f32, bf16 = jnp.float32, jnp.bfloat16
    experts, total_rows, slice_dev = slots.shape
    rows = 2 * total_rows // rep_count
    shape = jax.ShapeDtypeStruct
    dma = pltpu.SemaphoreType.DMA
    full = Reduce(rep_count, tp_count, rows, hidden_dev, 0)
    total = full.per * experts
    weights = w.size // experts // full.per * experts * 2 // experts
    most = max(1, ROOM // (full.chunk_bytes() + weights))
    begin, ups = 0, None
    while begin < total:
        red = Reduce(rep_count, tp_count, rows, hidden_dev, min(most, total - begin))
        extra = begin == 0
        scratch = red.scratch(2 * slice_dev)
        scratch["left"] = pltpu.VMEM((experts, rep_count * rows, 2 * slice_dev), bf16)
        scratch["sas"] = dma((2,))
        scratch["stats"] = pltpu.VMEM((rep_count * tp_count,) + stat.shape[1:], f32)
        scratch["seat"] = pltpu.VMEM((experts, rows // 2, LANES), f32)
        scratch["size"] = pltpu.VMEM((experts, rows // 2, LANES), f32)
        outs = [shape((experts, rows // 2, hidden_dev), bf16)]
        if extra:
            scratch["hos"] = dma((2,))
            outs += [shape(home.shape, bf16)]
        got = pl.pallas_call(
            functools.partial(last_kernel, red, tuple(scratch), begin, extra, experts_all, width),
            out_shape=outs,
            in_specs=in_vmem(4) + [pl.BlockSpec(memory_space=pl.ANY)],
            out_specs=in_vmem(len(outs)),
            scratch_shapes=list(scratch.values()),
            compiler_params=pltpu.CompilerParams(
                collective_id=10 + begin, has_side_effects=True, vmem_limit_bytes=62 * 2**20
            ),
            name="last_stage",
        )(slots, home, stat, ids, w)
        if extra:
            ups, homes = got
        else:
            edge = begin // full.per
            column = (begin % full.per) * 2 * full.half
            at = lax.broadcasted_iota(jnp.int32, (experts, 1, hidden_dev), 2)
            order = lax.broadcasted_iota(jnp.int32, (experts, 1, hidden_dev), 0)
            older = (order < edge) | ((order == edge) & (at < column))
            ups = jnp.where(older, ups, got[0])
        begin += red.chunks
    return ups, homes


def shards(
    tokens,
    conv_state,
    ssm_state,
    norm_gains,
    conv_weight,
    conv_skip,
    step_bias,
    decay_log,
    input_proj,
    select_proj,
    step_proj,
    output_proj,
    router,
    expert_proj,
    expert_ids,
):
    bf16 = jnp.bfloat16
    tp_count = lax.axis_size("tp")
    rep_count = lax.axis_size("rep")
    count = tp_count * rep_count
    tok_dev, width = tokens.shape
    slice_dev = width // count
    experts = expert_proj.shape[1]
    hidden_dev = expert_proj.shape[3] // tp_count

    pieces = tokens.reshape(tok_dev, count, slice_dev).transpose(1, 0, 2)
    ids = jnp.pad(expert_ids.astype(bf16), ((0, 0), (0, LANES - 2)))
    packed = jnp.concatenate([conv_weight, conv_skip, step_bias[None], decay_log], axis=0)
    packed = jnp.pad(packed, ((0, -packed.shape[0] % 16), (0, 0)))
    args = (
        pieces, ids, norm_gains, packed, select_proj.T, conv_state, router,
        step_proj, input_proj, ssm_state, output_proj,
    )
    conv_next, ssm_next, home, stat, slots, ids = mixer(args, rep_count, tp_count, experts)
    hidden, home = last_stage(
        slots, home, stat, ids.reshape(count * tok_dev, LANES), expert_proj,
        router.shape[1], width, rep_count, tp_count, hidden_dev,
    )
    mamba_out = home.transpose(1, 0, 2).reshape(tok_dev, width)
    hidden = hidden.reshape(experts, tp_count, CAPACITY, hidden_dev).transpose(1, 0, 2, 3)
    expert_hidden = hidden.reshape(experts * tp_count * CAPACITY, hidden_dev)
    return (mamba_out, conv_next, ssm_next, expert_hidden)


def solution(mesh):
    in_specs = (
        P(("rep", "tp"), None),
        P(None, "rep", "tp"),
        P("rep", None, "tp"),
        P(None, ("rep", "tp")),
        P(None, ("rep", "tp")),
        P(None, ("rep", "tp")),
        P(("rep", "tp")),
        P(None, ("rep", "tp")),
        P(("rep", "tp"), None, None),
        P("tp", "rep"),
        P(("rep", "tp"), None),
        P(None, ("rep", "tp")),
        P(("rep", "tp"), None),
        P(("rep", "tp"), None, None, None),
        P(("rep", "tp"), None),
    )
    out_specs = (P(("rep", "tp"), None), P(None, "rep", "tp"), P("rep", None, "tp"), P("rep", "tp"))
    return jax.shard_map(shards, mesh=mesh, in_specs=in_specs, out_specs=out_specs, check_vma=False)
```

```python
import functools

import jax
import jax.numpy as jnp
from jax import lax
from jax.experimental import pallas as pl
from jax.experimental.pallas import tpu as pltpu
from jax.sharding import PartitionSpec as P

CAPACITY = 2
LANES = 128


epsilon = 1e-05
MESH = pl.DeviceIdType.MESH


CORES = 2
LANE_PAIR = 2
ROOM = 40 * 2**20


def split_of(rep_count, tp_count):
    return rep_count // CORES, CORES, tp_count // CORES, CORES


def start_all(copies):
    for copy in copies:
        copy.start()


class Reduce:
    def __init__(self, rep_count, tp_count, rows, dev_cols, total_chunks):
        self.z, self.x, self.y, self.c = split_of(rep_count, tp_count)
        self.rows = rows
        self.half = 2 * LANES if dev_cols % (4 * LANES) == 0 else LANES
        self.per = dev_cols // (2 * self.half)
        self.dev_cols = dev_cols
        self.chunks = total_chunks
        self.blocks = self.z * self.x * self.y

    def chunk_bytes(self):
        return self.c * 2 * self.blocks * self.rows * self.half * 2 * 2

    def scratch(self, depth):
        n, z, x, y, rows, half = self.chunks, self.z, self.x, self.y, self.rows, self.half
        bf16 = jnp.bfloat16
        groups = self.c * y * 2 * (half // LANES)
        dma = pltpu.SemaphoreType.DMA
        buffers = dict(
            w=pltpu.VMEM((n, groups, depth // 2, 2, LANES), bf16),
            b0=pltpu.VMEM((n, self.c, 2, self.blocks, rows, half), bf16),
            r0=pltpu.VMEM((n, 2, self.blocks, rows, half), bf16),
            r1a=pltpu.VMEM((n, y - 1, x * z, rows, half), bf16),
            r1b=pltpu.VMEM((n, x - 1, y * z, rows, half), bf16),
            r2a=pltpu.VMEM((n, x - 1, z, rows, half), bf16),
            r2b=pltpu.VMEM((n, y - 1, z, rows, half), bf16),
            b3=pltpu.VMEM((n, z, 2, rows, half), bf16),
            r3=pltpu.VMEM((n, z - 1, 2, rows, half), bf16),
            ws=dma((n,)),
            s0=dma((2, n)),
            s1a=dma((2, n, y - 1)),
            s1b=dma((2, n, x - 1)),
            s2a=dma((2, n, x - 1)),
            s2b=dma((2, n, y - 1)),
            s3=dma((2, n, z - 1)),
        )
        return buffers

    def place(self):
        rep, tp = lax.axis_index("rep"), lax.axis_index("tp")
        self.rep, self.tp = rep, tp
        self.mz, self.mx = lax.div(rep, self.x), lax.rem(rep, self.x)
        self.my, self.mc = lax.div(tp, self.c), lax.rem(tp, self.c)

    def peer_z(self, to):
        return {"rep": to * self.x + self.mx}

    def peer_x(self, to):
        return {"rep": self.mz * self.x + to}

    def peer_y(self, to):
        return {"tp": to * self.c + self.mc}

    def peer_c(self):
        return {"tp": self.my * self.c + 1 - self.mc}

    def peers(self):
        out = [self.peer_c()]
        out += [self.peer_y(lax.rem(self.my + s, self.y)) for s in range(1, self.y)]
        out += [self.peer_x(lax.rem(self.mx + s, self.x)) for s in range(1, self.x)]
        out += [self.peer_z(lax.rem(self.mz + s, self.z)) for s in range(1, self.z)]
        return out

    def exchange(self, source, count, me, size, target, sems, i, peer):
        copies = []
        for step in range(1, count):
            to = lax.rem(me + step, count)
            copies.append(
                pltpu.make_async_remote_copy(
                    src_ref=source.at[pl.ds(to * size, size)],
                    dst_ref=target.at[i, step - 1],
                    send_sem=sems.at[0, i, step - 1],
                    recv_sem=sems.at[1, i, step - 1],
                    device_id=peer(to),
                    device_id_type=MESH,
                )
            )
        return copies

    def copies(self, s, i, stage):
        z, x, y = self.z, self.x, self.y
        if stage == 0:
            return [
                pltpu.make_async_remote_copy(
                    src_ref=s["b0"].at[i, 1 - self.mc],
                    dst_ref=s["r0"].at[i],
                    send_sem=s["s0"].at[0, i],
                    recv_sem=s["s0"].at[1, i],
                    device_id=self.peer_c(),
                    device_id_type=MESH,
                )
            ]
        if stage == 1:
            return self.exchange(
                s["r0"].at[i, 0], y, self.my, x * z, s["r1a"], s["s1a"], i, self.peer_y
            ) + self.exchange(
                s["r0"].at[i, 1], x, self.mx, y * z, s["r1b"], s["s1b"], i, self.peer_x
            )
        if stage == 2:
            return self.exchange(
                s["r1a"].at[i, 0], x, self.mx, z, s["r2a"], s["s2a"], i, self.peer_x
            ) + self.exchange(
                s["r1b"].at[i, 0], y, self.my, z, s["r2b"], s["s2b"], i, self.peer_y
            )
        third = []
        for step in range(1, z):
            to = lax.rem(self.mz + step, z)
            third.append(
                pltpu.make_async_remote_copy(
                    src_ref=s["b3"].at[i, to],
                    dst_ref=s["r3"].at[i, step - 1],
                    send_sem=s["s3"].at[0, i, step - 1],
                    recv_sem=s["s3"].at[1, i, step - 1],
                    device_id=self.peer_z(to),
                    device_id_type=MESH,
                )
            )
        return third

    def fetch(self, s, w_ref, i, column, pick):
        wide = 2 * self.half
        for y in range(self.y):
            for c in range(self.c):
                for k in range(wide // LANES):
                    at = (y * self.c + c) * self.dev_cols + column + k * LANES
                    at = pl.ds(pl.multiple_of(at, LANES), LANES)
                    pltpu.make_async_copy(
                        pick(w_ref, at),
                        s["w"].at[i, (y * self.c + c) * (wide // LANES) + k],
                        s["ws"].at[i],
                    ).start()

    def multiply(self, s, i, left):
        w = s["w"]
        pltpu.make_async_copy(w.at[i], w.at[i], s["ws"].at[i]).wait()
        depth = w.shape[2] * 2
        pieces = self.half // LANES
        for y in range(self.y):
            for c in range(self.c):
                for h in range(2):
                    first = ((y * self.c + c) * 2 + h) * pieces
                    right = [
                        w.at[i, first + k].reshape(depth, LANES)[...] for k in range(pieces)
                    ]
                    right = jnp.concatenate(right, axis=1) if pieces > 1 else right[0]
                    got = jnp.dot(left, right, preferred_element_type=jnp.float32)
                    got = got.astype(jnp.bfloat16)
                    got = got.reshape(self.z, self.x, self.rows, self.half)
                    for x in range(self.x):
                        at = (y * self.x + x) if h == 0 else (x * self.y + y)
                        s["b0"][i, c, h, at * self.z : (at + 1) * self.z] = got[:, x]
        start_all(self.copies(s, i, 0))

    def add(self, target, others):
        def piece(k, _):
            total = target[k].astype(jnp.float32)
            for other in others:
                total += other[k].astype(jnp.float32)
            target[k] = total.astype(jnp.bfloat16)
            return 0

        lax.fori_loop(0, target.shape[0], piece, 0, unroll=min(4, target.shape[0]))

    def after_core(self, s, i):
        for copy in self.copies(s, i, 0):
            copy.wait_recv()
        for h in range(2):
            self.add(s["r0"].at[i, h], [s["b0"].at[i, self.mc, h]])
        start_all(self.copies(s, i, 1))

    def after_first(self, s, i):
        for copy in self.copies(s, i, 1):
            copy.wait_recv()
        z = self.z
        for h, name, me, size, count in (
            (0, "r1a", self.my, self.x * z, self.y),
            (1, "r1b", self.mx, self.y * z, self.x),
        ):
            others = [s[name].at[i, k] for k in range(1, count - 1)]
            others.append(s["r0"].at[i, h, pl.ds(me * size, size)])
            self.add(s[name].at[i, 0], others)
        start_all(self.copies(s, i, 2))

    def after_second(self, s, i):
        for copy in self.copies(s, i, 2):
            copy.wait_recv()
        for h, name, came, me, count in (
            (0, "r2a", "r1a", self.mx, self.x),
            (1, "r2b", "r1b", self.my, self.y),
        ):
            for k in range(self.z):
                total = s[came][i, 0, me * self.z + k].astype(jnp.float32)
                for j in range(count - 1):
                    total += s[name][i, j, k].astype(jnp.float32)
                s["b3"][i, k, h] = total.astype(jnp.bfloat16)
        start_all(self.copies(s, i, 3))

    def after_third(self, s, i, store, done):
        for copy in self.copies(s, i, 3):
            copy.wait_recv()
        for h in range(2):
            total = s["b3"][i, self.mz, h].astype(jnp.float32)
            for k in range(self.z - 1):
                total += s["r3"][i, k, h].astype(jnp.float32)
            store(i, h, total)
        done(i)

    def finish(self, s):
        def one(i, _):
            for stage in range(4):
                for copy in self.copies(s, i, stage):
                    copy.wait_send()
            return 0

        lax.fori_loop(0, self.chunks, one, 0)

    def run(self, s, left_of, store, lags, extras=(), done=lambda i: None):
        n = self.chunks
        stages = (
            (lags[3], lambda i: self.after_third(s, i, store, done)),
            (lags[2], lambda i: self.after_second(s, i)),
            (lags[1], lambda i: self.after_first(s, i)),
            (lags[0], lambda i: self.after_core(s, i)),
            (0, lambda i: self.multiply(s, i, left_of(i))),
        )

        def step(t, _):
            for lag, work in stages:
                @pl.when((t >= lag) & (t < n + lag))
                def _(lag=lag, work=work):
                    work(t - lag)
            for when, work in extras:
                pl.when(t == when)(work)
            return 0

        lax.fori_loop(0, n + lags[3], step, 0)
        self.finish(s)


def spread(rows, per, pairs):
    count, depth = rows.shape
    lane = lax.broadcasted_iota(jnp.int32, (depth, depth * pairs), 1)
    source = lax.broadcasted_iota(jnp.int32, (depth, depth * pairs), 0)
    parts = []
    for j in range(pairs):
        moves = (lane == source * pairs + j).astype(jnp.bfloat16)
        part = jnp.dot(rows, moves, preferred_element_type=jnp.float32)
        parts.append(part.reshape(count // per, 1, per, depth * pairs))
    wide = jnp.concatenate(parts, axis=1)
    return wide.reshape(count * pairs, depth * pairs).astype(jnp.bfloat16)


def greet(ids):
    barrier = pltpu.get_barrier_semaphore()
    for device in ids:
        pl.semaphore_signal(barrier, inc=1, device_id=device, device_id_type=MESH)
    pl.semaphore_wait(barrier, len(ids))


def device_of(index, tp_count):
    return {"rep": lax.div(index, tp_count), "tp": lax.rem(index, tp_count)}


def greet_all(count, me, tp_count):
    barrier = pltpu.get_barrier_semaphore()

    def one(step, _):
        to = device_of(lax.rem(me + step, count), tp_count)
        pl.semaphore_signal(barrier, inc=1, device_id=to, device_id_type=MESH)
        return 0

    lax.fori_loop(1, count, one, 0)
    pl.semaphore_wait(barrier, count - 1)


def scatter_start(source, target, sems, count, me, tp_count):
    whole = len(source.shape) == len(target.shape) - 1

    def one(step, _):
        to = lax.rem(me + step, count)
        pltpu.make_async_remote_copy(
            src_ref=source if whole else source.at[to],
            dst_ref=target.at[me],
            send_sem=sems.at[0],
            recv_sem=sems.at[1],
            device_id=device_of(to, tp_count),
            device_id_type=MESH,
        ).start()
        return 0

    lax.fori_loop(1, count, one, 0)


def scatter_wait(target, sems, which, count):
    part = target.at[pl.ds(0, count - 1)]
    pltpu.make_async_copy(part, part, sems.at[which]).wait()


def in_vmem(count):
    return [pl.BlockSpec(memory_space=pltpu.VMEM)] * count


def remote(source, target, send_sem, recv_sem, device):
    return pltpu.make_async_remote_copy(
        src_ref=source,
        dst_ref=target,
        send_sem=send_sem,
        recv_sem=recv_sem,
        device_id=device,
        device_id_type=MESH,
    )


def silu(v):
    return v / (1.0 + jnp.exp(-v))


def softplus(v):
    return jnp.maximum(v, 0.0) + jnp.log1p(jnp.exp(-jnp.abs(v)))


def column_iota(shape, axis):
    return lax.broadcasted_iota(jnp.int32, shape, axis)


def named(ids, lane):
    ids = ids.astype(jnp.float32).astype(jnp.int32)
    return ids[:, :1] == lane, ids[:, 1:2] == lane


def slot_maps(ids, experts, tok_dev):
    rows = ids.shape[0]
    first, second = named(ids, column_iota((rows, LANES), 1))
    routed = (first | second).astype(jnp.float32)
    later, earlier = column_iota((rows, rows), 0), column_iota((rows, rows), 1)
    before = (earlier < later) & (lax.div(earlier, tok_dev) == lax.div(later, tok_dev))
    position = jnp.dot(
        before.astype(jnp.bfloat16), routed.astype(jnp.bfloat16), preferred_element_type=jnp.float32
    )
    slots = rows // tok_dev * CAPACITY
    row, slot = column_iota((rows, slots), 0), column_iota((rows, slots), 1)
    block = lax.div(row, tok_dev) == lax.div(slot, CAPACITY)
    seat = lax.rem(slot, CAPACITY).astype(jnp.float32)
    maps = []
    for e in range(experts):
        taken = block & (routed[:, e : e + 1] > 0.5) & (position[:, e : e + 1] == seat)
        maps.append(taken.astype(jnp.float32))
    return maps


def mixer_kernel(
    red, names, experts,
    tok_in_ref, ids_in_ref, gains_ref, weight_ref, skip_ref, bias_ref, decay_ref, sel_ref,
    history_ref, router_ref,
    step_ref, w_ref, state_ref, out_w_ref,
    next_ref, state_out_ref, home_ref, stat_ref, slots_ref, idsall_ref, *scratch
):
    f32, bf16 = jnp.float32, jnp.bfloat16
    s = dict(zip(names, scratch))
    red.place()
    z, x, y, c = red.z, red.x, red.y, red.c
    mz, mx, my, mc = red.mz, red.mx, red.my, red.mc
    tp_count, rep_count = y * c, z * x
    count = tp_count * rep_count
    rep, tp = red.rep, red.tp
    me = rep * tp_count + tp
    inner_dev = red.dev_cols
    req = red.rows // 2
    tok_ref, ids_ref, packed_ref = s["tok"], s["ids"], s["packed"]
    tok_dev, slice_dev = tok_ref.shape[1:]
    tokall, packall, stepall = s["tokall"], s["packall"], s["stepall"]
    taps = history_ref.shape[0] + 1
    states = tap0 = state_ref.shape[1]

    state_in = pltpu.make_async_copy(state_ref, s["state"], s["own"].at[1])
    out_in = pltpu.make_async_copy(out_w_ref, s["outw"], s["own"].at[2])
    for i in range(red.chunks):
        red.fetch(s, w_ref, i, i * 2 * red.half, lambda w, at: w.at[:, :, at])
    columns = pl.ds(pl.multiple_of(tp * inner_dev, LANES), inner_dev)
    own_step = pltpu.make_async_copy(step_ref.at[:, columns], stepall.at[rep, tp], s["own"].at[0])
    own_step.start()
    state_in.start()
    out_in.start()
    for k in range(count):
        tok_ref[k] = tok_in_ref[:, k * slice_dev : (k + 1) * slice_dev]
    ids = ids_in_ref[...].astype(f32)
    ids = jnp.concatenate([ids, jnp.zeros((tok_dev, LANES - ids.shape[1]), f32)], axis=1)
    ids_ref[...] = ids.astype(bf16)
    rows = [ref[...].astype(f32) for ref in (decay_ref, weight_ref, skip_ref, bias_ref)]
    spare = packed_ref.shape[0] - sum(row.shape[0] for row in rows)
    rows.append(jnp.zeros((spare, packed_ref.shape[1]), f32))
    packed_ref[...] = jnp.concatenate(rows, axis=0).astype(bf16)
    tok = tok_in_ref[...].astype(f32)
    width = tok.shape[1]
    square = jnp.sum(tok * tok, axis=-1, keepdims=True)
    s["scale"][...] = jnp.broadcast_to(lax.rsqrt(square / width + epsilon), s["scale"].shape)
    greet_all(count, me, tp_count)
    scatter_start(tok_ref, tokall, s["toks"], count, me, tp_count)
    tokall[me] = tok_ref[me]
    slot = lax.rem(me, rep_count)
    home_tp = lax.div(me, rep_count)

    def pack_copy(to_rep):
        return remote(
            packed_ref, packall.at[slot], s["pks"].at[0, to_rep], s["pks"].at[1, slot],
            {"rep": to_rep, "tp": home_tp},
        )

    def is_me(to_rep):
        return (to_rep == rep) & (home_tp == tp)

    def pack_start(to_rep, _):
        @pl.when(is_me(to_rep))
        def _():
            packall[slot] = packed_ref[...]

        @pl.when(jnp.logical_not(is_me(to_rep)))
        def _():
            pack_copy(to_rep).start()

        return 0

    lax.fori_loop(0, rep_count, pack_start, 0)
    scale_copies, step_copies = [], []
    for k in range(tp_count - 1):
        to = lax.rem(tp + k + 1, tp_count)
        scale_copies.append(
            remote(
                s["scale"], s["scales"].at[tp], s["scs"].at[0, k], s["scs"].at[1, k], {"tp": to}
            )
        )
        columns = pl.ds(pl.multiple_of(to * inner_dev, LANES), inner_dev)
        step_copies.append(
            remote(
                step_ref.at[:, columns], stepall.at[rep, tp],
                s["sts"].at[0, k], s["sts"].at[1, k], {"tp": to},
            )
        )
    start_all(scale_copies)
    s["scales"][tp] = s["scale"][...]
    start_all(step_copies)
    scatter_start(ids_ref, idsall_ref, s["idss"], count, me, tp_count)
    idsall_ref[me] = ids_ref[...]
    to_x = {"rep": mz * x + lax.rem(mx + 1, x)}

    def step_z(k):
        block = stepall.at[rep]
        return remote(
            block, block, s["tzs"].at[0, k], s["tzs"].at[1, k], red.peer_z(lax.rem(mz + k + 1, z))
        )

    def step_x(source_z):
        block = stepall.at[source_z * x + mx]
        return remote(block, block, s["txs"].at[0, source_z], s["txs"].at[1, source_z], to_x)

    s["sel"][...] = jnp.zeros(s["sel"].shape, bf16)
    part_cols = sel_ref.shape[0]
    s["sel"][:part_cols] = sel_ref[...]
    s["router"][...] = jnp.zeros(s["router"].shape, f32)
    s["router"][: router_ref.shape[0]] = router_ref[...].astype(f32)
    next_ref[: taps - 2] = history_ref[1:]

    scatter_wait(tokall, s["toks"], 1, count)
    tok_all = tokall.reshape(count * tok_dev, slice_dev)
    gain = gains_ref[...].astype(f32)
    x_rows = (tok_all[...].astype(f32) * gain[:1]).astype(bf16)
    s["left"][...] = spread(x_rows, req, 2)

    def step_first():
        own_step.wait()
        for copy in step_copies:
            copy.wait_recv()
        for k in range(z - 1):
            step_z(k).start()

    def step_second():
        for k in range(z - 1):
            step_z(k).wait_recv()
        for k in range(z // 2):
            step_x(k).start()

    def params():
        for copy in scale_copies:
            copy.wait_recv()

        def pack_came(k, _):
            @pl.when(tp * rep_count + k != me)
            def _():
                pltpu.make_async_copy(packall.at[k], packall.at[k], s["pks"].at[1, k]).wait()

            return 0

        lax.fori_loop(0, rep_count, pack_came, 0)
        own = packed_ref.shape[1]
        for k in range(rep_count):
            s["par"][:, k * own : (k + 1) * own] = packall[k].astype(f32)

    def maps():
        scatter_wait(idsall_ref, s["idss"], 1, count)
        ids = idsall_ref.reshape(count * tok_dev, LANES)[...]
        for e, taken in enumerate(slot_maps(ids, experts, tok_dev)):
            s["maps"][e] = taken.astype(bf16)

    def store(i, h, total):
        at = pl.ds(pl.multiple_of(i * 2 * red.half + h * red.half, LANES), red.half)
        scale = s["scales"].reshape(req, LANES)[:, :1]
        conv_input = total[:req] * scale
        s["gate"][:, at] = total[req:] * scale
        next_ref[taps - 2, :, at] = conv_input.astype(bf16)
        par = s["par"]
        mix = par[tap0 + taps - 1 : tap0 + taps, at] * conv_input
        mix += par[tap0 + taps : tap0 + taps + 1, at]
        for k in range(taps - 1):
            mix += par[tap0 + k : tap0 + k + 1, at] * history_ref[k, :, at].astype(f32)
        act = silu(mix)
        s["act"][:, at] = act
        s["actall"][rep, :, at] = act.astype(bf16)

    def act_copies(i):
        at = pl.ds(pl.multiple_of(i * 2 * red.half, LANES), 2 * red.half)
        block = s["actall"].at[rep, :, at]
        return [
            remote(
                block, block, s["acs"].at[0, i, k], s["acs"].at[1, i, k],
                {"rep": lax.rem(rep + k + 1, rep_count)},
            )
            for k in range(rep_count - 1)
        ]

    n = red.chunks
    lags = (1, n, n + 2, n + 4)
    extras = [(1, step_first), (2, params), (2, maps), (2 * n + 1, step_second)]
    red.run(
        s, lambda i: s["left"][...], store, lags, extras, lambda i: start_all(act_copies(i))
    )
    for k in range(z // 2, z):
        step_x(k).start()

    def act_came(i, _):
        for copy in act_copies(i):
            copy.wait_recv()
        return 0

    lax.fori_loop(0, red.chunks, act_came, 0)
    every = s["actall"].reshape(rep_count * req, inner_dev)[...]
    part = lax.dot_general(
        every, s["sel"][...], (((1,), (1,)), ((), ())), preferred_element_type=f32
    )
    s["part"][...] = part.astype(bf16).reshape(rep_count, req, LANES)

    def part_start(step, _):
        to = lax.rem(me + step, count)
        remote(
            s["part"].at[lax.div(to, tp_count)], s["parts"].at[me],
            s["pts"].at[0], s["pts"].at[1], device_of(to, tp_count),
        ).start()
        return 0

    lax.fori_loop(1, count, part_start, 0)
    s["parts"][me] = s["part"][rep]
    scatter_wait(s["parts"], s["pts"], 1, count)
    total_cols = part_cols * rep_count
    tiles = [jnp.zeros((req, LANES), f32) for _ in range(-(-total_cols // LANES))]
    lane = column_iota((req, LANES), 1)
    for r in range(rep_count):
        cols = s["parts"][r * tp_count].astype(f32)
        for p in range(1, tp_count):
            cols += s["parts"][r * tp_count + p].astype(f32)
        tile, shift = divmod(r * part_cols, LANES)
        if shift:
            cols = pltpu.roll(cols, shift, 1)
        tiles[tile] += jnp.where(lane >= shift, cols, 0.0)
        if shift + part_cols > LANES:
            tiles[tile + 1] += jnp.where(lane < shift + part_cols - LANES, cols, 0.0)
    rank = total_cols - 2 * states
    low_tiles = rank // LANES
    low = jnp.concatenate(tiles[:low_tiles], axis=1).astype(bf16)
    both_maps = jnp.concatenate(
        [tiles[low_tiles], jnp.zeros((LANES - req, LANES), f32)], axis=0
    ).T
    s["bc"][...] = both_maps
    for k in range(z):
        step_x(k).wait_recv()
    if step_ref.shape[0] % 8 == 0:
        step_rows = stepall.reshape(rank, inner_dev)[...]
    else:
        step_rows = stepall[...].reshape(rank, inner_dev)
    step_pre = jnp.dot(low, step_rows, preferred_element_type=f32)
    s["step"][...] = softplus(step_pre + s["par"][tap0 + taps + 2 : tap0 + taps + 3])
    state_in.wait()
    wide = 2 * LANES
    ways = CORES
    piece = inner_dev // ways
    gall = s["gall"]

    def scan_block(b, _):
        at = pl.ds(pl.multiple_of(b * wide, LANES), wide)
        decay = -jnp.exp(s["par"][:states, at])
        step, act = s["step"][:, at], s["act"][:, at]
        for t in range(req):
            row = step[t : t + 1]
            now = jnp.exp(row * decay) * s["state"][t, :, at]
            now += (row * act[t : t + 1]) * s["bc"][:states, t : t + 1]
            s["state"][t, :, at] = now
            s["read"][t : t + 1, at] = jnp.sum(
                now * s["bc"][states : 2 * states, t : t + 1], axis=0, keepdims=True
            )
        read = s["read"][:, at] + s["par"][tap0 + taps + 1 : tap0 + taps + 2, at] * act
        gall[my, mc, mz, mx, :, at] = (read * silu(s["gate"][:, at])).astype(bf16)
        return 0

    def along_z(h):
        at = pl.ds(h * piece, piece)
        block = gall.at[my, mc, mz, mx, :, at]
        return [
            remote(
                block, block, s["gzs"].at[0, h, k], s["gzs"].at[1, h, k],
                red.peer_z(lax.rem(mz + k + 1, z)),
            )
            for k in range(z - 1)
        ]

    def along_xy(h):
        at = pl.ds(h * piece, piece)
        block = gall.at[my, mc, :, mx, :, at]
        out = []
        for k in range(1, x * y):
            dx, dy = k % x, k // x
            device = {
                "rep": mz * x + lax.rem(mx + dx, x),
                "tp": lax.rem(my + dy, y) * c + mc,
            }
            out.append(
                remote(block, block, s["gxs"].at[0, h, k - 1], s["gxs"].at[1, h, k - 1], device)
            )
        return out

    def along_core(h):
        block = gall.at[:, mc, :, :, :, pl.ds(h * piece, piece)]
        return remote(block, block, s["gcs"].at[0, h], s["gcs"].at[1, h], red.peer_c())

    blocks = piece // wide
    for h in range(ways):
        lax.fori_loop(h * blocks, (h + 1) * blocks, scan_block, 0)
        start_all(along_z(h))
    state_out = pltpu.make_async_copy(s["state"], state_out_ref, s["own"].at[3])
    state_out.start()
    for h in range(ways):
        for copy in along_z(h):
            copy.wait_recv()
        start_all(along_xy(h))
    for h in range(ways):
        for copy in along_xy(h):
            copy.wait_recv()
        along_core(h).start()
    out_in.wait()

    def product(core):
        total = jnp.zeros((rep_count * req, slice_dev), f32)
        for k in range(y):
            rows = gall.at[k, core].reshape(rep_count * req, inner_dev)[...]
            at = pl.multiple_of((k * c + core) * inner_dev, LANES)
            total += jnp.dot(rows, s["outw"][pl.ds(at, inner_dev)], preferred_element_type=f32)
        return total

    mixed = product(mc)
    for h in range(ways):
        along_core(h).wait_recv()
    residual = tok_all[...].astype(f32) + mixed + product(1 - mc)
    home_ref.reshape(count * tok_dev, slice_dev)[...] = residual.astype(bf16)
    gained = residual * gain[1:2]
    stat = lax.dot_general(
        gained, s["router"][...], (((1,), (1,)), ((), ())), preferred_element_type=f32,
        precision=lax.Precision.HIGHEST,
    )
    squares = jnp.sum(residual * residual, axis=1, keepdims=True)
    lane = column_iota(stat.shape, 1)
    stat = jnp.where(lane == router_ref.shape[0], squares, stat)
    stat_ref[...] = stat.reshape(rep_count, req, LANES)
    for e in range(experts):
        slots_ref[e] = lax.dot_general(
            s["maps"][e], gained.astype(bf16), (((0,), (0,)), ((), ())), preferred_element_type=f32
        ).astype(bf16)

    for k in range(z - 1):
        step_z(k).wait_send()
    for k in range(z):
        step_x(k).wait_send()
    for copy in step_copies + scale_copies:
        copy.wait_send()

    def pack_sent(k, _):
        @pl.when(jnp.logical_not(is_me(k)))
        def _():
            pack_copy(k).wait_send()

        return 0

    lax.fori_loop(0, rep_count, pack_sent, 0)

    def act_sent(i, _):
        for copy in act_copies(i):
            copy.wait_send()
        return 0

    lax.fori_loop(0, red.chunks, act_sent, 0)
    for h in range(ways):
        for copy in along_z(h) + along_xy(h) + [along_core(h)]:
            copy.wait_send()
    scatter_wait(idsall_ref, s["idss"], 0, count)
    scatter_wait(tokall, s["toks"], 0, count)
    scatter_wait(s["parts"], s["pts"], 0, count)
    state_out.wait()


def mixer(args, rep_count, tp_count, experts):
    tok, ids, gains, weight, skip, bias, decay, sel, history, router = args[:-4]
    step_proj, w, state, out_w = args[-4:]
    f32, bf16 = jnp.float32, jnp.bfloat16
    count = rep_count * tp_count
    tok_dev = tok.shape[0]
    slice_dev = tok.shape[1] // count
    pieces = (count, tok_dev, slice_dev)
    packed_rows = weight.shape[0] + skip.shape[0] + bias.shape[0] + decay.shape[0]
    packed = (packed_rows + -packed_rows % 16, decay.shape[1])
    req, states, inner_dev = state.shape
    red = Reduce(rep_count, tp_count, 2 * req, inner_dev, 0)
    n = red.chunks = red.per
    dma = pltpu.SemaphoreType.DMA
    vmem = pltpu.VMEM
    z, x, y, c = red.z, red.x, red.y, red.c
    tokens = count * tok_dev
    scratch = red.scratch(2 * slice_dev)
    scratch.update(
        left=vmem((2 * tokens, 2 * slice_dev), bf16),
        scale=vmem((tok_dev, LANES), f32),
        scales=vmem((tp_count, tok_dev, LANES), f32),
        tok=vmem(pieces, bf16),
        ids=vmem((tok_dev, LANES), bf16),
        packed=vmem(packed, bf16),
        tokall=vmem(pieces, bf16),
        packall=vmem((rep_count,) + packed, bf16),
        par=vmem((packed[0], inner_dev), f32),
        stepall=vmem((rep_count, tp_count, step_proj.shape[0], inner_dev), bf16),
        sel=vmem((LANES, inner_dev), bf16),
        router=vmem((LANES, slice_dev), f32),
        maps=vmem((experts, tokens, count * CAPACITY), bf16),
        gate=vmem((req, inner_dev), f32),
        act=vmem((req, inner_dev), f32),
        actall=vmem((rep_count, req, inner_dev), bf16),
        part=vmem((rep_count, req, LANES), bf16),
        parts=vmem((count, req, LANES), bf16),
        bc=vmem((LANES, LANES), f32),
        step=vmem((req, inner_dev), f32),
        read=vmem((req, inner_dev), f32),
        state=vmem(state.shape, f32),
        outw=vmem(out_w.shape, bf16),
        gall=vmem((y, c, z, x, req, inner_dev), bf16),
        toks=dma((2,)),
        idss=dma((2,)),
        pts=dma((2,)),
        scs=dma((2, tp_count - 1)),
        sts=dma((2, tp_count - 1)),
        pks=dma((2, rep_count)),
        own=dma((4,)),
        txs=dma((2, z)),
        tzs=dma((2, z - 1)),
        acs=dma((2, n, rep_count - 1)),
        gzs=dma((2, CORES, z - 1)),
        gxs=dma((2, CORES, x * y - 1)),
        gcs=dma((2, CORES)),
    )
    shape = jax.ShapeDtypeStruct
    anywhere = pl.BlockSpec(memory_space=pl.ANY)
    return pl.pallas_call(
        functools.partial(mixer_kernel, red, tuple(scratch), experts),
        out_shape=[
            shape(history.shape, bf16),
            shape(state.shape, f32),
            shape(pieces, bf16),
            shape((rep_count, req, LANES), f32),
            shape((experts, count * CAPACITY, slice_dev), bf16),
            shape((count, tok_dev, LANES), bf16),
        ],
        in_specs=in_vmem(10) + [anywhere] * 4,
        out_specs=in_vmem(1) + [anywhere] + in_vmem(4),
        scratch_shapes=list(scratch.values()),
        compiler_params=pltpu.CompilerParams(
            collective_id=0, has_side_effects=True, vmem_limit_bytes=62 * 2**20
        ),
        name="mixer",
    )(*args)


def last_kernel(
    red, names, begin, extra, experts_all, width, x_ref, home_ref, stat_ref, ids_ref, w_ref, hid_ref, *refs
):
    outs = 1 if extra else 0
    s = dict(zip(names, refs[outs:]))
    red.place()
    tp_count, rep_count = red.y * red.c, red.z * red.x
    count = tp_count * rep_count
    rep, tp = red.rep, red.tp
    me = rep * tp_count + tp
    wide = 2 * red.half
    for i in range(red.chunks):
        expert, column = divmod(begin + i, red.per)
        red.fetch(
            s, w_ref, i, column * wide, lambda w, at, expert=expert: w.at[:, expert, :, at]
        )
    for expert in range(x_ref.shape[0]):
        s["left"][expert] = spread(x_ref[expert], red.rows // 2, 2)
    if extra:
        mamba_ref, homes_ref = refs[0], s["homes"]
    greet_all(count, me, tp_count)

    def left_of(i):
        return s["left"][lax.div(begin + i, red.per)]

    req = red.rows // 2
    stats_ref = s["stats"]
    tok_dev = home_ref.shape[1]
    experts = x_ref.shape[0]

    def gates():
        for which in range(2):
            scatter_wait(stats_ref, s["sas"], which, count)
        summed = stats_ref[0]
        for k in range(1, count):
            summed += stats_ref[k]
        tokens = tp_count * tok_dev
        ids = ids_ref[pl.ds(pl.multiple_of(rep * tokens, 8), tokens)]
        lane = lax.broadcasted_iota(jnp.int32, (tokens, LANES), 1)
        first, second = named(ids, lane)
        scale = lax.rsqrt(summed[:, experts_all : experts_all + 1] / width + epsilon)
        logits = summed * scale
        one = jnp.sum(jnp.where(first, logits, 0.0), axis=1, keepdims=True)
        two = jnp.sum(jnp.where(second, logits, 0.0), axis=1, keepdims=True)
        gate = jnp.where(first, 1.0 / (1.0 + jnp.exp(two - one)), 0.0)
        gate += jnp.where(second, 1.0 / (1.0 + jnp.exp(one - two)), 0.0)
        gate = jnp.where(lane == LANES - 1, scale, gate)
        for e, taken in enumerate(slot_maps(ids, experts, tok_dev)):
            row = lax.dot_general(
                taken, gate, (((0,), (0,)), ((), ())), preferred_element_type=jnp.float32,
                precision=lax.Precision.HIGHEST,
            )
            seat = row[:, e : e + 1].astype(jnp.bfloat16).astype(jnp.float32)
            s["seat"][e] = jnp.broadcast_to(seat, s["seat"].shape[1:])
            s["size"][e] = jnp.broadcast_to(row[:, LANES - 1 :], s["size"].shape[1:])

    def store(i, h, total):
        expert = lax.div(begin + i, red.per)
        column = lax.rem(begin + i, red.per) * wide + h * red.half
        size = s["size"][expert][:, :1]
        up = total[req:] * size
        hidden = s["seat"][expert][:, :1] * silu(total[:req] * size) * up
        at = pl.ds(pl.multiple_of(column, LANES), red.half)
        hid_ref[expert, :, at] = hidden.astype(jnp.bfloat16)

    def send_home():
        scatter_start(home_ref, homes_ref, s["hos"], count, me, tp_count)
        homes_ref[me] = home_ref[me]

    def send_stats():

        def one(step, _):
            to = lax.rem(me + step, count)
            pltpu.make_async_remote_copy(
                src_ref=stat_ref.at[lax.div(to, tp_count)],
                dst_ref=stats_ref.at[me],
                send_sem=s["sas"].at[0],
                recv_sem=s["sas"].at[1],
                device_id=device_of(to, tp_count),
                device_id_type=MESH,
            ).start()
            return 0

        lax.fori_loop(1, count, one, 0)
        stats_ref[me] = stat_ref[rep]

    lags = (2, 4, 6, 8)
    extras = [(0, send_stats), (lags[3] - 1, gates)]
    if extra:
        extras.append((2, send_home))
    red.run(s, left_of, store, lags, extras)
    if extra:
        for which in range(2):
            scatter_wait(homes_ref, s["hos"], which, count)
        slice_dev = homes_ref.shape[2]
        for k in range(count):
            mamba_ref[:, k * slice_dev : (k + 1) * slice_dev] = homes_ref[k]


def last_stage(slots, home, stat, ids, w, experts_all, width, rep_count, tp_count, hidden_dev):
    f32, bf16 = jnp.float32, jnp.bfloat16
    experts, total_rows, slice_dev = slots.shape
    rows = 2 * total_rows // rep_count
    shape = jax.ShapeDtypeStruct
    dma = pltpu.SemaphoreType.DMA
    full = Reduce(rep_count, tp_count, rows, hidden_dev, 0)
    total = full.per * experts
    weights = w.size // experts // full.per * experts * 2 // experts
    most = max(1, ROOM // (full.chunk_bytes() + weights))
    begin, ups = 0, None
    while begin < total:
        red = Reduce(rep_count, tp_count, rows, hidden_dev, min(most, total - begin))
        extra = begin == 0
        scratch = red.scratch(2 * slice_dev)
        scratch["left"] = pltpu.VMEM((experts, rep_count * rows, 2 * slice_dev), bf16)
        scratch["sas"] = dma((2,))
        scratch["stats"] = pltpu.VMEM((rep_count * tp_count,) + stat.shape[1:], f32)
        scratch["seat"] = pltpu.VMEM((experts, rows // 2, LANES), f32)
        scratch["size"] = pltpu.VMEM((experts, rows // 2, LANES), f32)
        outs = [shape((experts, rows // 2, hidden_dev), bf16)]
        if extra:
            scratch["hos"] = dma((2,))
            scratch["homes"] = pltpu.VMEM(home.shape, bf16)
            outs += [shape((home.shape[1], width), bf16)]
        got = pl.pallas_call(
            functools.partial(last_kernel, red, tuple(scratch), begin, extra, experts_all, width),
            out_shape=outs,
            in_specs=in_vmem(4) + [pl.BlockSpec(memory_space=pl.ANY)],
            out_specs=in_vmem(len(outs)),
            scratch_shapes=list(scratch.values()),
            compiler_params=pltpu.CompilerParams(
                collective_id=10 + begin, has_side_effects=True, vmem_limit_bytes=62 * 2**20
            ),
            name="last_stage",
        )(slots, home, stat, ids, w)
        if extra:
            ups, homes = got
        else:
            edge = begin // full.per
            column = (begin % full.per) * 2 * full.half
            at = lax.broadcasted_iota(jnp.int32, (experts, 1, hidden_dev), 2)
            order = lax.broadcasted_iota(jnp.int32, (experts, 1, hidden_dev), 0)
            older = (order < edge) | ((order == edge) & (at < column))
            ups = jnp.where(older, ups, got[0])
        begin += red.chunks
    return ups, homes


def shards(
    tokens,
    conv_state,
    ssm_state,
    norm_gains,
    conv_weight,
    conv_skip,
    step_bias,
    decay_log,
    input_proj,
    select_proj,
    step_proj,
    output_proj,
    router,
    expert_proj,
    expert_ids,
):
    tp_count = lax.axis_size("tp")
    rep_count = lax.axis_size("rep")
    count = tp_count * rep_count
    tok_dev, width = tokens.shape
    experts = expert_proj.shape[1]
    hidden_dev = expert_proj.shape[3] // tp_count

    args = (
        tokens, expert_ids, norm_gains, conv_weight, conv_skip, step_bias[None], decay_log,
        select_proj.T, conv_state, router.T, step_proj, input_proj, ssm_state, output_proj,
    )
    conv_next, ssm_next, home, stat, slots, ids = mixer(args, rep_count, tp_count, experts)
    hidden, mamba_out = last_stage(
        slots, home, stat, ids.reshape(count * tok_dev, LANES), expert_proj,
        router.shape[1], width, rep_count, tp_count, hidden_dev,
    )
    hidden = hidden.reshape(experts, tp_count, CAPACITY, hidden_dev).transpose(1, 0, 2, 3)
    expert_hidden = hidden.reshape(experts * tp_count * CAPACITY, hidden_dev)
    return (mamba_out, conv_next, ssm_next, expert_hidden)


def solution(mesh):
    in_specs = (
        P(("rep", "tp"), None),
        P(None, "rep", "tp"),
        P("rep", None, "tp"),
        P(None, ("rep", "tp")),
        P(None, ("rep", "tp")),
        P(None, ("rep", "tp")),
        P(("rep", "tp")),
        P(None, ("rep", "tp")),
        P(("rep", "tp"), None, None),
        P("tp", "rep"),
        P(("rep", "tp"), None),
        P(None, ("rep", "tp")),
        P(("rep", "tp"), None),
        P(("rep", "tp"), None, None, None),
        P(("rep", "tp"), None),
    )
    out_specs = (P(("rep", "tp"), None), P(None, "rep", "tp"), P("rep", None, "tp"), P("rep", "tp"))
    return jax.shard_map(shards, mesh=mesh, in_specs=in_specs, out_specs=out_specs, check_vma=False)
```

```python
import functools

import jax
import jax.numpy as jnp
from jax import lax
from jax.experimental import pallas as pl
from jax.experimental.pallas import tpu as pltpu
from jax.sharding import PartitionSpec as P

CAPACITY = 2
LANES = 128


epsilon = 1e-05
MESH = pl.DeviceIdType.MESH


CORES = 2
LANE_PAIR = 2
ROOM = 40 * 2**20


def split_of(rep_count, tp_count):
    return rep_count // CORES, CORES, tp_count // CORES, CORES


def start_all(copies):
    for copy in copies:
        copy.start()


class Reduce:
    def __init__(self, rep_count, tp_count, rows, dev_cols, total_chunks):
        self.z, self.x, self.y, self.c = split_of(rep_count, tp_count)
        self.rows = rows
        self.half = 2 * LANES if dev_cols % (4 * LANES) == 0 else LANES
        self.per = dev_cols // (2 * self.half)
        self.dev_cols = dev_cols
        self.chunks = total_chunks
        self.blocks = self.z * self.x * self.y

    def chunk_bytes(self):
        return self.c * 2 * self.blocks * self.rows * self.half * 2 * 2

    def scratch(self, depth):
        n, z, x, y, rows, half = self.chunks, self.z, self.x, self.y, self.rows, self.half
        bf16 = jnp.bfloat16
        groups = self.c * y * 2 * (half // LANES)
        dma = pltpu.SemaphoreType.DMA
        buffers = dict(
            w=pltpu.VMEM((n, groups, depth // 2, 2, LANES), bf16),
            b0=pltpu.VMEM((n, self.c, 2, self.blocks, rows, half), bf16),
            r0=pltpu.VMEM((n, 2, self.blocks, rows, half), bf16),
            r1a=pltpu.VMEM((n, y - 1, x * z, rows, half), bf16),
            r1b=pltpu.VMEM((n, x - 1, y * z, rows, half), bf16),
            r2a=pltpu.VMEM((n, x - 1, z, rows, half), bf16),
            r2b=pltpu.VMEM((n, y - 1, z, rows, half), bf16),
            b3=pltpu.VMEM((n, z, 2, rows, half), bf16),
            r3=pltpu.VMEM((n, z - 1, 2, rows, half), bf16),
            ws=dma((n,)),
            s0=dma((2, n)),
            s1a=dma((2, n, y - 1)),
            s1b=dma((2, n, x - 1)),
            s2a=dma((2, n, x - 1)),
            s2b=dma((2, n, y - 1)),
            s3=dma((2, n, z - 1)),
        )
        return buffers

    def place(self):
        rep, tp = lax.axis_index("rep"), lax.axis_index("tp")
        self.rep, self.tp = rep, tp
        self.mz, self.mx = lax.div(rep, self.x), lax.rem(rep, self.x)
        self.my, self.mc = lax.div(tp, self.c), lax.rem(tp, self.c)

    def peer_z(self, to):
        return {"rep": to * self.x + self.mx}

    def peer_x(self, to):
        return {"rep": self.mz * self.x + to}

    def peer_y(self, to):
        return {"tp": to * self.c + self.mc}

    def peer_c(self):
        return {"tp": self.my * self.c + 1 - self.mc}

    def peers(self):
        out = [self.peer_c()]
        out += [self.peer_y(lax.rem(self.my + s, self.y)) for s in range(1, self.y)]
        out += [self.peer_x(lax.rem(self.mx + s, self.x)) for s in range(1, self.x)]
        out += [self.peer_z(lax.rem(self.mz + s, self.z)) for s in range(1, self.z)]
        return out

    def exchange(self, source, count, me, size, target, sems, i, peer):
        copies = []
        for step in range(1, count):
            to = lax.rem(me + step, count)
            copies.append(
                pltpu.make_async_remote_copy(
                    src_ref=source.at[pl.ds(to * size, size)],
                    dst_ref=target.at[i, step - 1],
                    send_sem=sems.at[0, i, step - 1],
                    recv_sem=sems.at[1, i, step - 1],
                    device_id=peer(to),
                    device_id_type=MESH,
                )
            )
        return copies

    def copies(self, s, i, stage):
        z, x, y = self.z, self.x, self.y
        if stage == 0:
            return [
                pltpu.make_async_remote_copy(
                    src_ref=s["b0"].at[i, 1 - self.mc],
                    dst_ref=s["r0"].at[i],
                    send_sem=s["s0"].at[0, i],
                    recv_sem=s["s0"].at[1, i],
                    device_id=self.peer_c(),
                    device_id_type=MESH,
                )
            ]
        if stage == 1:
            return self.exchange(
                s["r0"].at[i, 0], y, self.my, x * z, s["r1a"], s["s1a"], i, self.peer_y
            ) + self.exchange(
                s["r0"].at[i, 1], x, self.mx, y * z, s["r1b"], s["s1b"], i, self.peer_x
            )
        if stage == 2:
            return self.exchange(
                s["r1a"].at[i, 0], x, self.mx, z, s["r2a"], s["s2a"], i, self.peer_x
            ) + self.exchange(
                s["r1b"].at[i, 0], y, self.my, z, s["r2b"], s["s2b"], i, self.peer_y
            )
        third = []
        for step in range(1, z):
            to = lax.rem(self.mz + step, z)
            third.append(
                pltpu.make_async_remote_copy(
                    src_ref=s["b3"].at[i, to],
                    dst_ref=s["r3"].at[i, step - 1],
                    send_sem=s["s3"].at[0, i, step - 1],
                    recv_sem=s["s3"].at[1, i, step - 1],
                    device_id=self.peer_z(to),
                    device_id_type=MESH,
                )
            )
        return third

    def fetch(self, s, w_ref, i, column, pick):
        wide = 2 * self.half
        for y in range(self.y):
            for c in range(self.c):
                for k in range(wide // LANES):
                    at = (y * self.c + c) * self.dev_cols + column + k * LANES
                    at = pl.ds(pl.multiple_of(at, LANES), LANES)
                    pltpu.make_async_copy(
                        pick(w_ref, at),
                        s["w"].at[i, (y * self.c + c) * (wide // LANES) + k],
                        s["ws"].at[i],
                    ).start()

    def multiply(self, s, i, left):
        w = s["w"]
        pltpu.make_async_copy(w.at[i], w.at[i], s["ws"].at[i]).wait()
        depth = w.shape[2] * 2
        pieces = self.half // LANES
        for y in range(self.y):
            for c in range(self.c):
                for h in range(2):
                    first = ((y * self.c + c) * 2 + h) * pieces
                    right = [
                        w.at[i, first + k].reshape(depth, LANES)[...] for k in range(pieces)
                    ]
                    right = jnp.concatenate(right, axis=1) if pieces > 1 else right[0]
                    got = jnp.dot(left, right, preferred_element_type=jnp.float32)
                    got = got.astype(jnp.bfloat16)
                    got = got.reshape(self.z, self.x, self.rows, self.half)
                    for x in range(self.x):
                        at = (y * self.x + x) if h == 0 else (x * self.y + y)
                        s["b0"][i, c, h, at * self.z : (at + 1) * self.z] = got[:, x]
        start_all(self.copies(s, i, 0))

    def add(self, target, others):
        def piece(k, _):
            total = target[k].astype(jnp.float32)
            for other in others:
                total += other[k].astype(jnp.float32)
            target[k] = total.astype(jnp.bfloat16)
            return 0

        lax.fori_loop(0, target.shape[0], piece, 0, unroll=min(4, target.shape[0]))

    def after_core(self, s, i):
        for copy in self.copies(s, i, 0):
            copy.wait_recv()
        for h in range(2):
            self.add(s["r0"].at[i, h], [s["b0"].at[i, self.mc, h]])
        start_all(self.copies(s, i, 1))

    def after_first(self, s, i):
        for copy in self.copies(s, i, 1):
            copy.wait_recv()
        z = self.z
        for h, name, me, size, count in (
            (0, "r1a", self.my, self.x * z, self.y),
            (1, "r1b", self.mx, self.y * z, self.x),
        ):
            others = [s[name].at[i, k] for k in range(1, count - 1)]
            others.append(s["r0"].at[i, h, pl.ds(me * size, size)])
            self.add(s[name].at[i, 0], others)
        start_all(self.copies(s, i, 2))

    def after_second(self, s, i):
        for copy in self.copies(s, i, 2):
            copy.wait_recv()
        for h, name, came, me, count in (
            (0, "r2a", "r1a", self.mx, self.x),
            (1, "r2b", "r1b", self.my, self.y),
        ):
            for k in range(self.z):
                total = s[came][i, 0, me * self.z + k].astype(jnp.float32)
                for j in range(count - 1):
                    total += s[name][i, j, k].astype(jnp.float32)
                s["b3"][i, k, h] = total.astype(jnp.bfloat16)
        start_all(self.copies(s, i, 3))

    def after_third(self, s, i, store, done):
        for copy in self.copies(s, i, 3):
            copy.wait_recv()
        for h in range(2):
            total = s["b3"][i, self.mz, h].astype(jnp.float32)
            for k in range(self.z - 1):
                total += s["r3"][i, k, h].astype(jnp.float32)
            store(i, h, total)
        done(i)

    def finish(self, s):
        def one(i, _):
            for stage in range(4):
                for copy in self.copies(s, i, stage):
                    copy.wait_send()
            return 0

        lax.fori_loop(0, self.chunks, one, 0)

    def run(self, s, left_of, store, lags, extras=(), done=lambda i: None):
        n = self.chunks
        stages = (
            (lags[3], lambda i: self.after_third(s, i, store, done)),
            (lags[2], lambda i: self.after_second(s, i)),
            (lags[1], lambda i: self.after_first(s, i)),
            (lags[0], lambda i: self.after_core(s, i)),
            (0, lambda i: self.multiply(s, i, left_of(i))),
        )

        def step(t, _):
            for lag, work in stages:
                @pl.when((t >= lag) & (t < n + lag))
                def _(lag=lag, work=work):
                    work(t - lag)
            for when, work in extras:
                pl.when(t == when)(work)
            return 0

        lax.fori_loop(0, n + lags[3], step, 0)
        self.finish(s)


def spread(rows, per, pairs):
    count, depth = rows.shape
    lane = lax.broadcasted_iota(jnp.int32, (depth, depth * pairs), 1)
    source = lax.broadcasted_iota(jnp.int32, (depth, depth * pairs), 0)
    parts = []
    for j in range(pairs):
        moves = (lane == source * pairs + j).astype(jnp.bfloat16)
        part = jnp.dot(rows, moves, preferred_element_type=jnp.float32)
        parts.append(part.reshape(count // per, 1, per, depth * pairs))
    wide = jnp.concatenate(parts, axis=1)
    return wide.reshape(count * pairs, depth * pairs).astype(jnp.bfloat16)


def greet(ids):
    barrier = pltpu.get_barrier_semaphore()
    for device in ids:
        pl.semaphore_signal(barrier, inc=1, device_id=device, device_id_type=MESH)
    pl.semaphore_wait(barrier, len(ids))


def device_of(index, tp_count):
    return {"rep": lax.div(index, tp_count), "tp": lax.rem(index, tp_count)}


def greet_all(count, me, tp_count):
    barrier = pltpu.get_barrier_semaphore()

    def one(step, _):
        to = device_of(lax.rem(me + step, count), tp_count)
        pl.semaphore_signal(barrier, inc=1, device_id=to, device_id_type=MESH)
        return 0

    lax.fori_loop(1, count, one, 0)
    pl.semaphore_wait(barrier, count - 1)


def scatter_start(source, target, sems, count, me, tp_count):
    whole = len(source.shape) == len(target.shape) - 1

    def one(step, _):
        to = lax.rem(me + step, count)
        pltpu.make_async_remote_copy(
            src_ref=source if whole else source.at[to],
            dst_ref=target.at[me],
            send_sem=sems.at[0],
            recv_sem=sems.at[1],
            device_id=device_of(to, tp_count),
            device_id_type=MESH,
        ).start()
        return 0

    lax.fori_loop(1, count, one, 0)


def scatter_wait(target, sems, which, count):
    part = target.at[pl.ds(0, count - 1)]
    pltpu.make_async_copy(part, part, sems.at[which]).wait()


def in_vmem(count):
    return [pl.BlockSpec(memory_space=pltpu.VMEM)] * count


def remote(source, target, send_sem, recv_sem, device):
    return pltpu.make_async_remote_copy(
        src_ref=source,
        dst_ref=target,
        send_sem=send_sem,
        recv_sem=recv_sem,
        device_id=device,
        device_id_type=MESH,
    )


def silu(v):
    return v / (1.0 + jnp.exp(-v))


def softplus(v):
    return jnp.maximum(v, 0.0) + jnp.log1p(jnp.exp(-jnp.abs(v)))


def column_iota(shape, axis):
    return lax.broadcasted_iota(jnp.int32, shape, axis)


def named(ids, lane):
    ids = ids.astype(jnp.float32).astype(jnp.int32)
    return ids[:, :1] == lane, ids[:, 1:2] == lane


def slot_maps(ids, experts, tok_dev):
    rows = ids.shape[0]
    first, second = named(ids, column_iota((rows, LANES), 1))
    routed = (first | second).astype(jnp.float32)
    later, earlier = column_iota((rows, rows), 0), column_iota((rows, rows), 1)
    before = (earlier < later) & (lax.div(earlier, tok_dev) == lax.div(later, tok_dev))
    position = jnp.dot(
        before.astype(jnp.bfloat16), routed.astype(jnp.bfloat16), preferred_element_type=jnp.float32
    )
    slots = rows // tok_dev * CAPACITY
    row, slot = column_iota((rows, slots), 0), column_iota((rows, slots), 1)
    block = lax.div(row, tok_dev) == lax.div(slot, CAPACITY)
    seat = lax.rem(slot, CAPACITY).astype(jnp.float32)
    maps = []
    for e in range(experts):
        taken = block & (routed[:, e : e + 1] > 0.5) & (position[:, e : e + 1] == seat)
        maps.append(taken.astype(jnp.float32))
    return maps


def mixer_kernel(red, names, experts, tail, *refs):
    (
        tok_in_ref, ids_in_ref, gains_ref, weight_ref, skip_ref, bias_ref, decay_ref, sel_ref,
        history_ref, router_ref, step_ref, w_ref, state_ref, out_w_ref,
    ) = refs[:14]
    refs = refs[14:]
    if tail:
        expert_red, expert_names, experts_all = tail
        expert_w_ref, next_ref, state_out_ref, hid_ref, mamba_ref = refs[:5]
        scratch, expert_refs = refs[5 : 5 + len(names)], refs[5 + len(names) :]
    else:
        next_ref, state_out_ref, home_ref, stat_ref, slots_ref, idsall_ref = refs[:6]
        scratch = refs[6:]
    f32, bf16 = jnp.float32, jnp.bfloat16
    s = dict(zip(names, scratch))
    red.place()
    if tail:
        es = dict(zip(expert_names, expert_refs))
        expert_red.place()
        home_ref, stat_ref, slots_ref = s["home"], s["stat"], s["slots"]
        idsall_ref = s["idsall"]
    z, x, y, c = red.z, red.x, red.y, red.c
    mz, mx, my, mc = red.mz, red.mx, red.my, red.mc
    tp_count, rep_count = y * c, z * x
    count = tp_count * rep_count
    rep, tp = red.rep, red.tp
    me = rep * tp_count + tp
    inner_dev = red.dev_cols
    req = red.rows // 2
    tok_ref, ids_ref, packed_ref = s["tok"], s["ids"], s["packed"]
    tok_dev, slice_dev = tok_ref.shape[1:]
    tokall, packall, stepall = s["tokall"], s["packall"], s["stepall"]
    taps = history_ref.shape[0] + 1
    states = tap0 = state_ref.shape[1]

    state_in = pltpu.make_async_copy(state_ref, s["state"], s["own"].at[1])
    out_in = pltpu.make_async_copy(out_w_ref, s["outw"], s["own"].at[2])
    for i in range(red.chunks):
        red.fetch(s, w_ref, i, i * 2 * red.half, lambda w, at: w.at[:, :, at])
    columns = pl.ds(pl.multiple_of(tp * inner_dev, LANES), inner_dev)
    own_step = pltpu.make_async_copy(step_ref.at[:, columns], stepall.at[rep, tp], s["own"].at[0])
    own_step.start()
    state_in.start()
    out_in.start()
    for k in range(count):
        tok_ref[k] = tok_in_ref[:, k * slice_dev : (k + 1) * slice_dev]
    ids = ids_in_ref[...].astype(f32)
    ids = jnp.concatenate([ids, jnp.zeros((tok_dev, LANES - ids.shape[1]), f32)], axis=1)
    ids_ref[...] = ids.astype(bf16)
    rows = [ref[...].astype(f32) for ref in (decay_ref, weight_ref, skip_ref, bias_ref)]
    spare = packed_ref.shape[0] - sum(row.shape[0] for row in rows)
    rows.append(jnp.zeros((spare, packed_ref.shape[1]), f32))
    packed_ref[...] = jnp.concatenate(rows, axis=0).astype(bf16)
    tok = tok_in_ref[...].astype(f32)
    width = tok.shape[1]
    square = jnp.sum(tok * tok, axis=-1, keepdims=True)
    s["scale"][...] = jnp.broadcast_to(lax.rsqrt(square / width + epsilon), s["scale"].shape)
    greet_all(count, me, tp_count)
    scatter_start(tok_ref, tokall, s["toks"], count, me, tp_count)
    tokall[me] = tok_ref[me]
    slot = lax.rem(me, rep_count)
    home_tp = lax.div(me, rep_count)

    def pack_copy(to_rep):
        return remote(
            packed_ref, packall.at[slot], s["pks"].at[0, to_rep], s["pks"].at[1, slot],
            {"rep": to_rep, "tp": home_tp},
        )

    def is_me(to_rep):
        return (to_rep == rep) & (home_tp == tp)

    def pack_start(to_rep, _):
        @pl.when(is_me(to_rep))
        def _():
            packall[slot] = packed_ref[...]

        @pl.when(jnp.logical_not(is_me(to_rep)))
        def _():
            pack_copy(to_rep).start()

        return 0

    lax.fori_loop(0, rep_count, pack_start, 0)
    scale_copies, step_copies = [], []
    for k in range(tp_count - 1):
        to = lax.rem(tp + k + 1, tp_count)
        scale_copies.append(
            remote(
                s["scale"], s["scales"].at[tp], s["scs"].at[0, k], s["scs"].at[1, k], {"tp": to}
            )
        )
        columns = pl.ds(pl.multiple_of(to * inner_dev, LANES), inner_dev)
        step_copies.append(
            remote(
                step_ref.at[:, columns], stepall.at[rep, tp],
                s["sts"].at[0, k], s["sts"].at[1, k], {"tp": to},
            )
        )
    start_all(scale_copies)
    s["scales"][tp] = s["scale"][...]
    start_all(step_copies)
    scatter_start(ids_ref, idsall_ref, s["idss"], count, me, tp_count)
    idsall_ref[me] = ids_ref[...]
    to_x = {"rep": mz * x + lax.rem(mx + 1, x)}

    def step_z(k):
        block = stepall.at[rep]
        return remote(
            block, block, s["tzs"].at[0, k], s["tzs"].at[1, k], red.peer_z(lax.rem(mz + k + 1, z))
        )

    def step_x(source_z):
        block = stepall.at[source_z * x + mx]
        return remote(block, block, s["txs"].at[0, source_z], s["txs"].at[1, source_z], to_x)

    s["sel"][...] = jnp.zeros(s["sel"].shape, bf16)
    part_cols = sel_ref.shape[0]
    s["sel"][:part_cols] = sel_ref[...]
    s["router"][...] = jnp.zeros(s["router"].shape, f32)
    s["router"][: router_ref.shape[0]] = router_ref[...].astype(f32)
    next_ref[: taps - 2] = history_ref[1:]

    if tail:
        expert_fetch(expert_red, es, 0, expert_w_ref)
    scatter_wait(tokall, s["toks"], 1, count)
    tok_all = tokall.reshape(count * tok_dev, slice_dev)
    gain = gains_ref[...].astype(f32)
    x_rows = (tok_all[...].astype(f32) * gain[:1]).astype(bf16)
    s["left"][...] = spread(x_rows, req, 2)

    def step_first():
        own_step.wait()
        for copy in step_copies:
            copy.wait_recv()
        for k in range(z - 1):
            step_z(k).start()

    def step_second():
        for k in range(z - 1):
            step_z(k).wait_recv()
        for k in range(z // 2):
            step_x(k).start()

    def params():
        for copy in scale_copies:
            copy.wait_recv()

        def pack_came(k, _):
            @pl.when(tp * rep_count + k != me)
            def _():
                pltpu.make_async_copy(packall.at[k], packall.at[k], s["pks"].at[1, k]).wait()

            return 0

        lax.fori_loop(0, rep_count, pack_came, 0)
        own = packed_ref.shape[1]
        for k in range(rep_count):
            s["par"][:, k * own : (k + 1) * own] = packall[k].astype(f32)

    def maps():
        scatter_wait(idsall_ref, s["idss"], 1, count)
        ids = idsall_ref.reshape(count * tok_dev, LANES)[...]
        for e, taken in enumerate(slot_maps(ids, experts, tok_dev)):
            s["maps"][e] = taken.astype(bf16)

    def store(i, h, total):
        at = pl.ds(pl.multiple_of(i * 2 * red.half + h * red.half, LANES), red.half)
        scale = s["scales"].reshape(req, LANES)[:, :1]
        conv_input = total[:req] * scale
        s["gate"][:, at] = total[req:] * scale
        next_ref[taps - 2, :, at] = conv_input.astype(bf16)
        par = s["par"]
        mix = par[tap0 + taps - 1 : tap0 + taps, at] * conv_input
        mix += par[tap0 + taps : tap0 + taps + 1, at]
        for k in range(taps - 1):
            mix += par[tap0 + k : tap0 + k + 1, at] * history_ref[k, :, at].astype(f32)
        act = silu(mix)
        s["act"][:, at] = act
        s["actall"][rep, :, at] = act.astype(bf16)

    def act_copies(i):
        at = pl.ds(pl.multiple_of(i * 2 * red.half, LANES), 2 * red.half)
        block = s["actall"].at[rep, :, at]
        return [
            remote(
                block, block, s["acs"].at[0, i, k], s["acs"].at[1, i, k],
                {"rep": lax.rem(rep + k + 1, rep_count)},
            )
            for k in range(rep_count - 1)
        ]

    n = red.chunks
    lags = (1, n, n + 2, n + 4)
    extras = [(1, step_first), (2, params), (2, maps), (2 * n + 1, step_second)]
    red.run(
        s, lambda i: s["left"][...], store, lags, extras, lambda i: start_all(act_copies(i))
    )
    for k in range(z // 2, z):
        step_x(k).start()

    def act_came(i, _):
        for copy in act_copies(i):
            copy.wait_recv()
        return 0

    lax.fori_loop(0, red.chunks, act_came, 0)
    every = s["actall"].reshape(rep_count * req, inner_dev)[...]
    part = lax.dot_general(
        every, s["sel"][...], (((1,), (1,)), ((), ())), preferred_element_type=f32
    )
    s["part"][...] = part.astype(bf16).reshape(rep_count, req, LANES)

    def part_start(step, _):
        to = lax.rem(me + step, count)
        remote(
            s["part"].at[lax.div(to, tp_count)], s["parts"].at[me],
            s["pts"].at[0], s["pts"].at[1], device_of(to, tp_count),
        ).start()
        return 0

    lax.fori_loop(1, count, part_start, 0)
    s["parts"][me] = s["part"][rep]
    scatter_wait(s["parts"], s["pts"], 1, count)
    total_cols = part_cols * rep_count
    tiles = [jnp.zeros((req, LANES), f32) for _ in range(-(-total_cols // LANES))]
    lane = column_iota((req, LANES), 1)
    for r in range(rep_count):
        cols = s["parts"][r * tp_count].astype(f32)
        for p in range(1, tp_count):
            cols += s["parts"][r * tp_count + p].astype(f32)
        tile, shift = divmod(r * part_cols, LANES)
        if shift:
            cols = pltpu.roll(cols, shift, 1)
        tiles[tile] += jnp.where(lane >= shift, cols, 0.0)
        if shift + part_cols > LANES:
            tiles[tile + 1] += jnp.where(lane < shift + part_cols - LANES, cols, 0.0)
    rank = total_cols - 2 * states
    low_tiles = rank // LANES
    low = jnp.concatenate(tiles[:low_tiles], axis=1).astype(bf16)
    both_maps = jnp.concatenate(
        [tiles[low_tiles], jnp.zeros((LANES - req, LANES), f32)], axis=0
    ).T
    s["bc"][...] = both_maps
    for k in range(z):
        step_x(k).wait_recv()
    if step_ref.shape[0] % 8 == 0:
        step_rows = stepall.reshape(rank, inner_dev)[...]
    else:
        step_rows = stepall[...].reshape(rank, inner_dev)
    step_pre = jnp.dot(low, step_rows, preferred_element_type=f32)
    s["step"][...] = softplus(step_pre + s["par"][tap0 + taps + 2 : tap0 + taps + 3])
    state_in.wait()
    wide = 2 * LANES
    ways = s["gcs"].shape[1]
    piece = inner_dev // ways
    gall = s["gall"]

    def scan_block(b, _):
        at = pl.ds(pl.multiple_of(b * wide, LANES), wide)
        decay = -jnp.exp(s["par"][:states, at])
        step, act = s["step"][:, at], s["act"][:, at]
        for t in range(req):
            row = step[t : t + 1]
            now = jnp.exp(row * decay) * s["state"][t, :, at]
            now += (row * act[t : t + 1]) * s["bc"][:states, t : t + 1]
            s["state"][t, :, at] = now
            s["read"][t : t + 1, at] = jnp.sum(
                now * s["bc"][states : 2 * states, t : t + 1], axis=0, keepdims=True
            )
        read = s["read"][:, at] + s["par"][tap0 + taps + 1 : tap0 + taps + 2, at] * act
        gall[my, mc, mz, mx, :, at] = (read * silu(s["gate"][:, at])).astype(bf16)
        return 0

    def along_z(h):
        at = pl.ds(h * piece, piece)
        block = gall.at[my, mc, mz, mx, :, at]
        return [
            remote(
                block, block, s["gzs"].at[0, h, k], s["gzs"].at[1, h, k],
                red.peer_z(lax.rem(mz + k + 1, z)),
            )
            for k in range(z - 1)
        ]

    def along_xy(h):
        at = pl.ds(h * piece, piece)
        block = gall.at[my, mc, :, mx, :, at]
        out = []
        for k in range(1, x * y):
            dx, dy = k % x, k // x
            device = {
                "rep": mz * x + lax.rem(mx + dx, x),
                "tp": lax.rem(my + dy, y) * c + mc,
            }
            out.append(
                remote(block, block, s["gxs"].at[0, h, k - 1], s["gxs"].at[1, h, k - 1], device)
            )
        return out

    def along_core(h):
        block = gall.at[:, mc, :, :, :, pl.ds(h * piece, piece)]
        return remote(block, block, s["gcs"].at[0, h], s["gcs"].at[1, h], red.peer_c())

    blocks = piece // wide
    for h in range(ways):
        lax.fori_loop(h * blocks, (h + 1) * blocks, scan_block, 0)
        start_all(along_z(h))
    state_out = pltpu.make_async_copy(s["state"], state_out_ref, s["own"].at[3])
    state_out.start()
    for h in range(ways):
        for copy in along_z(h):
            copy.wait_recv()
        start_all(along_xy(h))
    for h in range(ways):
        for copy in along_xy(h):
            copy.wait_recv()
        along_core(h).start()
    out_in.wait()

    def product(core):
        total = jnp.zeros((rep_count * req, slice_dev), f32)
        for k in range(y):
            rows = gall.at[k, core].reshape(rep_count * req, inner_dev)[...]
            at = pl.multiple_of((k * c + core) * inner_dev, LANES)
            total += jnp.dot(rows, s["outw"][pl.ds(at, inner_dev)], preferred_element_type=f32)
        return total

    mixed = product(mc)
    for h in range(ways):
        along_core(h).wait_recv()
    residual = tok_all[...].astype(f32) + mixed + product(1 - mc)
    home_ref.reshape(count * tok_dev, slice_dev)[...] = residual.astype(bf16)
    gained = residual * gain[1:2]
    stat = lax.dot_general(
        gained, s["router"][...], (((1,), (1,)), ((), ())), preferred_element_type=f32,
        precision=lax.Precision.HIGHEST,
    )
    squares = jnp.sum(residual * residual, axis=1, keepdims=True)
    lane = column_iota(stat.shape, 1)
    stat = jnp.where(lane == router_ref.shape[0], squares, stat)
    stat_ref[...] = stat.reshape(rep_count, req, LANES)
    for e in range(experts):
        slots_ref[e] = lax.dot_general(
            s["maps"][e], gained.astype(bf16), (((0,), (0,)), ((), ())), preferred_element_type=f32
        ).astype(bf16)

    if tail:
        expert_part(
            expert_red, es, 0, experts_all, width, slots_ref, home_ref, stat_ref,
            idsall_ref.reshape(count * tok_dev, LANES), hid_ref, mamba_ref,
        )
    for k in range(z - 1):
        step_z(k).wait_send()
    for k in range(z):
        step_x(k).wait_send()
    for copy in step_copies + scale_copies:
        copy.wait_send()

    def pack_sent(k, _):
        @pl.when(jnp.logical_not(is_me(k)))
        def _():
            pack_copy(k).wait_send()

        return 0

    lax.fori_loop(0, rep_count, pack_sent, 0)

    def act_sent(i, _):
        for copy in act_copies(i):
            copy.wait_send()
        return 0

    lax.fori_loop(0, red.chunks, act_sent, 0)
    for h in range(ways):
        for copy in along_z(h) + along_xy(h) + [along_core(h)]:
            copy.wait_send()
    scatter_wait(idsall_ref, s["idss"], 0, count)
    scatter_wait(tokall, s["toks"], 0, count)
    scatter_wait(s["parts"], s["pts"], 0, count)
    state_out.wait()


def mixer(args, expert_w, experts_all, rep_count, tp_count):
    tok, ids, gains, weight, skip, bias, decay, sel, history, router = args[:10]
    step_proj, w, state, out_w = args[10:]
    experts, hidden_dev = expert_w.shape[1], expert_w.shape[3] // tp_count
    f32, bf16 = jnp.float32, jnp.bfloat16
    count = rep_count * tp_count
    tok_dev = tok.shape[0]
    slice_dev = tok.shape[1] // count
    pieces = (count, tok_dev, slice_dev)
    packed_rows = weight.shape[0] + skip.shape[0] + bias.shape[0] + decay.shape[0]
    packed = (packed_rows + -packed_rows % 16, decay.shape[1])
    req, states, inner_dev = state.shape
    red = Reduce(rep_count, tp_count, 2 * req, inner_dev, 0)
    n = red.chunks = red.per
    dma = pltpu.SemaphoreType.DMA
    vmem = pltpu.VMEM
    z, x, y, c = red.z, red.x, red.y, red.c
    tokens = count * tok_dev
    ways = 4 if inner_dev % (8 * LANES) == 0 else 2
    expert_rows = 2 * count * CAPACITY // rep_count
    expert_red = Reduce(rep_count, tp_count, expert_rows, hidden_dev, 0)
    expert_red.chunks = expert_red.per * experts
    held = sum(r.chunks * r.chunk_bytes() for r in (red, expert_red)) + 2 * (w.size + expert_w.size)
    fused = held <= ROOM
    scratch = red.scratch(2 * slice_dev)
    scratch.update(
        left=vmem((2 * tokens, 2 * slice_dev), bf16),
        scale=vmem((tok_dev, LANES), f32),
        scales=vmem((tp_count, tok_dev, LANES), f32),
        tok=vmem(pieces, bf16),
        ids=vmem((tok_dev, LANES), bf16),
        packed=vmem(packed, bf16),
        tokall=vmem(pieces, bf16),
        packall=vmem((rep_count,) + packed, bf16),
        par=vmem((packed[0], inner_dev), f32),
        stepall=vmem((rep_count, tp_count, step_proj.shape[0], inner_dev), bf16),
        sel=vmem((LANES, inner_dev), bf16),
        router=vmem((LANES, slice_dev), f32),
        maps=vmem((experts, tokens, count * CAPACITY), bf16),
        gate=vmem((req, inner_dev), f32),
        act=vmem((req, inner_dev), f32),
        actall=vmem((rep_count, req, inner_dev), bf16),
        part=vmem((rep_count, req, LANES), bf16),
        parts=vmem((count, req, LANES), bf16),
        bc=vmem((LANES, LANES), f32),
        step=vmem((req, inner_dev), f32),
        read=vmem((req, inner_dev), f32),
        state=vmem(state.shape, f32),
        outw=vmem(out_w.shape, bf16),
        gall=vmem((y, c, z, x, req, inner_dev), bf16),
        toks=dma((2,)),
        idss=dma((2,)),
        pts=dma((2,)),
        scs=dma((2, tp_count - 1)),
        sts=dma((2, tp_count - 1)),
        pks=dma((2, rep_count)),
        own=dma((4,)),
        txs=dma((2, z)),
        tzs=dma((2, z - 1)),
        acs=dma((2, n, rep_count - 1)),
        gzs=dma((2, ways, z - 1)),
        gxs=dma((2, ways, x * y - 1)),
        gcs=dma((2, ways)),
    )
    shape = jax.ShapeDtypeStruct
    anywhere = pl.BlockSpec(memory_space=pl.ANY)
    home, stat = pieces, (rep_count, req, LANES)
    slots = (experts, count * CAPACITY, slice_dev)
    idsall = (count, tok_dev, LANES)
    outs = [shape(history.shape, bf16), shape(state.shape, f32)]
    tail, names = None, tuple(scratch)
    if fused:
        scratch["home"] = vmem(home, bf16)
        scratch["stat"] = vmem(stat, f32)
        scratch["slots"] = vmem(slots, bf16)
        scratch["idsall"] = vmem(idsall, bf16)
        names = tuple(scratch)
        more = expert_scratch(expert_red, 2 * slice_dev, experts, stat, home)
        tail = (expert_red, tuple(more), experts_all)
        outs += [
            shape((experts, expert_rows // 2, hidden_dev), bf16), shape(tok.shape, bf16)
        ]
        args = args + (expert_w,)
        spaces = list(scratch.values()) + list(more.values())
    else:
        outs += [shape(home, bf16), shape(stat, f32), shape(slots, bf16), shape(idsall, bf16)]
        spaces = list(scratch.values())
    got = pl.pallas_call(
        functools.partial(mixer_kernel, red, names, experts, tail),
        out_shape=outs,
        in_specs=in_vmem(10) + [anywhere] * (len(args) - 10),
        out_specs=in_vmem(1) + [anywhere] + in_vmem(len(outs) - 2),
        scratch_shapes=spaces,
        compiler_params=pltpu.CompilerParams(
            collective_id=0, has_side_effects=True, vmem_limit_bytes=62 * 2**20
        ),
        name="mixer",
    )(*args)
    if fused:
        return got
    home, stat, slots, idsall = got[2:]
    hidden, mamba = last_stage(
        slots, home, stat, idsall.reshape(tokens, LANES), expert_w, experts_all,
        tok.shape[1], rep_count, tp_count, hidden_dev,
    )
    return got[0], got[1], hidden, mamba


def expert_fetch(red, s, begin, w_ref):
    for i in range(red.chunks):
        expert, column = divmod(begin + i, red.per)
        red.fetch(
            s, w_ref, i, column * 2 * red.half,
            lambda w, at, expert=expert: w.at[:, expert, :, at],
        )


def last_kernel(
    red, names, begin, extra, experts_all, width, x_ref, home_ref, stat_ref, ids_ref, w_ref, hid_ref, *refs
):
    outs = 1 if extra else 0
    s = dict(zip(names, refs[outs:]))
    red.place()
    expert_fetch(red, s, begin, w_ref)
    count = red.z * red.x * red.y * red.c
    greet_all(count, red.rep * red.y * red.c + red.tp, red.y * red.c)
    mamba_ref = refs[0] if extra else None
    expert_part(
        red, s, begin, experts_all, width, x_ref, home_ref, stat_ref, ids_ref, hid_ref, mamba_ref
    )


def expert_part(
    red, s, begin, experts_all, width, x_ref, home_ref, stat_ref, ids_ref, hid_ref, mamba_ref
):
    extra = mamba_ref is not None
    tp_count, rep_count = red.y * red.c, red.z * red.x
    count = tp_count * rep_count
    rep, tp = red.rep, red.tp
    me = rep * tp_count + tp
    wide = 2 * red.half
    homes_ref = s["homes"] if extra else None
    for expert in range(x_ref.shape[0]):
        s["left"][expert] = spread(x_ref[expert], red.rows // 2, 2)

    def left_of(i):
        return s["left"][lax.div(begin + i, red.per)]

    req = red.rows // 2
    stats_ref = s["stats"]
    tok_dev = home_ref.shape[1]
    experts = x_ref.shape[0]

    def gates():
        for which in range(2):
            scatter_wait(stats_ref, s["sas"], which, count)
        summed = stats_ref[0]
        for k in range(1, count):
            summed += stats_ref[k]
        tokens = tp_count * tok_dev
        ids = ids_ref[pl.ds(pl.multiple_of(rep * tokens, 8), tokens)]
        lane = lax.broadcasted_iota(jnp.int32, (tokens, LANES), 1)
        first, second = named(ids, lane)
        scale = lax.rsqrt(summed[:, experts_all : experts_all + 1] / width + epsilon)
        logits = summed * scale
        one = jnp.sum(jnp.where(first, logits, 0.0), axis=1, keepdims=True)
        two = jnp.sum(jnp.where(second, logits, 0.0), axis=1, keepdims=True)
        gate = jnp.where(first, 1.0 / (1.0 + jnp.exp(two - one)), 0.0)
        gate += jnp.where(second, 1.0 / (1.0 + jnp.exp(one - two)), 0.0)
        gate = jnp.where(lane == LANES - 1, scale, gate)
        for e, taken in enumerate(slot_maps(ids, experts, tok_dev)):
            row = lax.dot_general(
                taken, gate, (((0,), (0,)), ((), ())), preferred_element_type=jnp.float32,
                precision=lax.Precision.HIGHEST,
            )
            seat = row[:, e : e + 1].astype(jnp.bfloat16).astype(jnp.float32)
            s["seat"][e] = jnp.broadcast_to(seat, s["seat"].shape[1:])
            s["size"][e] = jnp.broadcast_to(row[:, LANES - 1 :], s["size"].shape[1:])

    def store(i, h, total):
        expert = lax.div(begin + i, red.per)
        column = lax.rem(begin + i, red.per) * wide + h * red.half
        size = s["size"][expert][:, :1]
        up = total[req:] * size
        hidden = s["seat"][expert][:, :1] * silu(total[:req] * size) * up
        at = pl.ds(pl.multiple_of(column, LANES), red.half)
        hid_ref[expert, :, at] = hidden.astype(jnp.bfloat16)

    def send_home():
        scatter_start(home_ref, homes_ref, s["hos"], count, me, tp_count)
        homes_ref[me] = home_ref[me]

    def send_stats():
        def one(step, _):
            to = lax.rem(me + step, count)
            pltpu.make_async_remote_copy(
                src_ref=stat_ref.at[lax.div(to, tp_count)],
                dst_ref=stats_ref.at[me],
                send_sem=s["sas"].at[0],
                recv_sem=s["sas"].at[1],
                device_id=device_of(to, tp_count),
                device_id_type=MESH,
            ).start()
            return 0

        lax.fori_loop(1, count, one, 0)
        stats_ref[me] = stat_ref[rep]

    lags = (2, 4, 6, 8)
    extras = [(0, send_stats), (lags[3] - 1, gates)]
    if extra:
        extras.append((2, send_home))
    red.run(s, left_of, store, lags, extras)
    if extra:
        for which in range(2):
            scatter_wait(homes_ref, s["hos"], which, count)
        slice_dev = homes_ref.shape[2]
        for k in range(count):
            mamba_ref[:, k * slice_dev : (k + 1) * slice_dev] = homes_ref[k]


def expert_scratch(red, depth, experts, stat, home):
    bf16, f32 = jnp.bfloat16, jnp.float32
    dma = pltpu.SemaphoreType.DMA
    rep_count, tp_count = red.z * red.x, red.y * red.c
    scratch = red.scratch(depth)
    scratch["left"] = pltpu.VMEM((experts, rep_count * red.rows, depth), bf16)
    scratch["sas"] = dma((2,))
    scratch["stats"] = pltpu.VMEM((rep_count * tp_count,) + stat[1:], f32)
    scratch["seat"] = pltpu.VMEM((experts, red.rows // 2, LANES), f32)
    scratch["size"] = pltpu.VMEM((experts, red.rows // 2, LANES), f32)
    if home is not None:
        scratch["hos"] = dma((2,))
        scratch["homes"] = pltpu.VMEM(home, bf16)
    return scratch


def last_stage(slots, home, stat, ids, w, experts_all, width, rep_count, tp_count, hidden_dev):
    bf16 = jnp.bfloat16
    experts, total_rows, slice_dev = slots.shape
    rows = 2 * total_rows // rep_count
    shape = jax.ShapeDtypeStruct
    full = Reduce(rep_count, tp_count, rows, hidden_dev, 0)
    total = full.per * experts
    most = max(1, ROOM // (full.chunk_bytes() + 2 * w.size // total))
    begin, ups = 0, None
    while begin < total:
        red = Reduce(rep_count, tp_count, rows, hidden_dev, min(most, total - begin))
        extra = begin == 0
        scratch = expert_scratch(
            red, 2 * slice_dev, experts, stat.shape, home.shape if extra else None
        )
        outs = [shape((experts, rows // 2, hidden_dev), bf16)]
        if extra:
            outs += [shape((home.shape[1], width), bf16)]
        got = pl.pallas_call(
            functools.partial(last_kernel, red, tuple(scratch), begin, extra, experts_all, width),
            out_shape=outs,
            in_specs=in_vmem(4) + [pl.BlockSpec(memory_space=pl.ANY)],
            out_specs=in_vmem(len(outs)),
            scratch_shapes=list(scratch.values()),
            compiler_params=pltpu.CompilerParams(
                collective_id=10 + begin, has_side_effects=True, vmem_limit_bytes=62 * 2**20
            ),
            name="last_stage",
        )(slots, home, stat, ids, w)
        if extra:
            ups, homes = got
        else:
            edge = begin // full.per
            column = (begin % full.per) * 2 * full.half
            at = lax.broadcasted_iota(jnp.int32, (experts, 1, hidden_dev), 2)
            order = lax.broadcasted_iota(jnp.int32, (experts, 1, hidden_dev), 0)
            older = (order < edge) | ((order == edge) & (at < column))
            ups = jnp.where(older, ups, got[0])
        begin += red.chunks
    return ups, homes


def finish_kernel(
    experts, next_ref, mamba_ref, hid_ref, state_ref,
    next_out, mamba_out, hid_out, state_out, held, sems
):
    parts = sems.shape[1]
    size = state_ref.shape[0] // parts

    def move(k, which):
        at = pl.ds(k * size, size)
        if which == 0:
            return pltpu.make_async_copy(state_ref.at[at], held.at[at], sems.at[0, k])
        return pltpu.make_async_copy(held.at[at], state_out.at[at], sems.at[1, k])

    for k in range(parts):
        move(k, 0).start()
    next_out[...] = next_ref[...]
    mamba_out[...] = mamba_ref[...]
    rows = hid_out.shape[0]
    to, source = column_iota((rows, rows), 0), column_iota((rows, rows), 1)
    block, seat = lax.div(to, experts * CAPACITY), lax.rem(to, CAPACITY)
    expert = lax.rem(lax.div(to, CAPACITY), experts)
    moves = source == expert * (rows // experts) + block * CAPACITY + seat
    hid_out[...] = jnp.dot(
        moves.astype(jnp.bfloat16), hid_ref[...], preferred_element_type=jnp.float32
    ).astype(jnp.bfloat16)
    for k in range(parts):
        move(k, 0).wait()
        move(k, 1).start()
    for k in range(parts):
        move(k, 1).wait()


def finish(conv_next, mamba, hidden, state, experts):
    anywhere = pl.BlockSpec(memory_space=pl.ANY)
    arrays = (conv_next, mamba, hidden, state)
    return pl.pallas_call(
        functools.partial(finish_kernel, experts),
        out_shape=[jax.ShapeDtypeStruct(array.shape, array.dtype) for array in arrays],
        in_specs=in_vmem(3) + [anywhere],
        out_specs=in_vmem(3) + [anywhere],
        scratch_shapes=[
            pltpu.VMEM(state.shape, state.dtype), pltpu.SemaphoreType.DMA((2, 4))
        ],
        name="finish",
    )(*arrays)


def shards(
    tokens,
    conv_state,
    ssm_state,
    norm_gains,
    conv_weight,
    conv_skip,
    step_bias,
    decay_log,
    input_proj,
    select_proj,
    step_proj,
    output_proj,
    router,
    expert_proj,
    expert_ids,
):
    tp_count = lax.axis_size("tp")
    rep_count = lax.axis_size("rep")
    args = (
        tokens, expert_ids, norm_gains, conv_weight, conv_skip, step_bias[None], decay_log,
        select_proj.T, conv_state, router.T, step_proj, input_proj, ssm_state, output_proj,
    )
    conv_next, ssm_next, hidden, mamba = mixer(
        args, expert_proj, router.shape[1], rep_count, tp_count
    )
    hidden = hidden.reshape(-1, hidden.shape[2])
    conv_next, mamba_out, expert_hidden, ssm_next = finish(
        conv_next, mamba, hidden, ssm_next, expert_proj.shape[1]
    )
    return (mamba_out, conv_next, ssm_next, expert_hidden)


def solution(mesh):
    in_specs = (
        P(("rep", "tp"), None),
        P(None, "rep", "tp"),
        P("rep", None, "tp"),
        P(None, ("rep", "tp")),
        P(None, ("rep", "tp")),
        P(None, ("rep", "tp")),
        P(("rep", "tp")),
        P(None, ("rep", "tp")),
        P(("rep", "tp"), None, None),
        P("tp", "rep"),
        P(("rep", "tp"), None),
        P(None, ("rep", "tp")),
        P(("rep", "tp"), None),
        P(("rep", "tp"), None, None, None),
        P(("rep", "tp"), None),
    )
    out_specs = (P(("rep", "tp"), None), P(None, "rep", "tp"), P("rep", None, "tp"), P("rep", "tp"))
    return jax.shard_map(shards, mesh=mesh, in_specs=in_specs, out_specs=out_specs, check_vma=False)
```

```python
import functools

import jax
import jax.numpy as jnp
from jax import lax
from jax.experimental import pallas as pl
from jax.experimental.pallas import tpu as pltpu
from jax.sharding import PartitionSpec as P

CAPACITY = 2
LANES = 128


epsilon = 1e-05
MESH = pl.DeviceIdType.MESH


CORES = 2
LANE_PAIR = 2
ROOM = 40 * 2**20


def split_of(rep_count, tp_count):
    return rep_count // CORES, CORES, tp_count // CORES, CORES


def start_all(copies):
    for copy in copies:
        copy.start()


class Reduce:
    def __init__(self, rep_count, tp_count, rows, dev_cols, total_chunks):
        self.z, self.x, self.y, self.c = split_of(rep_count, tp_count)
        self.rows = rows
        self.half = 2 * LANES if dev_cols % (4 * LANES) == 0 else LANES
        self.per = dev_cols // (2 * self.half)
        self.dev_cols = dev_cols
        self.chunks = total_chunks
        self.blocks = self.z * self.x * self.y

    def chunk_bytes(self):
        return self.c * 2 * self.blocks * self.rows * self.half * 2 * 2

    def scratch(self, depth):
        n, z, x, y, rows, half = self.chunks, self.z, self.x, self.y, self.rows, self.half
        bf16 = jnp.bfloat16
        groups = self.c * y * 2 * (half // LANES)
        dma = pltpu.SemaphoreType.DMA
        buffers = dict(
            w=pltpu.VMEM((n, groups, depth // 2, 2, LANES), bf16),
            b0=pltpu.VMEM((n, self.c, 2, self.blocks, rows, half), bf16),
            r0=pltpu.VMEM((n, 2, self.blocks, rows, half), bf16),
            r1a=pltpu.VMEM((n, y - 1, x * z, rows, half), bf16),
            r1b=pltpu.VMEM((n, x - 1, y * z, rows, half), bf16),
            r2a=pltpu.VMEM((n, x - 1, z, rows, half), bf16),
            r2b=pltpu.VMEM((n, y - 1, z, rows, half), bf16),
            b3=pltpu.VMEM((n, z, 2, rows, half), bf16),
            r3=pltpu.VMEM((n, z - 1, 2, rows, half), bf16),
            ws=dma((n,)),
            s0=dma((2, n)),
            s1a=dma((2, n, y - 1)),
            s1b=dma((2, n, x - 1)),
            s2a=dma((2, n, x - 1)),
            s2b=dma((2, n, y - 1)),
            s3=dma((2, n, z - 1)),
        )
        return buffers

    def place(self):
        rep, tp = lax.axis_index("rep"), lax.axis_index("tp")
        self.rep, self.tp = rep, tp
        self.mz, self.mx = lax.div(rep, self.x), lax.rem(rep, self.x)
        self.my, self.mc = lax.div(tp, self.c), lax.rem(tp, self.c)

    def peer_z(self, to):
        return {"rep": to * self.x + self.mx}

    def peer_x(self, to):
        return {"rep": self.mz * self.x + to}

    def peer_y(self, to):
        return {"tp": to * self.c + self.mc}

    def peer_c(self):
        return {"tp": self.my * self.c + 1 - self.mc}

    def peers(self):
        out = [self.peer_c()]
        out += [self.peer_y(lax.rem(self.my + s, self.y)) for s in range(1, self.y)]
        out += [self.peer_x(lax.rem(self.mx + s, self.x)) for s in range(1, self.x)]
        out += [self.peer_z(lax.rem(self.mz + s, self.z)) for s in range(1, self.z)]
        return out

    def exchange(self, source, count, me, size, target, sems, i, peer):
        copies = []
        for step in range(1, count):
            to = lax.rem(me + step, count)
            copies.append(
                pltpu.make_async_remote_copy(
                    src_ref=source.at[pl.ds(to * size, size)],
                    dst_ref=target.at[i, step - 1],
                    send_sem=sems.at[0, i, step - 1],
                    recv_sem=sems.at[1, i, step - 1],
                    device_id=peer(to),
                    device_id_type=MESH,
                )
            )
        return copies

    def copies(self, s, i, stage):
        z, x, y = self.z, self.x, self.y
        if stage == 0:
            return [
                pltpu.make_async_remote_copy(
                    src_ref=s["b0"].at[i, 1 - self.mc],
                    dst_ref=s["r0"].at[i],
                    send_sem=s["s0"].at[0, i],
                    recv_sem=s["s0"].at[1, i],
                    device_id=self.peer_c(),
                    device_id_type=MESH,
                )
            ]
        if stage == 1:
            return self.exchange(
                s["r0"].at[i, 0], y, self.my, x * z, s["r1a"], s["s1a"], i, self.peer_y
            ) + self.exchange(
                s["r0"].at[i, 1], x, self.mx, y * z, s["r1b"], s["s1b"], i, self.peer_x
            )
        if stage == 2:
            return self.exchange(
                s["r1a"].at[i, 0], x, self.mx, z, s["r2a"], s["s2a"], i, self.peer_x
            ) + self.exchange(
                s["r1b"].at[i, 0], y, self.my, z, s["r2b"], s["s2b"], i, self.peer_y
            )
        third = []
        for step in range(1, z):
            to = lax.rem(self.mz + step, z)
            third.append(
                pltpu.make_async_remote_copy(
                    src_ref=s["b3"].at[i, to],
                    dst_ref=s["r3"].at[i, step - 1],
                    send_sem=s["s3"].at[0, i, step - 1],
                    recv_sem=s["s3"].at[1, i, step - 1],
                    device_id=self.peer_z(to),
                    device_id_type=MESH,
                )
            )
        return third

    def fetch(self, s, w_ref, i, column, pick):
        wide = 2 * self.half
        for y in range(self.y):
            for c in range(self.c):
                for k in range(wide // LANES):
                    at = (y * self.c + c) * self.dev_cols + column + k * LANES
                    at = pl.ds(pl.multiple_of(at, LANES), LANES)
                    pltpu.make_async_copy(
                        pick(w_ref, at),
                        s["w"].at[i, (y * self.c + c) * (wide // LANES) + k],
                        s["ws"].at[i],
                    ).start()

    def multiply(self, s, i, left):
        w = s["w"]
        pltpu.make_async_copy(w.at[i], w.at[i], s["ws"].at[i]).wait()
        depth = w.shape[2] * 2
        pieces = self.half // LANES
        for y in range(self.y):
            for c in range(self.c):
                for h in range(2):
                    first = ((y * self.c + c) * 2 + h) * pieces
                    right = [
                        w.at[i, first + k].reshape(depth, LANES)[...] for k in range(pieces)
                    ]
                    right = jnp.concatenate(right, axis=1) if pieces > 1 else right[0]
                    got = jnp.dot(left, right, preferred_element_type=jnp.float32)
                    got = got.astype(jnp.bfloat16)
                    got = got.reshape(self.z, self.x, self.rows, self.half)
                    for x in range(self.x):
                        at = (y * self.x + x) if h == 0 else (x * self.y + y)
                        s["b0"][i, c, h, at * self.z : (at + 1) * self.z] = got[:, x]
        start_all(self.copies(s, i, 0))

    def add(self, target, others):
        def piece(k, _):
            total = target[k].astype(jnp.float32)
            for other in others:
                total += other[k].astype(jnp.float32)
            target[k] = total.astype(jnp.bfloat16)
            return 0

        lax.fori_loop(0, target.shape[0], piece, 0, unroll=min(4, target.shape[0]))

    def after_core(self, s, i):
        for copy in self.copies(s, i, 0):
            copy.wait_recv()
        for h in range(2):
            self.add(s["r0"].at[i, h], [s["b0"].at[i, self.mc, h]])
        start_all(self.copies(s, i, 1))

    def after_first(self, s, i):
        for copy in self.copies(s, i, 1):
            copy.wait_recv()
        z = self.z
        for h, name, me, size, count in (
            (0, "r1a", self.my, self.x * z, self.y),
            (1, "r1b", self.mx, self.y * z, self.x),
        ):
            others = [s[name].at[i, k] for k in range(1, count - 1)]
            others.append(s["r0"].at[i, h, pl.ds(me * size, size)])
            self.add(s[name].at[i, 0], others)
        start_all(self.copies(s, i, 2))

    def after_second(self, s, i):
        for copy in self.copies(s, i, 2):
            copy.wait_recv()
        for h, name, came, me, count in (
            (0, "r2a", "r1a", self.mx, self.x),
            (1, "r2b", "r1b", self.my, self.y),
        ):
            for k in range(self.z):
                total = s[came][i, 0, me * self.z + k].astype(jnp.float32)
                for j in range(count - 1):
                    total += s[name][i, j, k].astype(jnp.float32)
                s["b3"][i, k, h] = total.astype(jnp.bfloat16)
        start_all(self.copies(s, i, 3))

    def after_third(self, s, i, store, done):
        for copy in self.copies(s, i, 3):
            copy.wait_recv()
        for h in range(2):
            total = s["b3"][i, self.mz, h].astype(jnp.float32)
            for k in range(self.z - 1):
                total += s["r3"][i, k, h].astype(jnp.float32)
            store(i, h, total)
        done(i)

    def finish(self, s):
        def one(i, _):
            for stage in range(4):
                for copy in self.copies(s, i, stage):
                    copy.wait_send()
            return 0

        lax.fori_loop(0, self.chunks, one, 0)

    def run(self, s, left_of, store, lags, extras=(), done=lambda i: None):
        n = self.chunks
        stages = (
            (lags[3], lambda i: self.after_third(s, i, store, done)),
            (lags[2], lambda i: self.after_second(s, i)),
            (lags[1], lambda i: self.after_first(s, i)),
            (lags[0], lambda i: self.after_core(s, i)),
            (0, lambda i: self.multiply(s, i, left_of(i))),
        )

        def step(t, _):
            for lag, work in stages:
                @pl.when((t >= lag) & (t < n + lag))
                def _(lag=lag, work=work):
                    work(t - lag)
            for when, work in extras:
                pl.when(t == when)(work)
            return 0

        lax.fori_loop(0, n + lags[3], step, 0)
        self.finish(s)


def spread(rows, per, pairs):
    count, depth = rows.shape
    lane = lax.broadcasted_iota(jnp.int32, (depth, depth * pairs), 1)
    source = lax.broadcasted_iota(jnp.int32, (depth, depth * pairs), 0)
    parts = []
    for j in range(pairs):
        moves = (lane == source * pairs + j).astype(jnp.bfloat16)
        part = jnp.dot(rows, moves, preferred_element_type=jnp.float32)
        parts.append(part.reshape(count // per, 1, per, depth * pairs))
    wide = jnp.concatenate(parts, axis=1)
    return wide.reshape(count * pairs, depth * pairs).astype(jnp.bfloat16)


def greet(ids):
    barrier = pltpu.get_barrier_semaphore()
    for device in ids:
        pl.semaphore_signal(barrier, inc=1, device_id=device, device_id_type=MESH)
    pl.semaphore_wait(barrier, len(ids))


def device_of(index, tp_count):
    return {"rep": lax.div(index, tp_count), "tp": lax.rem(index, tp_count)}


def greet_all(count, me, tp_count):
    barrier = pltpu.get_barrier_semaphore()

    def one(step, _):
        to = device_of(lax.rem(me + step, count), tp_count)
        pl.semaphore_signal(barrier, inc=1, device_id=to, device_id_type=MESH)
        return 0

    lax.fori_loop(1, count, one, 0)
    pl.semaphore_wait(barrier, count - 1)


def scatter_start(source, target, sems, count, me, tp_count):
    whole = len(source.shape) == len(target.shape) - 1

    def one(step, _):
        to = lax.rem(me + step, count)
        pltpu.make_async_remote_copy(
            src_ref=source if whole else source.at[to],
            dst_ref=target.at[me],
            send_sem=sems.at[0],
            recv_sem=sems.at[1],
            device_id=device_of(to, tp_count),
            device_id_type=MESH,
        ).start()
        return 0

    lax.fori_loop(1, count, one, 0)


def scatter_wait(target, sems, which, count):
    part = target.at[pl.ds(0, count - 1)]
    pltpu.make_async_copy(part, part, sems.at[which]).wait()


def in_vmem(count):
    return [pl.BlockSpec(memory_space=pltpu.VMEM)] * count


def remote(source, target, send_sem, recv_sem, device):
    return pltpu.make_async_remote_copy(
        src_ref=source,
        dst_ref=target,
        send_sem=send_sem,
        recv_sem=recv_sem,
        device_id=device,
        device_id_type=MESH,
    )


def silu(v):
    return v / (1.0 + jnp.exp(-v))


def softplus(v):
    return jnp.maximum(v, 0.0) + jnp.log1p(jnp.exp(-jnp.abs(v)))


def column_iota(shape, axis):
    return lax.broadcasted_iota(jnp.int32, shape, axis)


def named(ids, lane):
    ids = ids.astype(jnp.float32).astype(jnp.int32)
    return ids[:, :1] == lane, ids[:, 1:2] == lane


def slot_maps(ids, experts, tok_dev):
    rows = ids.shape[0]
    first, second = named(ids, column_iota((rows, LANES), 1))
    routed = (first | second).astype(jnp.float32)
    later, earlier = column_iota((rows, rows), 0), column_iota((rows, rows), 1)
    before = (earlier < later) & (lax.div(earlier, tok_dev) == lax.div(later, tok_dev))
    position = jnp.dot(
        before.astype(jnp.bfloat16), routed.astype(jnp.bfloat16), preferred_element_type=jnp.float32
    )
    slots = rows // tok_dev * CAPACITY
    row, slot = column_iota((rows, slots), 0), column_iota((rows, slots), 1)
    block = lax.div(row, tok_dev) == lax.div(slot, CAPACITY)
    seat = lax.rem(slot, CAPACITY).astype(jnp.float32)
    maps = []
    for e in range(experts):
        taken = block & (routed[:, e : e + 1] > 0.5) & (position[:, e : e + 1] == seat)
        maps.append(taken.astype(jnp.float32))
    return maps


def mixer_kernel(red, names, experts, tail, *refs):
    (
        tok_in_ref, ids_in_ref, gains_ref, weight_ref, skip_ref, bias_ref, decay_ref, sel_ref,
        history_ref, router_ref, step_ref, w_ref, state_ref, out_w_ref,
    ) = refs[:14]
    refs = refs[14:]
    if tail:
        expert_red, expert_names, experts_all = tail
        expert_w_ref, next_ref, state_out_ref, hid_ref, mamba_ref = refs[:5]
        scratch, expert_refs = refs[5 : 5 + len(names)], refs[5 + len(names) :]
    else:
        next_ref, state_out_ref, home_ref, stat_ref, slots_ref, idsall_ref = refs[:6]
        scratch = refs[6:]
    f32, bf16 = jnp.float32, jnp.bfloat16
    s = dict(zip(names, scratch))
    red.place()
    if tail:
        es = dict(zip(expert_names, expert_refs))
        expert_red.place()
        home_ref, stat_ref, slots_ref = s["home"], s["stat"], s["slots"]
        idsall_ref = s["idsall"]
    z, x, y, c = red.z, red.x, red.y, red.c
    mz, mx, my, mc = red.mz, red.mx, red.my, red.mc
    tp_count, rep_count = y * c, z * x
    count = tp_count * rep_count
    rep, tp = red.rep, red.tp
    me = rep * tp_count + tp
    inner_dev = red.dev_cols
    req = red.rows // 2
    tok_ref, ids_ref, packed_ref = s["tok"], s["ids"], s["packed"]
    tok_dev, slice_dev = tok_ref.shape[1:]
    tokall, packall, stepz = s["tokall"], s["packall"], s["stepz"]
    step_dev, part_cols = step_ref.shape[0], sel_ref.shape[0]
    group_cols = part_cols * x
    owners = group_cols // step_dev
    taps = history_ref.shape[0] + 1
    states = tap0 = state_ref.shape[1]

    state_in = pltpu.make_async_copy(state_ref, s["state"], s["own"].at[1])
    out_in = pltpu.make_async_copy(out_w_ref, s["outw"], s["own"].at[2])
    for i in range(red.chunks):
        red.fetch(s, w_ref, i, i * 2 * red.half, lambda w, at: w.at[:, :, at])
    state_in.start()
    out_in.start()
    for k in range(count):
        tok_ref[k] = tok_in_ref[:, k * slice_dev : (k + 1) * slice_dev]
    ids = ids_in_ref[...].astype(f32)
    ids = jnp.concatenate([ids, jnp.zeros((tok_dev, LANES - ids.shape[1]), f32)], axis=1)
    ids_ref[...] = ids.astype(bf16)
    rows = [ref[...].astype(f32) for ref in (decay_ref, weight_ref, skip_ref)]
    rows.append(bias_ref[...].astype(f32).reshape(1, -1))
    spare = packed_ref.shape[0] - sum(row.shape[0] for row in rows)
    rows.append(jnp.zeros((spare, packed_ref.shape[1]), f32))
    packed_ref[...] = jnp.concatenate(rows, axis=0).astype(bf16)
    tok = tok_in_ref[...].astype(f32)
    width = tok.shape[1]
    square = jnp.sum(tok * tok, axis=-1, keepdims=True)
    s["scale"][...] = jnp.broadcast_to(lax.rsqrt(square / width + epsilon), s["scale"].shape)
    stepz[...] = jnp.zeros(stepz.shape, bf16)
    greet_all(count, me, tp_count)
    scatter_start(tok_ref, tokall, s["toks"], count, me, tp_count)
    tokall[me] = tok_ref[me]
    slot = lax.rem(me, rep_count)
    home_tp = lax.div(me, rep_count)

    def pack_copy(to_rep):
        return remote(
            packed_ref, packall.at[slot], s["pks"].at[0, to_rep], s["pks"].at[1, slot],
            {"rep": to_rep, "tp": home_tp},
        )

    def is_me(to_rep):
        return (to_rep == rep) & (home_tp == tp)

    def pack_start(to_rep, _):
        @pl.when(is_me(to_rep))
        def _():
            packall[slot] = packed_ref[...]

        @pl.when(jnp.logical_not(is_me(to_rep)))
        def _():
            pack_copy(to_rep).start()

        return 0

    lax.fori_loop(0, rep_count, pack_start, 0)
    scale_copies = []
    for k in range(tp_count - 1):
        to = lax.rem(tp + k + 1, tp_count)
        scale_copies.append(
            remote(
                s["scale"], s["scales"].at[tp], s["scs"].at[0, k], s["scs"].at[1, k], {"tp": to}
            )
        )
    start_all(scale_copies)
    s["scales"][tp] = s["scale"][...]
    scatter_start(ids_ref, idsall_ref, s["idss"], count, me, tp_count)
    idsall_ref[me] = ids_ref[...]
    sel_copies = [
        remote(
            sel_ref, s["sel"].at[mx], s["sxs"].at[0, k], s["sxs"].at[1, k],
            red.peer_x(lax.rem(mx + k + 1, x)),
        )
        for k in range(x - 1)
    ]
    start_all(sel_copies)
    step_slot, step_home = lax.rem(me, owners), lax.div(me, owners)

    def step_target(k):
        return step_home * x + lax.div(k, tp_count), lax.rem(k, tp_count)

    def step_is_me(k):
        to_rep, to_tp = step_target(k)
        return (to_rep == rep) & (to_tp == tp)

    def step_source(to_tp):
        return step_ref.at[:, pl.ds(pl.multiple_of(to_tp * inner_dev, LANES), inner_dev)]

    def step_copy(k):
        to_rep, to_tp = step_target(k)
        return remote(
            step_source(to_tp), stepz.at[step_slot],
            s["sts"].at[0, k], s["sts"].at[1, step_slot], {"rep": to_rep, "tp": to_tp},
        )

    own_step = pltpu.make_async_copy(step_source(tp), stepz.at[step_slot], s["own"].at[0])

    def step_start(k, _):
        @pl.when(step_is_me(k))
        def _():
            own_step.start()

        @pl.when(jnp.logical_not(step_is_me(k)))
        def _():
            step_copy(k).start()

        return 0

    lax.fori_loop(0, x * tp_count, step_start, 0)

    s["sel"][mx] = sel_ref[...]
    s["router"][...] = jnp.zeros(s["router"].shape, f32)
    s["router"][: router_ref.shape[0]] = router_ref[...].astype(f32)
    next_ref[: taps - 2] = history_ref[1:]

    if tail:
        expert_fetch(expert_red, es, 0, expert_w_ref)
    scatter_wait(tokall, s["toks"], 1, count)
    tok_all = tokall.reshape(count * tok_dev, slice_dev)
    gain = gains_ref[...].astype(f32)
    x_rows = (tok_all[...].astype(f32) * gain[:1]).astype(bf16)
    s["left"][...] = spread(x_rows, req, 2)

    def weights():
        for copy in sel_copies:
            copy.wait_recv()

        def step_came(k, _):
            @pl.when((mz * owners + k != me) & (mz * owners + k < count))
            def _():
                pltpu.make_async_copy(stepz.at[k], stepz.at[k], s["sts"].at[1, k]).wait()

            return 0

        lax.fori_loop(0, owners, step_came, 0)

        def own_came(k, _):
            pl.when(step_is_me(k))(own_step.wait)
            return 0

        lax.fori_loop(0, x * tp_count, own_came, 0)

    def params():
        for copy in scale_copies:
            copy.wait_recv()

        def pack_came(k, _):
            @pl.when(tp * rep_count + k != me)
            def _():
                pltpu.make_async_copy(packall.at[k], packall.at[k], s["pks"].at[1, k]).wait()

            return 0

        lax.fori_loop(0, rep_count, pack_came, 0)
        own = packed_ref.shape[1]
        for k in range(rep_count):
            s["par"][:, k * own : (k + 1) * own] = packall[k].astype(f32)

    def maps():
        scatter_wait(idsall_ref, s["idss"], 1, count)
        ids = idsall_ref.reshape(count * tok_dev, LANES)[...]
        for e, taken in enumerate(slot_maps(ids, experts, tok_dev)):
            s["maps"][e] = taken.astype(bf16)

    def store(i, h, total):
        at = pl.ds(pl.multiple_of(i * 2 * red.half + h * red.half, LANES), red.half)
        scale = s["scales"].reshape(req, LANES)[:, :1]
        conv_input = total[:req] * scale
        s["gate"][:, at] = total[req:] * scale
        next_ref[taps - 2, :, at] = conv_input.astype(bf16)
        par = s["par"]
        mix = par[tap0 + taps - 1 : tap0 + taps, at] * conv_input
        mix += par[tap0 + taps : tap0 + taps + 1, at]
        for k in range(taps - 1):
            mix += par[tap0 + k : tap0 + k + 1, at] * history_ref[k, :, at].astype(f32)
        act = silu(mix)
        s["act"][:, at] = act
        s["actall"][mz, :, at] = act.astype(bf16)

    def act_copies(i):
        at = pl.ds(pl.multiple_of(i * 2 * red.half, LANES), 2 * red.half)
        block = s["actall"].at[mz, :, at]
        return [
            remote(
                block, block, s["acs"].at[0, i, k], s["acs"].at[1, i, k],
                red.peer_z(lax.rem(mz + k + 1, z)),
            )
            for k in range(z - 1)
        ]

    n = red.chunks
    lags = (1, n, n + 2, n + 4)
    extras = [(2, params), (2, maps), (n, weights)]
    red.run(
        s, lambda i: s["left"][...], store, lags, extras, lambda i: start_all(act_copies(i))
    )
    def act_came(i, _):
        for copy in act_copies(i):
            copy.wait_recv()
        return 0

    lax.fori_loop(0, red.chunks, act_came, 0)
    every = s["actall"].reshape(z * req, inner_dev)[...]
    part = jnp.zeros((z * req, LANES), f32)
    for k in range(x):
        cols = lax.dot_general(
            every, s["sel"][k], (((1,), (1,)), ((), ())), preferred_element_type=f32
        )
        spare = jnp.zeros((z * req, LANES - part_cols), f32)
        cols = jnp.concatenate([cols, spare], axis=1)
        part += pltpu.roll(cols, k * part_cols, 1) if k else cols
    s["parts"][tp] = part.astype(bf16)
    part_copies = [
        remote(
            s["parts"].at[tp], s["parts"].at[tp], s["pts"].at[0, k], s["pts"].at[1, k],
            {"tp": lax.rem(tp + k + 1, tp_count)},
        )
        for k in range(tp_count - 1)
    ]
    start_all(part_copies)
    for copy in part_copies:
        copy.wait_recv()
    selected = s["parts"][0].astype(f32)
    for k in range(1, tp_count):
        selected += s["parts"][k].astype(f32)
    s["picks"][...] = selected.reshape(z, req, LANES)
    if step_dev % 8 == 0:
        step_rows = stepz.reshape(LANES, inner_dev)[...]
    else:
        step_rows = stepz[...].reshape(LANES, inner_dev)
    pre = jnp.dot(selected.astype(bf16), step_rows, preferred_element_type=f32)
    s["pre"][...] = pre.astype(bf16).reshape(z, req, inner_dev)
    pre_copies = []
    for k in range(z - 1):
        to = lax.rem(mz + k + 1, z)
        for name, slots, sems in (("picks", "picked", "mzs"), ("pre", "preall", "pzs")):
            pre_copies.append(
                remote(
                    s[name].at[to], s[slots].at[mz], s[sems].at[0, k], s[sems].at[1, k],
                    red.peer_z(to),
                )
            )
    start_all(pre_copies)
    s["picked"][mz] = s["picks"][mz]
    s["preall"][mz] = s["pre"][mz]
    for copy in pre_copies:
        copy.wait_recv()
    rank = step_dev * count
    maps_z, maps_lane = divmod(rank, group_cols)
    both = jnp.concatenate(
        [s["picked"][maps_z], jnp.zeros((LANES - req, LANES), f32)], axis=0
    )
    s["bc"][...] = (pltpu.roll(both, LANES - maps_lane, 1) if maps_lane else both).T
    step_pre = s["preall"][0].astype(f32)
    for k in range(1, z):
        step_pre += s["preall"][k].astype(f32)
    s["step"][...] = softplus(step_pre + s["par"][tap0 + taps + 2 : tap0 + taps + 3])
    state_in.wait()
    wide = 2 * LANES
    ways = s["gcs"].shape[1]
    piece = inner_dev // ways
    gall = s["gall"]

    def scan_block(b, _):
        at = pl.ds(pl.multiple_of(b * wide, LANES), wide)
        decay = -jnp.exp(s["par"][:states, at])
        step, act = s["step"][:, at], s["act"][:, at]
        for t in range(req):
            row = step[t : t + 1]
            now = jnp.exp(row * decay) * s["state"][t, :, at]
            now += (row * act[t : t + 1]) * s["bc"][:states, t : t + 1]
            s["state"][t, :, at] = now
            s["read"][t : t + 1, at] = jnp.sum(
                now * s["bc"][states : 2 * states, t : t + 1], axis=0, keepdims=True
            )
        read = s["read"][:, at] + s["par"][tap0 + taps + 1 : tap0 + taps + 2, at] * act
        gall[my, mc, mz, mx, :, at] = (read * silu(s["gate"][:, at])).astype(bf16)
        return 0

    def along_z(h):
        at = pl.ds(h * piece, piece)
        block = gall.at[my, mc, mz, mx, :, at]
        return [
            remote(
                block, block, s["gzs"].at[0, h, k], s["gzs"].at[1, h, k],
                red.peer_z(lax.rem(mz + k + 1, z)),
            )
            for k in range(z - 1)
        ]

    def along_xy(h):
        at = pl.ds(h * piece, piece)
        block = gall.at[my, mc, :, mx, :, at]
        out = []
        for k in range(1, x * y):
            dx, dy = k % x, k // x
            device = {
                "rep": mz * x + lax.rem(mx + dx, x),
                "tp": lax.rem(my + dy, y) * c + mc,
            }
            out.append(
                remote(block, block, s["gxs"].at[0, h, k - 1], s["gxs"].at[1, h, k - 1], device)
            )
        return out

    def along_core(h):
        block = gall.at[:, mc, :, :, :, pl.ds(h * piece, piece)]
        return remote(block, block, s["gcs"].at[0, h], s["gcs"].at[1, h], red.peer_c())

    blocks = piece // wide
    for h in range(ways):
        lax.fori_loop(h * blocks, (h + 1) * blocks, scan_block, 0)
        start_all(along_z(h))
    state_out = pltpu.make_async_copy(s["state"], state_out_ref, s["own"].at[3])
    state_out.start()
    for h in range(ways):
        for copy in along_z(h):
            copy.wait_recv()
        start_all(along_xy(h))
    for h in range(ways):
        for copy in along_xy(h):
            copy.wait_recv()
        along_core(h).start()
    out_in.wait()

    def product(core):
        total = jnp.zeros((rep_count * req, slice_dev), f32)
        for k in range(y):
            rows = gall.at[k, core].reshape(rep_count * req, inner_dev)[...]
            at = pl.multiple_of((k * c + core) * inner_dev, LANES)
            total += jnp.dot(rows, s["outw"][pl.ds(at, inner_dev)], preferred_element_type=f32)
        return total

    mixed = product(mc)
    for h in range(ways):
        along_core(h).wait_recv()
    residual = tok_all[...].astype(f32) + mixed + product(1 - mc)
    home_ref.reshape(count * tok_dev, slice_dev)[...] = residual.astype(bf16)
    gained = residual * gain[1:2]
    stat = lax.dot_general(
        gained, s["router"][...], (((1,), (1,)), ((), ())), preferred_element_type=f32,
        precision=lax.Precision.HIGHEST,
    )
    squares = jnp.sum(residual * residual, axis=1, keepdims=True)
    lane = column_iota(stat.shape, 1)
    stat = jnp.where(lane == router_ref.shape[0], squares, stat)
    stat_ref[...] = stat.reshape(rep_count, req, LANES)
    for e in range(experts):
        slots_ref[e] = lax.dot_general(
            s["maps"][e], gained.astype(bf16), (((0,), (0,)), ((), ())), preferred_element_type=f32
        ).astype(bf16)

    if tail:
        expert_part(
            expert_red, es, 0, experts_all, width, slots_ref, home_ref, stat_ref,
            idsall_ref.reshape(count * tok_dev, LANES), hid_ref, mamba_ref,
        )
    for copy in sel_copies + scale_copies + part_copies + pre_copies:
        copy.wait_send()

    def step_sent(k, _):
        @pl.when(jnp.logical_not(step_is_me(k)))
        def _():
            step_copy(k).wait_send()

        return 0

    lax.fori_loop(0, x * tp_count, step_sent, 0)

    def pack_sent(k, _):
        @pl.when(jnp.logical_not(is_me(k)))
        def _():
            pack_copy(k).wait_send()

        return 0

    lax.fori_loop(0, rep_count, pack_sent, 0)

    def act_sent(i, _):
        for copy in act_copies(i):
            copy.wait_send()
        return 0

    lax.fori_loop(0, red.chunks, act_sent, 0)
    for h in range(ways):
        for copy in along_z(h) + along_xy(h) + [along_core(h)]:
            copy.wait_send()
    scatter_wait(idsall_ref, s["idss"], 0, count)
    scatter_wait(tokall, s["toks"], 0, count)
    state_out.wait()


def mixer(args, expert_w, experts_all, rep_count, tp_count):
    tok, ids, gains, weight, skip, bias, decay, sel, history, router = args[:10]
    step_proj, w, state, out_w = args[10:]
    experts, hidden_dev = expert_w.shape[1], expert_w.shape[3] // tp_count
    f32, bf16 = jnp.float32, jnp.bfloat16
    count = rep_count * tp_count
    tok_dev = tok.shape[0]
    slice_dev = tok.shape[1] // count
    pieces = (count, tok_dev, slice_dev)
    packed_rows = weight.shape[0] + skip.shape[0] + 1 + decay.shape[0]
    packed = (packed_rows + -packed_rows % 16, decay.shape[1])
    req, states, inner_dev = state.shape
    red = Reduce(rep_count, tp_count, 2 * req, inner_dev, 0)
    n = red.chunks = red.per
    dma = pltpu.SemaphoreType.DMA
    vmem = pltpu.VMEM
    z, x, y, c = red.z, red.x, red.y, red.c
    tokens = count * tok_dev
    ways = CORES
    expert_rows = 2 * count * CAPACITY // rep_count
    expert_red = Reduce(rep_count, tp_count, expert_rows, hidden_dev, 0)
    expert_red.chunks = expert_red.per * experts
    held = sum(r.chunks * r.chunk_bytes() for r in (red, expert_red)) + 2 * (w.size + expert_w.size)
    fused = held <= ROOM
    scratch = red.scratch(2 * slice_dev)
    scratch.update(
        left=vmem((2 * tokens, 2 * slice_dev), bf16),
        scale=vmem((tok_dev, LANES), f32),
        scales=vmem((tp_count, tok_dev, LANES), f32),
        tok=vmem(pieces, bf16),
        ids=vmem((tok_dev, LANES), bf16),
        packed=vmem(packed, bf16),
        tokall=vmem(pieces, bf16),
        packall=vmem((rep_count,) + packed, bf16),
        par=vmem((packed[0], inner_dev), f32),
        stepz=vmem((LANES // step_proj.shape[0], step_proj.shape[0], inner_dev), bf16),
        sel=vmem((x,) + sel.shape, bf16),
        router=vmem((LANES, slice_dev), f32),
        maps=vmem((experts, tokens, count * CAPACITY), bf16),
        gate=vmem((req, inner_dev), f32),
        act=vmem((req, inner_dev), f32),
        actall=vmem((z, req, inner_dev), bf16),
        parts=vmem((tp_count, z * req, LANES), bf16),
        picks=vmem((z, req, LANES), f32),
        picked=vmem((z, req, LANES), f32),
        pre=vmem((z, req, inner_dev), bf16),
        preall=vmem((z, req, inner_dev), bf16),
        bc=vmem((LANES, LANES), f32),
        step=vmem((req, inner_dev), f32),
        read=vmem((req, inner_dev), f32),
        state=vmem(state.shape, f32),
        outw=vmem(out_w.shape, bf16),
        gall=vmem((y, c, z, x, req, inner_dev), bf16),
        toks=dma((2,)),
        idss=dma((2,)),
        pts=dma((2, tp_count - 1)),
        mzs=dma((2, z - 1)),
        pzs=dma((2, z - 1)),
        scs=dma((2, tp_count - 1)),
        sts=dma((2, max(x * tp_count, x * sel.shape[0] // step_proj.shape[0]))),
        sxs=dma((2, x - 1)),
        pks=dma((2, rep_count)),
        own=dma((4,)),
        acs=dma((2, n, z - 1)),
        gzs=dma((2, ways, z - 1)),
        gxs=dma((2, ways, x * y - 1)),
        gcs=dma((2, ways)),
    )
    shape = jax.ShapeDtypeStruct
    anywhere = pl.BlockSpec(memory_space=pl.ANY)
    home, stat = pieces, (rep_count, req, LANES)
    slots = (experts, count * CAPACITY, slice_dev)
    idsall = (count, tok_dev, LANES)
    outs = [shape(history.shape, bf16), shape(state.shape, f32)]
    tail, names = None, tuple(scratch)
    if fused:
        scratch["home"] = vmem(home, bf16)
        scratch["stat"] = vmem(stat, f32)
        scratch["slots"] = vmem(slots, bf16)
        scratch["idsall"] = vmem(idsall, bf16)
        names = tuple(scratch)
        more = expert_scratch(expert_red, 2 * slice_dev, experts, stat, home)
        tail = (expert_red, tuple(more), experts_all)
        outs += [
            shape((experts, expert_rows // 2, hidden_dev), bf16), shape(tok.shape, bf16)
        ]
        args = args + (expert_w,)
        spaces = list(scratch.values()) + list(more.values())
    else:
        outs += [shape(home, bf16), shape(stat, f32), shape(slots, bf16), shape(idsall, bf16)]
        spaces = list(scratch.values())
    got = pl.pallas_call(
        functools.partial(mixer_kernel, red, names, experts, tail),
        out_shape=outs,
        in_specs=in_vmem(10) + [anywhere] * (len(args) - 10),
        out_specs=in_vmem(1) + [anywhere] + in_vmem(len(outs) - 2),
        scratch_shapes=spaces,
        compiler_params=pltpu.CompilerParams(
            collective_id=0, has_side_effects=True, vmem_limit_bytes=62 * 2**20
        ),
        name="mixer",
    )(*args)
    if fused:
        return got
    home, stat, slots, idsall = got[2:]
    hidden, mamba = last_stage(
        slots, home, stat, idsall.reshape(tokens, LANES), expert_w, experts_all,
        tok.shape[1], rep_count, tp_count, hidden_dev,
    )
    return got[0], got[1], hidden, mamba


def expert_fetch(red, s, begin, w_ref):
    for i in range(red.chunks):
        expert, column = divmod(begin + i, red.per)
        red.fetch(
            s, w_ref, i, column * 2 * red.half,
            lambda w, at, expert=expert: w.at[:, expert, :, at],
        )


def last_kernel(
    red, names, begin, extra, experts_all, width, x_ref, home_ref, stat_ref, ids_ref, w_ref, hid_ref, *refs
):
    outs = 1 if extra else 0
    s = dict(zip(names, refs[outs:]))
    red.place()
    expert_fetch(red, s, begin, w_ref)
    count = red.z * red.x * red.y * red.c
    greet_all(count, red.rep * red.y * red.c + red.tp, red.y * red.c)
    mamba_ref = refs[0] if extra else None
    expert_part(
        red, s, begin, experts_all, width, x_ref, home_ref, stat_ref, ids_ref, hid_ref, mamba_ref
    )


def expert_part(
    red, s, begin, experts_all, width, x_ref, home_ref, stat_ref, ids_ref, hid_ref, mamba_ref
):
    extra = mamba_ref is not None
    tp_count, rep_count = red.y * red.c, red.z * red.x
    count = tp_count * rep_count
    rep, tp = red.rep, red.tp
    me = rep * tp_count + tp
    wide = 2 * red.half
    homes_ref = s["homes"] if extra else None
    for expert in range(x_ref.shape[0]):
        s["left"][expert] = spread(x_ref[expert], red.rows // 2, 2)

    def left_of(i):
        return s["left"][lax.div(begin + i, red.per)]

    req = red.rows // 2
    stats_ref = s["stats"]
    tok_dev = home_ref.shape[1]
    experts = x_ref.shape[0]

    def gates():
        for which in range(2):
            scatter_wait(stats_ref, s["sas"], which, count)
        summed = stats_ref[0]
        for k in range(1, count):
            summed += stats_ref[k]
        tokens = tp_count * tok_dev
        ids = ids_ref[pl.ds(pl.multiple_of(rep * tokens, 8), tokens)]
        lane = lax.broadcasted_iota(jnp.int32, (tokens, LANES), 1)
        first, second = named(ids, lane)
        scale = lax.rsqrt(summed[:, experts_all : experts_all + 1] / width + epsilon)
        logits = summed * scale
        one = jnp.sum(jnp.where(first, logits, 0.0), axis=1, keepdims=True)
        two = jnp.sum(jnp.where(second, logits, 0.0), axis=1, keepdims=True)
        gate = jnp.where(first, 1.0 / (1.0 + jnp.exp(two - one)), 0.0)
        gate += jnp.where(second, 1.0 / (1.0 + jnp.exp(one - two)), 0.0)
        gate = jnp.where(lane == LANES - 1, scale, gate)
        for e, taken in enumerate(slot_maps(ids, experts, tok_dev)):
            row = lax.dot_general(
                taken, gate, (((0,), (0,)), ((), ())), preferred_element_type=jnp.float32,
                precision=lax.Precision.HIGHEST,
            )
            seat = row[:, e : e + 1].astype(jnp.bfloat16).astype(jnp.float32)
            s["seat"][e] = jnp.broadcast_to(seat, s["seat"].shape[1:])
            s["size"][e] = jnp.broadcast_to(row[:, LANES - 1 :], s["size"].shape[1:])

    def store(i, h, total):
        expert = lax.div(begin + i, red.per)
        column = lax.rem(begin + i, red.per) * wide + h * red.half
        size = s["size"][expert][:, :1]
        up = total[req:] * size
        hidden = s["seat"][expert][:, :1] * silu(total[:req] * size) * up
        at = pl.ds(pl.multiple_of(column, LANES), red.half)
        hid_ref[expert, :, at] = hidden.astype(jnp.bfloat16)

    def send_home():
        scatter_start(home_ref, homes_ref, s["hos"], count, me, tp_count)
        homes_ref[me] = home_ref[me]

    def send_stats():
        def one(step, _):
            to = lax.rem(me + step, count)
            pltpu.make_async_remote_copy(
                src_ref=stat_ref.at[lax.div(to, tp_count)],
                dst_ref=stats_ref.at[me],
                send_sem=s["sas"].at[0],
                recv_sem=s["sas"].at[1],
                device_id=device_of(to, tp_count),
                device_id_type=MESH,
            ).start()
            return 0

        lax.fori_loop(1, count, one, 0)
        stats_ref[me] = stat_ref[rep]

    lags = (2, 4, 6, 8)
    extras = [(0, send_stats), (lags[3] - 1, gates)]
    if extra:
        extras.append((2, send_home))
    red.run(s, left_of, store, lags, extras)
    if extra:
        for which in range(2):
            scatter_wait(homes_ref, s["hos"], which, count)
        slice_dev = homes_ref.shape[2]
        for k in range(count):
            mamba_ref[:, k * slice_dev : (k + 1) * slice_dev] = homes_ref[k]


def expert_scratch(red, depth, experts, stat, home):
    bf16, f32 = jnp.bfloat16, jnp.float32
    dma = pltpu.SemaphoreType.DMA
    rep_count, tp_count = red.z * red.x, red.y * red.c
    scratch = red.scratch(depth)
    scratch["left"] = pltpu.VMEM((experts, rep_count * red.rows, depth), bf16)
    scratch["sas"] = dma((2,))
    scratch["stats"] = pltpu.VMEM((rep_count * tp_count,) + stat[1:], f32)
    scratch["seat"] = pltpu.VMEM((experts, red.rows // 2, LANES), f32)
    scratch["size"] = pltpu.VMEM((experts, red.rows // 2, LANES), f32)
    if home is not None:
        scratch["hos"] = dma((2,))
        scratch["homes"] = pltpu.VMEM(home, bf16)
    return scratch


def last_stage(slots, home, stat, ids, w, experts_all, width, rep_count, tp_count, hidden_dev):
    bf16 = jnp.bfloat16
    experts, total_rows, slice_dev = slots.shape
    rows = 2 * total_rows // rep_count
    shape = jax.ShapeDtypeStruct
    full = Reduce(rep_count, tp_count, rows, hidden_dev, 0)
    total = full.per * experts
    most = max(1, ROOM // (full.chunk_bytes() + 2 * w.size // total))
    begin, ups = 0, None
    while begin < total:
        red = Reduce(rep_count, tp_count, rows, hidden_dev, min(most, total - begin))
        extra = begin == 0
        scratch = expert_scratch(
            red, 2 * slice_dev, experts, stat.shape, home.shape if extra else None
        )
        outs = [shape((experts, rows // 2, hidden_dev), bf16)]
        if extra:
            outs += [shape((home.shape[1], width), bf16)]
        got = pl.pallas_call(
            functools.partial(last_kernel, red, tuple(scratch), begin, extra, experts_all, width),
            out_shape=outs,
            in_specs=in_vmem(4) + [pl.BlockSpec(memory_space=pl.ANY)],
            out_specs=in_vmem(len(outs)),
            scratch_shapes=list(scratch.values()),
            compiler_params=pltpu.CompilerParams(
                collective_id=10 + begin, has_side_effects=True, vmem_limit_bytes=62 * 2**20
            ),
            name="last_stage",
        )(slots, home, stat, ids, w)
        if extra:
            ups, homes = got
        else:
            edge = begin // full.per
            column = (begin % full.per) * 2 * full.half
            at = lax.broadcasted_iota(jnp.int32, (experts, 1, hidden_dev), 2)
            order = lax.broadcasted_iota(jnp.int32, (experts, 1, hidden_dev), 0)
            older = (order < edge) | ((order == edge) & (at < column))
            ups = jnp.where(older, ups, got[0])
        begin += red.chunks
    return ups, homes


def finish_kernel(
    experts, next_ref, mamba_ref, hid_ref, state_ref,
    next_out, mamba_out, hid_out, state_out, held, sems
):
    parts = sems.shape[1]
    size = state_ref.shape[0] // parts

    def move(k, which):
        at = pl.ds(k * size, size)
        if which == 0:
            return pltpu.make_async_copy(state_ref.at[at], held.at[at], sems.at[0, k])
        return pltpu.make_async_copy(held.at[at], state_out.at[at], sems.at[1, k])

    for k in range(parts):
        move(k, 0).start()
    next_out[...] = next_ref[...]
    mamba_out[...] = mamba_ref[...]
    rows = hid_out.shape[0]
    to, source = column_iota((rows, rows), 0), column_iota((rows, rows), 1)
    block, seat = lax.div(to, experts * CAPACITY), lax.rem(to, CAPACITY)
    expert = lax.rem(lax.div(to, CAPACITY), experts)
    moves = source == expert * (rows // experts) + block * CAPACITY + seat
    hid_out[...] = jnp.dot(
        moves.astype(jnp.bfloat16), hid_ref[...], preferred_element_type=jnp.float32
    ).astype(jnp.bfloat16)
    for k in range(parts):
        move(k, 0).wait()
        move(k, 1).start()
    for k in range(parts):
        move(k, 1).wait()


def finish(conv_next, mamba, hidden, state, experts):
    anywhere = pl.BlockSpec(memory_space=pl.ANY)
    arrays = (conv_next, mamba, hidden, state)
    return pl.pallas_call(
        functools.partial(finish_kernel, experts),
        out_shape=[jax.ShapeDtypeStruct(array.shape, array.dtype) for array in arrays],
        in_specs=in_vmem(3) + [anywhere],
        out_specs=in_vmem(3) + [anywhere],
        scratch_shapes=[
            pltpu.VMEM(state.shape, state.dtype), pltpu.SemaphoreType.DMA((2, 4))
        ],
        name="finish",
    )(*arrays)


def shards(
    tokens,
    conv_state,
    ssm_state,
    norm_gains,
    conv_weight,
    conv_skip,
    step_bias,
    decay_log,
    input_proj,
    select_proj,
    step_proj,
    output_proj,
    router,
    expert_proj,
    expert_ids,
):
    tp_count = lax.axis_size("tp")
    rep_count = lax.axis_size("rep")
    args = (
        tokens, expert_ids, norm_gains, conv_weight, conv_skip, step_bias, decay_log,
        select_proj.T, conv_state, router.T, step_proj, input_proj, ssm_state, output_proj,
    )
    conv_next, ssm_next, hidden, mamba = mixer(
        args, expert_proj, router.shape[1], rep_count, tp_count
    )
    hidden = hidden.reshape(-1, hidden.shape[2])
    conv_next, mamba_out, expert_hidden, ssm_next = finish(
        conv_next, mamba, hidden, ssm_next, expert_proj.shape[1]
    )
    return (mamba_out, conv_next, ssm_next, expert_hidden)


def solution(mesh):
    in_specs = (
        P(("rep", "tp"), None),
        P(None, "rep", "tp"),
        P("rep", None, "tp"),
        P(None, ("rep", "tp")),
        P(None, ("rep", "tp")),
        P(None, ("rep", "tp")),
        P(("rep", "tp")),
        P(None, ("rep", "tp")),
        P(("rep", "tp"), None, None),
        P("tp", "rep"),
        P(("rep", "tp"), None),
        P(None, ("rep", "tp")),
        P(("rep", "tp"), None),
        P(("rep", "tp"), None, None, None),
        P(("rep", "tp"), None),
    )
    out_specs = (P(("rep", "tp"), None), P(None, "rep", "tp"), P("rep", None, "tp"), P("rep", "tp"))
    return jax.shard_map(shards, mesh=mesh, in_specs=in_specs, out_specs=out_specs, check_vma=False)
```

```python
import functools

import jax
import jax.numpy as jnp
from jax import lax
from jax.experimental import pallas as pl
from jax.experimental.pallas import tpu as pltpu
from jax.sharding import PartitionSpec as P

CAPACITY = 2
LANES = 128


epsilon = 1e-05
MESH = pl.DeviceIdType.MESH


CORES = 2
LANE_PAIR = 2
ROOM = 40 * 2**20


def split_of(rep_count, tp_count):
    return rep_count // CORES, CORES, tp_count // CORES, CORES


def start_all(copies):
    for copy in copies:
        copy.start()


class Reduce:
    def __init__(self, rep_count, tp_count, rows, dev_cols, total_chunks):
        self.z, self.x, self.y, self.c = split_of(rep_count, tp_count)
        self.rows = rows
        self.half = 2 * LANES if dev_cols % (4 * LANES) == 0 else LANES
        self.per = dev_cols // (2 * self.half)
        self.dev_cols = dev_cols
        self.chunks = total_chunks
        self.mix = 0
        self.blocks = self.z * self.x * self.y

    def chunk_bytes(self):
        return self.c * 2 * self.blocks * self.rows * self.half * 2 * 2

    def scratch(self, depth):
        n, z, x, y, rows, half = self.chunks, self.z, self.x, self.y, self.rows, self.half
        bf16 = jnp.bfloat16
        groups = self.c * y * 2 * (half // LANES)
        dma = pltpu.SemaphoreType.DMA
        buffers = dict(
            w=pltpu.VMEM((n, groups, depth // 2, 2, LANES), bf16),
            b0=pltpu.VMEM((n, self.c, 2, self.blocks, rows, half), bf16),
            r0=pltpu.VMEM((n, 2, self.blocks, rows, half), bf16),
            r1a=pltpu.VMEM((n, y - 1, x * z, rows, half), bf16),
            r1b=pltpu.VMEM((n, x - 1, y * z, rows, half), bf16),
            r2a=pltpu.VMEM((n, x - 1, z, rows, half), bf16),
            r2b=pltpu.VMEM((n, y - 1, z, rows, half), bf16),
            b3=pltpu.VMEM((n, z, 2, rows, half), bf16),
            r3=pltpu.VMEM((n, z - 1, 2, rows, half), bf16),
            ws=dma((n,)),
            s0=dma((2, n)),
            s1a=dma((2, n, y - 1)),
            s1b=dma((2, n, x - 1)),
            s2a=dma((2, n, x - 1)),
            s2b=dma((2, n, y - 1)),
            s3=dma((2, n, z - 1)),
        )
        if self.mix:
            m, far = -(-n // self.mix), z // 2
            buffers.update(
                rz=pltpu.VMEM((m, 2, self.blocks // 2, rows, half), bf16),
                q1a=pltpu.VMEM((m, x - 1, y * far, rows, half), bf16),
                q1b=pltpu.VMEM((m, y - 1, x * far, rows, half), bf16),
                q2a=pltpu.VMEM((m, y - 1, far, rows, half), bf16),
                q2b=pltpu.VMEM((m, x - 1, far, rows, half), bf16),
                c3=pltpu.VMEM((m, far, 2, rows, half), bf16),
                d3=pltpu.VMEM((m, far - 1, 2, rows, half), bf16),
                sz=dma((2, m, 2)),
                t1a=dma((2, m, x - 1)),
                t1b=dma((2, m, y - 1)),
                t2a=dma((2, m, y - 1)),
                t2b=dma((2, m, x - 1)),
                t3=dma((2, m, far - 1)),
            )
        return buffers

    def mixed_copies(self, s, e, stage):
        z, x, y = self.z, self.x, self.y
        far, low, high = z // 2, lax.rem(self.mz, 2), lax.div(self.mz, 2)
        if stage == 1:
            size = self.blocks // 2
            return [
                remote(
                    s["r0"].at[e * self.mix, h, pl.ds((1 - low) * size, size)],
                    s["rz"].at[e, h], s["sz"].at[0, e, h], s["sz"].at[1, e, h],
                    self.peer_z(high * 2 + 1 - low),
                )
                for h in range(2)
            ]
        if stage == 2:
            return self.exchange(
                s["rz"].at[e, 0], x, self.mx, y * far, s["q1a"], s["t1a"], e, self.peer_x
            ) + self.exchange(
                s["rz"].at[e, 1], y, self.my, x * far, s["q1b"], s["t1b"], e, self.peer_y
            )
        if stage == 3:
            return self.exchange(
                s["q1a"].at[e, 0], y, self.my, far, s["q2a"], s["t2a"], e, self.peer_y
            ) + self.exchange(
                s["q1b"].at[e, 0], x, self.mx, far, s["q2b"], s["t2b"], e, self.peer_x
            )
        out = []
        for step in range(1, far):
            to = lax.rem(high + step, far)
            out.append(
                remote(
                    s["c3"].at[e, to], s["d3"].at[e, step - 1],
                    s["t3"].at[0, e, step - 1], s["t3"].at[1, e, step - 1],
                    self.peer_z(to * 2 + low),
                )
            )
        return out

    def mixed_core(self, s, i):
        for copy in self.copies(s, i, 0):
            copy.wait_recv()
        for h in range(2):
            self.add(s["r0"].at[i, h], [s["b0"].at[i, self.mc, h]])
        start_all(self.mixed_copies(s, lax.div(i, self.mix), 1))

    def mixed_near(self, s, i):
        e = lax.div(i, self.mix)
        for copy in self.mixed_copies(s, e, 1):
            copy.wait_recv()
        size, low = self.blocks // 2, lax.rem(self.mz, 2)
        for h in range(2):
            self.add(s["rz"].at[e, h], [s["r0"].at[i, h, pl.ds(low * size, size)]])
        start_all(self.mixed_copies(s, e, 2))

    def mixed_first(self, s, i):
        e = lax.div(i, self.mix)
        for copy in self.mixed_copies(s, e, 2):
            copy.wait_recv()
        far = self.z // 2
        for h, name, me, size, count in (
            (0, "q1a", self.mx, self.y * far, self.x),
            (1, "q1b", self.my, self.x * far, self.y),
        ):
            others = [s[name].at[e, k] for k in range(1, count - 1)]
            others.append(s["rz"].at[e, h, pl.ds(me * size, size)])
            self.add(s[name].at[e, 0], others)
        start_all(self.mixed_copies(s, e, 3))

    def mixed_second(self, s, i):
        e = lax.div(i, self.mix)
        for copy in self.mixed_copies(s, e, 3):
            copy.wait_recv()
        far = self.z // 2
        for h, name, came, me, count in (
            (0, "q2a", "q1a", self.my, self.y),
            (1, "q2b", "q1b", self.mx, self.x),
        ):
            for k in range(far):
                total = s[came][e, 0, me * far + k].astype(jnp.float32)
                for j in range(count - 1):
                    total += s[name][e, j, k].astype(jnp.float32)
                s["c3"][e, k, h] = total.astype(jnp.bfloat16)
        start_all(self.mixed_copies(s, e, 4))

    def mixed_last(self, s, i, store, done):
        e = lax.div(i, self.mix)
        for copy in self.mixed_copies(s, e, 4):
            copy.wait_recv()
        for h in range(2):
            total = s["c3"][e, lax.div(self.mz, 2), h].astype(jnp.float32)
            for k in range(self.z // 2 - 1):
                total += s["d3"][e, k, h].astype(jnp.float32)
            store(i, h, total)
        done(i)

    def is_mixed(self, i):
        return lax.rem(i, self.mix) == 0

    def place(self):
        rep, tp = lax.axis_index("rep"), lax.axis_index("tp")
        self.rep, self.tp = rep, tp
        self.mz, self.mx = lax.div(rep, self.x), lax.rem(rep, self.x)
        self.my, self.mc = lax.div(tp, self.c), lax.rem(tp, self.c)

    def peer_z(self, to):
        return {"rep": to * self.x + self.mx}

    def peer_x(self, to):
        return {"rep": self.mz * self.x + to}

    def peer_y(self, to):
        return {"tp": to * self.c + self.mc}

    def peer_c(self):
        return {"tp": self.my * self.c + 1 - self.mc}

    def peers(self):
        out = [self.peer_c()]
        out += [self.peer_y(lax.rem(self.my + s, self.y)) for s in range(1, self.y)]
        out += [self.peer_x(lax.rem(self.mx + s, self.x)) for s in range(1, self.x)]
        out += [self.peer_z(lax.rem(self.mz + s, self.z)) for s in range(1, self.z)]
        return out

    def exchange(self, source, count, me, size, target, sems, i, peer):
        copies = []
        for step in range(1, count):
            to = lax.rem(me + step, count)
            copies.append(
                pltpu.make_async_remote_copy(
                    src_ref=source.at[pl.ds(to * size, size)],
                    dst_ref=target.at[i, step - 1],
                    send_sem=sems.at[0, i, step - 1],
                    recv_sem=sems.at[1, i, step - 1],
                    device_id=peer(to),
                    device_id_type=MESH,
                )
            )
        return copies

    def copies(self, s, i, stage):
        z, x, y = self.z, self.x, self.y
        if stage == 0:
            return [
                pltpu.make_async_remote_copy(
                    src_ref=s["b0"].at[i, 1 - self.mc],
                    dst_ref=s["r0"].at[i],
                    send_sem=s["s0"].at[0, i],
                    recv_sem=s["s0"].at[1, i],
                    device_id=self.peer_c(),
                    device_id_type=MESH,
                )
            ]
        if stage == 1:
            return self.exchange(
                s["r0"].at[i, 0], y, self.my, x * z, s["r1a"], s["s1a"], i, self.peer_y
            ) + self.exchange(
                s["r0"].at[i, 1], x, self.mx, y * z, s["r1b"], s["s1b"], i, self.peer_x
            )
        if stage == 2:
            return self.exchange(
                s["r1a"].at[i, 0], x, self.mx, z, s["r2a"], s["s2a"], i, self.peer_x
            ) + self.exchange(
                s["r1b"].at[i, 0], y, self.my, z, s["r2b"], s["s2b"], i, self.peer_y
            )
        third = []
        for step in range(1, z):
            to = lax.rem(self.mz + step, z)
            third.append(
                pltpu.make_async_remote_copy(
                    src_ref=s["b3"].at[i, to],
                    dst_ref=s["r3"].at[i, step - 1],
                    send_sem=s["s3"].at[0, i, step - 1],
                    recv_sem=s["s3"].at[1, i, step - 1],
                    device_id=self.peer_z(to),
                    device_id_type=MESH,
                )
            )
        return third

    def fetch(self, s, w_ref, i, column, pick):
        wide = 2 * self.half
        for y in range(self.y):
            for c in range(self.c):
                for k in range(wide // LANES):
                    at = (y * self.c + c) * self.dev_cols + column + k * LANES
                    at = pl.ds(pl.multiple_of(at, LANES), LANES)
                    pltpu.make_async_copy(
                        pick(w_ref, at),
                        s["w"].at[i, (y * self.c + c) * (wide // LANES) + k],
                        s["ws"].at[i],
                    ).start()

    def multiply(self, s, i, left, mixed):
        w = s["w"]
        pltpu.make_async_copy(w.at[i], w.at[i], s["ws"].at[i]).wait()
        depth = w.shape[2] * 2
        pieces = self.half // LANES
        for y in range(self.y):
            for c in range(self.c):
                for h in range(2):
                    first = ((y * self.c + c) * 2 + h) * pieces
                    right = [
                        w.at[i, first + k].reshape(depth, LANES)[...] for k in range(pieces)
                    ]
                    right = jnp.concatenate(right, axis=1) if pieces > 1 else right[0]
                    got = jnp.dot(left, right, preferred_element_type=jnp.float32)
                    got = got.astype(jnp.bfloat16)
                    got = got.reshape(self.z, self.x, self.rows, self.half)
                    self.put(s, i, c, h, y, got, mixed)
        start_all(self.copies(s, i, 0))

    def put(self, s, i, c, h, y, got, mixed):
        if not mixed:
            for x in range(self.x):
                at = (y * self.x + x) if h == 0 else (x * self.y + y)
                s["b0"][i, c, h, at * self.z : (at + 1) * self.z] = got[:, x]
            return
        far = self.z // 2
        split = got.reshape(far, 2, self.x, self.rows, self.half)
        for x in range(self.x):
            pair = (x * self.y + y) if h == 0 else (y * self.x + x)
            for low in range(2):
                at = (low * self.x * self.y + pair) * far
                s["b0"][i, c, h, at : at + far] = split[:, low, x]

    def add(self, target, others):
        def piece(k, _):
            total = target[k].astype(jnp.float32)
            for other in others:
                total += other[k].astype(jnp.float32)
            target[k] = total.astype(jnp.bfloat16)
            return 0

        lax.fori_loop(0, target.shape[0], piece, 0, unroll=min(4, target.shape[0]))

    def after_core(self, s, i):
        for copy in self.copies(s, i, 0):
            copy.wait_recv()
        for h in range(2):
            self.add(s["r0"].at[i, h], [s["b0"].at[i, self.mc, h]])
        start_all(self.copies(s, i, 1))

    def after_first(self, s, i):
        for copy in self.copies(s, i, 1):
            copy.wait_recv()
        z = self.z
        for h, name, me, size, count in (
            (0, "r1a", self.my, self.x * z, self.y),
            (1, "r1b", self.mx, self.y * z, self.x),
        ):
            others = [s[name].at[i, k] for k in range(1, count - 1)]
            others.append(s["r0"].at[i, h, pl.ds(me * size, size)])
            self.add(s[name].at[i, 0], others)
        start_all(self.copies(s, i, 2))

    def after_second(self, s, i):
        for copy in self.copies(s, i, 2):
            copy.wait_recv()
        for h, name, came, me, count in (
            (0, "r2a", "r1a", self.mx, self.x),
            (1, "r2b", "r1b", self.my, self.y),
        ):
            for k in range(self.z):
                total = s[came][i, 0, me * self.z + k].astype(jnp.float32)
                for j in range(count - 1):
                    total += s[name][i, j, k].astype(jnp.float32)
                s["b3"][i, k, h] = total.astype(jnp.bfloat16)
        start_all(self.copies(s, i, 3))

    def after_third(self, s, i, store, done):
        for copy in self.copies(s, i, 3):
            copy.wait_recv()
        for h in range(2):
            total = s["b3"][i, self.mz, h].astype(jnp.float32)
            for k in range(self.z - 1):
                total += s["r3"][i, k, h].astype(jnp.float32)
            store(i, h, total)
        done(i)

    def finish(self, s):
        def one(i, _):
            for copy in self.copies(s, i, 0):
                copy.wait_send()

            def plain():
                for stage in range(1, 4):
                    for copy in self.copies(s, i, stage):
                        copy.wait_send()

            def mixed():
                for stage in range(1, 5):
                    for copy in self.mixed_copies(s, lax.div(i, self.mix), stage):
                        copy.wait_send()

            if not self.mix:
                plain()
            else:
                pl.when(self.is_mixed(i))(mixed)
                pl.when(jnp.logical_not(self.is_mixed(i)))(plain)
            return 0

        lax.fori_loop(0, self.chunks, one, 0)

    def run(self, s, left_of, store, lags, extras=(), done=lambda i: None):
        n = self.chunks
        plain = (
            None,
            lambda i: self.after_third(s, i, store, done),
            lambda i: self.after_second(s, i),
            lambda i: self.after_first(s, i),
            lambda i: self.after_core(s, i),
        )
        mixed = (
            lambda i: self.mixed_last(s, i, store, done),
            lambda i: self.mixed_second(s, i),
            lambda i: self.mixed_first(s, i),
            lambda i: self.mixed_near(s, i),
            lambda i: self.mixed_core(s, i),
        )
        after = lags[3] + lags[3] - lags[2]
        stages = []
        for lag, one, two in zip((after,) + lags[::-1], plain, mixed):
            if one is not None:
                stages.append((lag, one, False))
            if self.mix:
                stages.append((lag, two, True))
        stages.append((0, lambda i: self.multiply(s, i, left_of(i), False), False))
        if self.mix:
            stages.append((0, lambda i: self.multiply(s, i, left_of(i), True), True))

        def step(t, _):
            for lag, work, kind in stages:
                now = (t >= lag) & (t < n + lag)
                if self.mix:
                    now = now & (self.is_mixed(t - lag + self.mix * lag) == kind)

                @pl.when(now)
                def _(lag=lag, work=work):
                    work(t - lag)
            for when, work in extras:
                pl.when(t == when)(work)
            return 0

        lax.fori_loop(0, n + (after if self.mix else lags[3]), step, 0)
        self.finish(s)


def spread(rows, per, pairs):
    count, depth = rows.shape
    lane = lax.broadcasted_iota(jnp.int32, (depth, depth * pairs), 1)
    source = lax.broadcasted_iota(jnp.int32, (depth, depth * pairs), 0)
    parts = []
    for j in range(pairs):
        moves = (lane == source * pairs + j).astype(jnp.bfloat16)
        part = jnp.dot(rows, moves, preferred_element_type=jnp.float32)
        parts.append(part.reshape(count // per, 1, per, depth * pairs))
    wide = jnp.concatenate(parts, axis=1)
    return wide.reshape(count * pairs, depth * pairs).astype(jnp.bfloat16)


def greet(ids):
    barrier = pltpu.get_barrier_semaphore()
    for device in ids:
        pl.semaphore_signal(barrier, inc=1, device_id=device, device_id_type=MESH)
    pl.semaphore_wait(barrier, len(ids))


def device_of(index, tp_count):
    return {"rep": lax.div(index, tp_count), "tp": lax.rem(index, tp_count)}


def greet_all(count, me, tp_count):
    barrier = pltpu.get_barrier_semaphore()

    def one(step, _):
        to = device_of(lax.rem(me + step, count), tp_count)
        pl.semaphore_signal(barrier, inc=1, device_id=to, device_id_type=MESH)
        return 0

    lax.fori_loop(1, count, one, 0)
    pl.semaphore_wait(barrier, count - 1)


def scatter_start(source, target, sems, count, me, tp_count):
    whole = len(source.shape) == len(target.shape) - 1

    def one(step, _):
        to = lax.rem(me + step, count)
        pltpu.make_async_remote_copy(
            src_ref=source if whole else source.at[to],
            dst_ref=target.at[me],
            send_sem=sems.at[0],
            recv_sem=sems.at[1],
            device_id=device_of(to, tp_count),
            device_id_type=MESH,
        ).start()
        return 0

    lax.fori_loop(1, count, one, 0)


def scatter_wait(target, sems, which, count):
    part = target.at[pl.ds(0, count - 1)]
    pltpu.make_async_copy(part, part, sems.at[which]).wait()


def in_vmem(count):
    return [pl.BlockSpec(memory_space=pltpu.VMEM)] * count


def remote(source, target, send_sem, recv_sem, device):
    return pltpu.make_async_remote_copy(
        src_ref=source,
        dst_ref=target,
        send_sem=send_sem,
        recv_sem=recv_sem,
        device_id=device,
        device_id_type=MESH,
    )


def silu(v):
    return v / (1.0 + jnp.exp(-v))


def softplus(v):
    return jnp.maximum(v, 0.0) + jnp.log1p(jnp.exp(-jnp.abs(v)))


def column_iota(shape, axis):
    return lax.broadcasted_iota(jnp.int32, shape, axis)


def named(ids, lane):
    ids = ids.astype(jnp.float32).astype(jnp.int32)
    return ids[:, :1] == lane, ids[:, 1:2] == lane


def slot_maps(ids, experts, tok_dev):
    rows = ids.shape[0]
    first, second = named(ids, column_iota((rows, LANES), 1))
    routed = (first | second).astype(jnp.float32)
    later, earlier = column_iota((rows, rows), 0), column_iota((rows, rows), 1)
    before = (earlier < later) & (lax.div(earlier, tok_dev) == lax.div(later, tok_dev))
    position = jnp.dot(
        before.astype(jnp.bfloat16), routed.astype(jnp.bfloat16), preferred_element_type=jnp.float32
    )
    slots = rows // tok_dev * CAPACITY
    row, slot = column_iota((rows, slots), 0), column_iota((rows, slots), 1)
    block = lax.div(row, tok_dev) == lax.div(slot, CAPACITY)
    seat = lax.rem(slot, CAPACITY).astype(jnp.float32)
    maps = []
    for e in range(experts):
        taken = block & (routed[:, e : e + 1] > 0.5) & (position[:, e : e + 1] == seat)
        maps.append(taken.astype(jnp.float32))
    return maps


def mixer_kernel(red, names, experts, tail, *refs):
    (
        tok_in_ref, ids_in_ref, gains_ref, weight_ref, skip_ref, bias_ref, decay_ref, sel_ref,
        history_ref, router_ref, step_ref, w_ref, state_ref, out_w_ref,
    ) = refs[:14]
    refs = refs[14:]
    if tail:
        expert_red, expert_names, experts_all = tail
        expert_w_ref, next_ref, state_out_ref, hid_ref, mamba_ref = refs[:5]
        scratch, expert_refs = refs[5 : 5 + len(names)], refs[5 + len(names) :]
    else:
        next_ref, state_out_ref, home_ref, stat_ref, slots_ref, idsall_ref = refs[:6]
        scratch = refs[6:]
    f32, bf16 = jnp.float32, jnp.bfloat16
    s = dict(zip(names, scratch))
    red.place()
    if tail:
        es = dict(zip(expert_names, expert_refs))
        expert_red.place()
        home_ref, stat_ref, slots_ref = s["home"], s["stat"], s["slots"]
        idsall_ref = s["idsall"]
    z, x, y, c = red.z, red.x, red.y, red.c
    mz, mx, my, mc = red.mz, red.mx, red.my, red.mc
    tp_count, rep_count = y * c, z * x
    count = tp_count * rep_count
    rep, tp = red.rep, red.tp
    me = rep * tp_count + tp
    inner_dev = red.dev_cols
    req = red.rows // 2
    tok_ref, ids_ref, packed_ref = s["tok"], s["ids"], s["packed"]
    tok_dev, slice_dev = tok_ref.shape[1:]
    tokall, packall, stepz = s["tokall"], s["packall"], s["stepz"]
    step_dev, part_cols = step_ref.shape[0], sel_ref.shape[0]
    group_cols = part_cols * x
    owners = group_cols // step_dev
    taps = history_ref.shape[0] + 1
    states = tap0 = state_ref.shape[1]

    state_in = pltpu.make_async_copy(state_ref, s["state"], s["own"].at[1])
    out_in = pltpu.make_async_copy(out_w_ref, s["outw"], s["own"].at[2])
    for i in range(red.chunks):
        red.fetch(s, w_ref, i, i * 2 * red.half, lambda w, at: w.at[:, :, at])
    state_in.start()
    out_in.start()
    for k in range(count):
        tok_ref[k] = tok_in_ref[:, k * slice_dev : (k + 1) * slice_dev]
    ids = ids_in_ref[...].astype(f32)
    ids = jnp.concatenate([ids, jnp.zeros((tok_dev, LANES - ids.shape[1]), f32)], axis=1)
    ids_ref[...] = ids.astype(bf16)
    rows = [ref[...].astype(f32) for ref in (decay_ref, weight_ref, skip_ref)]
    rows.append(bias_ref[...].astype(f32).reshape(1, -1))
    spare = packed_ref.shape[0] - sum(row.shape[0] for row in rows)
    rows.append(jnp.zeros((spare, packed_ref.shape[1]), f32))
    packed_ref[...] = jnp.concatenate(rows, axis=0).astype(bf16)
    tok = tok_in_ref[...].astype(f32)
    width = tok.shape[1]
    square = jnp.sum(tok * tok, axis=-1, keepdims=True)
    s["scale"][...] = jnp.broadcast_to(lax.rsqrt(square / width + epsilon), s["scale"].shape)
    stepz[...] = jnp.zeros(stepz.shape, bf16)
    greet_all(count, me, tp_count)
    scatter_start(tok_ref, tokall, s["toks"], count, me, tp_count)
    tokall[me] = tok_ref[me]
    slot = lax.rem(me, rep_count)
    home_tp = lax.div(me, rep_count)

    def pack_copy(to_rep):
        return remote(
            packed_ref, packall.at[slot], s["pks"].at[0, to_rep], s["pks"].at[1, slot],
            {"rep": to_rep, "tp": home_tp},
        )

    def is_me(to_rep):
        return (to_rep == rep) & (home_tp == tp)

    def pack_start(to_rep, _):
        @pl.when(is_me(to_rep))
        def _():
            packall[slot] = packed_ref[...]

        @pl.when(jnp.logical_not(is_me(to_rep)))
        def _():
            pack_copy(to_rep).start()

        return 0

    lax.fori_loop(0, rep_count, pack_start, 0)
    scale_copies = []
    for k in range(tp_count - 1):
        to = lax.rem(tp + k + 1, tp_count)
        scale_copies.append(
            remote(
                s["scale"], s["scales"].at[tp], s["scs"].at[0, k], s["scs"].at[1, k], {"tp": to}
            )
        )
    start_all(scale_copies)
    s["scales"][tp] = s["scale"][...]
    scatter_start(ids_ref, idsall_ref, s["idss"], count, me, tp_count)
    idsall_ref[me] = ids_ref[...]
    sel_copies = [
        remote(
            sel_ref, s["sel"].at[mx], s["sxs"].at[0, k], s["sxs"].at[1, k],
            red.peer_x(lax.rem(mx + k + 1, x)),
        )
        for k in range(x - 1)
    ]
    start_all(sel_copies)
    step_slot, step_home = lax.rem(me, owners), lax.div(me, owners)

    def step_target(k):
        return step_home * x + lax.div(k, tp_count), lax.rem(k, tp_count)

    def step_is_me(k):
        to_rep, to_tp = step_target(k)
        return (to_rep == rep) & (to_tp == tp)

    def step_source(to_tp):
        return step_ref.at[:, pl.ds(pl.multiple_of(to_tp * inner_dev, LANES), inner_dev)]

    def step_copy(k):
        to_rep, to_tp = step_target(k)
        return remote(
            step_source(to_tp), stepz.at[step_slot],
            s["sts"].at[0, k], s["sts"].at[1, step_slot], {"rep": to_rep, "tp": to_tp},
        )

    own_step = pltpu.make_async_copy(step_source(tp), stepz.at[step_slot], s["own"].at[0])

    def step_start(k, _):
        @pl.when(step_is_me(k))
        def _():
            own_step.start()

        @pl.when(jnp.logical_not(step_is_me(k)))
        def _():
            step_copy(k).start()

        return 0

    lax.fori_loop(0, x * tp_count, step_start, 0)

    s["sel"][mx] = sel_ref[...]
    s["router"][...] = jnp.zeros(s["router"].shape, f32)
    s["router"][: router_ref.shape[0]] = router_ref[...].astype(f32)
    next_ref[: taps - 2] = history_ref[1:]

    if tail:
        expert_fetch(expert_red, es, 0, expert_w_ref)
    scatter_wait(tokall, s["toks"], 1, count)
    tok_all = tokall.reshape(count * tok_dev, slice_dev)
    gain = gains_ref[...].astype(f32)
    x_rows = (tok_all[...].astype(f32) * gain[:1]).astype(bf16)
    s["left"][...] = spread(x_rows, req, 2)

    def weights():
        for copy in sel_copies:
            copy.wait_recv()

        def step_came(k, _):
            @pl.when((mz * owners + k != me) & (mz * owners + k < count))
            def _():
                pltpu.make_async_copy(stepz.at[k], stepz.at[k], s["sts"].at[1, k]).wait()

            return 0

        lax.fori_loop(0, owners, step_came, 0)

        def own_came(k, _):
            pl.when(step_is_me(k))(own_step.wait)
            return 0

        lax.fori_loop(0, x * tp_count, own_came, 0)

    def params():
        for copy in scale_copies:
            copy.wait_recv()

        def pack_came(k, _):
            @pl.when(tp * rep_count + k != me)
            def _():
                pltpu.make_async_copy(packall.at[k], packall.at[k], s["pks"].at[1, k]).wait()

            return 0

        lax.fori_loop(0, rep_count, pack_came, 0)
        own = packed_ref.shape[1]
        for k in range(rep_count):
            s["par"][:, k * own : (k + 1) * own] = packall[k].astype(f32)

    def maps():
        scatter_wait(idsall_ref, s["idss"], 1, count)
        ids = idsall_ref.reshape(count * tok_dev, LANES)[...]
        for e, taken in enumerate(slot_maps(ids, experts, tok_dev)):
            s["maps"][e] = taken.astype(bf16)

    def store(i, h, total):
        at = pl.ds(pl.multiple_of(i * 2 * red.half + h * red.half, LANES), red.half)
        scale = s["scales"].reshape(req, LANES)[:, :1]
        conv_input = total[:req] * scale
        s["gate"][:, at] = total[req:] * scale
        next_ref[taps - 2, :, at] = conv_input.astype(bf16)
        par = s["par"]
        mix = par[tap0 + taps - 1 : tap0 + taps, at] * conv_input
        mix += par[tap0 + taps : tap0 + taps + 1, at]
        for k in range(taps - 1):
            mix += par[tap0 + k : tap0 + k + 1, at] * history_ref[k, :, at].astype(f32)
        act = silu(mix)
        s["act"][:, at] = act
        s["actall"][mz, :, at] = act.astype(bf16)

    def act_copies(i):
        at = pl.ds(pl.multiple_of(i * 2 * red.half, LANES), 2 * red.half)
        block = s["actall"].at[mz, :, at]
        return [
            remote(
                block, block, s["acs"].at[0, i, k], s["acs"].at[1, i, k],
                red.peer_z(lax.rem(mz + k + 1, z)),
            )
            for k in range(z - 1)
        ]

    n = red.chunks
    lags = (1, n, n + 2, n + 4)
    extras = [(2, params), (2, maps), (n, weights)]
    red.run(
        s, lambda i: s["left"][...], store, lags, extras, lambda i: start_all(act_copies(i))
    )
    def act_came(i, _):
        for copy in act_copies(i):
            copy.wait_recv()
        return 0

    lax.fori_loop(0, red.chunks, act_came, 0)
    every = s["actall"].reshape(z * req, inner_dev)[...]
    part = jnp.zeros((z * req, LANES), f32)
    for k in range(x):
        cols = lax.dot_general(
            every, s["sel"][k], (((1,), (1,)), ((), ())), preferred_element_type=f32
        )
        spare = jnp.zeros((z * req, LANES - part_cols), f32)
        cols = jnp.concatenate([cols, spare], axis=1)
        part += pltpu.roll(cols, k * part_cols, 1) if k else cols
    s["parts"][tp] = part.astype(bf16)
    part_copies = [
        remote(
            s["parts"].at[tp], s["parts"].at[tp], s["pts"].at[0, k], s["pts"].at[1, k],
            {"tp": lax.rem(tp + k + 1, tp_count)},
        )
        for k in range(tp_count - 1)
    ]
    start_all(part_copies)
    for copy in part_copies:
        copy.wait_recv()
    selected = s["parts"][0].astype(f32)
    for k in range(1, tp_count):
        selected += s["parts"][k].astype(f32)
    s["picks"][...] = selected.reshape(z, req, LANES)
    if step_dev % 8 == 0:
        step_rows = stepz.reshape(LANES, inner_dev)[...]
    else:
        step_rows = stepz[...].reshape(LANES, inner_dev)
    pre = jnp.dot(selected.astype(bf16), step_rows, preferred_element_type=f32)
    s["pre"][...] = pre.astype(bf16).reshape(z, req, inner_dev)
    pre_copies = []
    for k in range(z - 1):
        to = lax.rem(mz + k + 1, z)
        for name, slots, sems in (("picks", "picked", "mzs"), ("pre", "preall", "pzs")):
            pre_copies.append(
                remote(
                    s[name].at[to], s[slots].at[mz], s[sems].at[0, k], s[sems].at[1, k],
                    red.peer_z(to),
                )
            )
    start_all(pre_copies)
    s["picked"][mz] = s["picks"][mz]
    s["preall"][mz] = s["pre"][mz]
    for copy in pre_copies:
        copy.wait_recv()
    rank = step_dev * count
    maps_z, maps_lane = divmod(rank, group_cols)
    both = jnp.concatenate(
        [s["picked"][maps_z], jnp.zeros((LANES - req, LANES), f32)], axis=0
    )
    s["bc"][...] = (pltpu.roll(both, LANES - maps_lane, 1) if maps_lane else both).T
    step_pre = s["preall"][0].astype(f32)
    for k in range(1, z):
        step_pre += s["preall"][k].astype(f32)
    s["step"][...] = softplus(step_pre + s["par"][tap0 + taps + 2 : tap0 + taps + 3])
    state_in.wait()
    wide = 2 * LANES
    ways = s["gcs"].shape[1]
    piece = inner_dev // ways
    gall = s["gall"]

    def scan_block(b, _):
        at = pl.ds(pl.multiple_of(b * wide, LANES), wide)
        decay = -jnp.exp(s["par"][:states, at])
        step, act = s["step"][:, at], s["act"][:, at]
        for t in range(req):
            row = step[t : t + 1]
            now = jnp.exp(row * decay) * s["state"][t, :, at]
            now += (row * act[t : t + 1]) * s["bc"][:states, t : t + 1]
            s["state"][t, :, at] = now
            s["read"][t : t + 1, at] = jnp.sum(
                now * s["bc"][states : 2 * states, t : t + 1], axis=0, keepdims=True
            )
        read = s["read"][:, at] + s["par"][tap0 + taps + 1 : tap0 + taps + 2, at] * act
        gall[my, mc, mz, mx, :, at] = (read * silu(s["gate"][:, at])).astype(bf16)
        return 0

    def along_z(h):
        at = pl.ds(h * piece, piece)
        block = gall.at[my, mc, mz, mx, :, at]
        return [
            remote(
                block, block, s["gzs"].at[0, h, k], s["gzs"].at[1, h, k],
                red.peer_z(lax.rem(mz + k + 1, z)),
            )
            for k in range(z - 1)
        ]

    def along_xy(h):
        at = pl.ds(h * piece, piece)
        block = gall.at[my, mc, :, mx, :, at]
        out = []
        for k in range(1, x * y):
            dx, dy = k % x, k // x
            device = {
                "rep": mz * x + lax.rem(mx + dx, x),
                "tp": lax.rem(my + dy, y) * c + mc,
            }
            out.append(
                remote(block, block, s["gxs"].at[0, h, k - 1], s["gxs"].at[1, h, k - 1], device)
            )
        return out

    def along_core(h):
        block = gall.at[:, mc, :, :, :, pl.ds(h * piece, piece)]
        return remote(block, block, s["gcs"].at[0, h], s["gcs"].at[1, h], red.peer_c())

    blocks = piece // wide
    for h in range(ways):
        lax.fori_loop(h * blocks, (h + 1) * blocks, scan_block, 0)
        start_all(along_z(h))
    state_out = pltpu.make_async_copy(s["state"], state_out_ref, s["own"].at[3])
    state_out.start()
    for h in range(ways):
        for copy in along_z(h):
            copy.wait_recv()
        start_all(along_xy(h))
    for h in range(ways):
        for copy in along_xy(h):
            copy.wait_recv()
        along_core(h).start()
    out_in.wait()

    def product(core):
        total = jnp.zeros((rep_count * req, slice_dev), f32)
        for k in range(y):
            rows = gall.at[k, core].reshape(rep_count * req, inner_dev)[...]
            at = pl.multiple_of((k * c + core) * inner_dev, LANES)
            total += jnp.dot(rows, s["outw"][pl.ds(at, inner_dev)], preferred_element_type=f32)
        return total

    mixed = product(mc)
    for h in range(ways):
        along_core(h).wait_recv()
    residual = tok_all[...].astype(f32) + mixed + product(1 - mc)
    home_ref.reshape(count * tok_dev, slice_dev)[...] = residual.astype(bf16)
    gained = residual * gain[1:2]
    stat = lax.dot_general(
        gained, s["router"][...], (((1,), (1,)), ((), ())), preferred_element_type=f32,
        precision=lax.Precision.HIGHEST,
    )
    squares = jnp.sum(residual * residual, axis=1, keepdims=True)
    lane = column_iota(stat.shape, 1)
    stat = jnp.where(lane == router_ref.shape[0], squares, stat)
    stat_ref[...] = stat.reshape(rep_count, req, LANES)
    for e in range(experts):
        slots_ref[e] = lax.dot_general(
            s["maps"][e], gained.astype(bf16), (((0,), (0,)), ((), ())), preferred_element_type=f32
        ).astype(bf16)

    if tail:
        expert_part(
            expert_red, es, 0, experts_all, width, slots_ref, home_ref, stat_ref,
            idsall_ref.reshape(count * tok_dev, LANES), hid_ref, mamba_ref,
        )
    for copy in sel_copies + scale_copies + part_copies + pre_copies:
        copy.wait_send()

    def step_sent(k, _):
        @pl.when(jnp.logical_not(step_is_me(k)))
        def _():
            step_copy(k).wait_send()

        return 0

    lax.fori_loop(0, x * tp_count, step_sent, 0)

    def pack_sent(k, _):
        @pl.when(jnp.logical_not(is_me(k)))
        def _():
            pack_copy(k).wait_send()

        return 0

    lax.fori_loop(0, rep_count, pack_sent, 0)

    def act_sent(i, _):
        for copy in act_copies(i):
            copy.wait_send()
        return 0

    lax.fori_loop(0, red.chunks, act_sent, 0)
    for h in range(ways):
        for copy in along_z(h) + along_xy(h) + [along_core(h)]:
            copy.wait_send()
    scatter_wait(idsall_ref, s["idss"], 0, count)
    scatter_wait(tokall, s["toks"], 0, count)
    state_out.wait()


def mixer(args, expert_w, experts_all, rep_count, tp_count):
    tok, ids, gains, weight, skip, bias, decay, sel, history, router = args[:10]
    step_proj, w, state, out_w = args[10:]
    experts, hidden_dev = expert_w.shape[1], expert_w.shape[3] // tp_count
    f32, bf16 = jnp.float32, jnp.bfloat16
    count = rep_count * tp_count
    tok_dev = tok.shape[0]
    slice_dev = tok.shape[1] // count
    pieces = (count, tok_dev, slice_dev)
    packed_rows = weight.shape[0] + skip.shape[0] + 1 + decay.shape[0]
    packed = (packed_rows + -packed_rows % 16, decay.shape[1])
    req, states, inner_dev = state.shape
    red = Reduce(rep_count, tp_count, 2 * req, inner_dev, 0)
    n = red.chunks = red.per
    dma = pltpu.SemaphoreType.DMA
    vmem = pltpu.VMEM
    z, x, y, c = red.z, red.x, red.y, red.c
    tokens = count * tok_dev
    ways = CORES
    expert_rows = 2 * count * CAPACITY // rep_count
    expert_red = Reduce(rep_count, tp_count, expert_rows, hidden_dev, 0)
    expert_red.chunks = expert_red.per * experts
    expert_red.mix = 3 if expert_red.z % 2 == 0 and expert_red.z > 2 else 0
    held = sum(r.chunks * r.chunk_bytes() for r in (red, expert_red)) + 2 * (w.size + expert_w.size)
    fused = held <= ROOM
    scratch = red.scratch(2 * slice_dev)
    scratch.update(
        left=vmem((2 * tokens, 2 * slice_dev), bf16),
        scale=vmem((tok_dev, LANES), f32),
        scales=vmem((tp_count, tok_dev, LANES), f32),
        tok=vmem(pieces, bf16),
        ids=vmem((tok_dev, LANES), bf16),
        packed=vmem(packed, bf16),
        tokall=vmem(pieces, bf16),
        packall=vmem((rep_count,) + packed, bf16),
        par=vmem((packed[0], inner_dev), f32),
        stepz=vmem((LANES // step_proj.shape[0], step_proj.shape[0], inner_dev), bf16),
        sel=vmem((x,) + sel.shape, bf16),
        router=vmem((LANES, slice_dev), f32),
        maps=vmem((experts, tokens, count * CAPACITY), bf16),
        gate=vmem((req, inner_dev), f32),
        act=vmem((req, inner_dev), f32),
        actall=vmem((z, req, inner_dev), bf16),
        parts=vmem((tp_count, z * req, LANES), bf16),
        picks=vmem((z, req, LANES), f32),
        picked=vmem((z, req, LANES), f32),
        pre=vmem((z, req, inner_dev), bf16),
        preall=vmem((z, req, inner_dev), bf16),
        bc=vmem((LANES, LANES), f32),
        step=vmem((req, inner_dev), f32),
        read=vmem((req, inner_dev), f32),
        state=vmem(state.shape, f32),
        outw=vmem(out_w.shape, bf16),
        gall=vmem((y, c, z, x, req, inner_dev), bf16),
        toks=dma((2,)),
        idss=dma((2,)),
        pts=dma((2, tp_count - 1)),
        mzs=dma((2, z - 1)),
        pzs=dma((2, z - 1)),
        scs=dma((2, tp_count - 1)),
        sts=dma((2, max(x * tp_count, x * sel.shape[0] // step_proj.shape[0]))),
        sxs=dma((2, x - 1)),
        pks=dma((2, rep_count)),
        own=dma((4,)),
        acs=dma((2, n, z - 1)),
        gzs=dma((2, ways, z - 1)),
        gxs=dma((2, ways, x * y - 1)),
        gcs=dma((2, ways)),
    )
    shape = jax.ShapeDtypeStruct
    anywhere = pl.BlockSpec(memory_space=pl.ANY)
    home, stat = pieces, (rep_count, req, LANES)
    slots = (experts, count * CAPACITY, slice_dev)
    idsall = (count, tok_dev, LANES)
    outs = [shape(history.shape, bf16), shape(state.shape, f32)]
    tail, names = None, tuple(scratch)
    if fused:
        scratch["home"] = vmem(home, bf16)
        scratch["stat"] = vmem(stat, f32)
        scratch["slots"] = vmem(slots, bf16)
        scratch["idsall"] = vmem(idsall, bf16)
        names = tuple(scratch)
        more = expert_scratch(expert_red, 2 * slice_dev, experts, stat, home)
        tail = (expert_red, tuple(more), experts_all)
        outs += [
            shape((experts, expert_rows // 2, hidden_dev), bf16), shape(tok.shape, bf16)
        ]
        args = args + (expert_w,)
        spaces = list(scratch.values()) + list(more.values())
    else:
        outs += [shape(home, bf16), shape(stat, f32), shape(slots, bf16), shape(idsall, bf16)]
        spaces = list(scratch.values())
    got = pl.pallas_call(
        functools.partial(mixer_kernel, red, names, experts, tail),
        out_shape=outs,
        in_specs=in_vmem(10) + [anywhere] * (len(args) - 10),
        out_specs=in_vmem(1) + [anywhere] + in_vmem(len(outs) - 2),
        scratch_shapes=spaces,
        compiler_params=pltpu.CompilerParams(
            collective_id=0, has_side_effects=True, vmem_limit_bytes=62 * 2**20
        ),
        name="mixer",
    )(*args)
    if fused:
        return got
    home, stat, slots, idsall = got[2:]
    hidden, mamba = last_stage(
        slots, home, stat, idsall.reshape(tokens, LANES), expert_w, experts_all,
        tok.shape[1], rep_count, tp_count, hidden_dev,
    )
    return got[0], got[1], hidden, mamba


def expert_fetch(red, s, begin, w_ref):
    for i in range(red.chunks):
        expert, column = divmod(begin + i, red.per)
        red.fetch(
            s, w_ref, i, column * 2 * red.half,
            lambda w, at, expert=expert: w.at[:, expert, :, at],
        )


def last_kernel(
    red, names, begin, extra, experts_all, width, x_ref, home_ref, stat_ref, ids_ref, w_ref, hid_ref, *refs
):
    outs = 1 if extra else 0
    s = dict(zip(names, refs[outs:]))
    red.place()
    expert_fetch(red, s, begin, w_ref)
    count = red.z * red.x * red.y * red.c
    greet_all(count, red.rep * red.y * red.c + red.tp, red.y * red.c)
    mamba_ref = refs[0] if extra else None
    expert_part(
        red, s, begin, experts_all, width, x_ref, home_ref, stat_ref, ids_ref, hid_ref, mamba_ref
    )


def expert_part(
    red, s, begin, experts_all, width, x_ref, home_ref, stat_ref, ids_ref, hid_ref, mamba_ref
):
    extra = mamba_ref is not None
    tp_count, rep_count = red.y * red.c, red.z * red.x
    count = tp_count * rep_count
    rep, tp = red.rep, red.tp
    me = rep * tp_count + tp
    wide = 2 * red.half
    homes_ref = s["homes"] if extra else None
    for expert in range(x_ref.shape[0]):
        s["left"][expert] = spread(x_ref[expert], red.rows // 2, 2)

    def left_of(i):
        return s["left"][lax.div(begin + i, red.per)]

    req = red.rows // 2
    tok_dev = home_ref.shape[1]
    experts = x_ref.shape[0]

    def hop_copies(hop):
        axis, count_on, mine = ("rep", rep_count, rep) if hop == 0 else ("tp", tp_count, tp)
        out = []
        for k in range(count_on - 1):
            to = lax.rem(mine + k + 1, count_on)
            source = stat_ref.at[to] if hop == 0 else s["own"].at[0]
            target = s["stats" if hop == 0 else "stats_tp"].at[mine]
            sems = s["sas" if hop == 0 else "sbs"]
            out.append(remote(source, target, sems.at[0, k], sems.at[1, k], {axis: to}))
        return out

    def send_stats():
        start_all(hop_copies(0))
        s["stats"][rep] = stat_ref[rep]

    def pass_stats():
        for copy in hop_copies(0):
            copy.wait()
        summed = s["stats"][0]
        for k in range(1, rep_count):
            summed += s["stats"][k]
        s["own"][0] = summed
        s["stats_tp"][tp] = summed
        start_all(hop_copies(1))

    def gates():
        for copy in hop_copies(1):
            copy.wait()
        summed = s["stats_tp"][0]
        for k in range(1, tp_count):
            summed += s["stats_tp"][k]
        tokens = tp_count * tok_dev
        ids = ids_ref[pl.ds(pl.multiple_of(rep * tokens, 8), tokens)]
        lane = lax.broadcasted_iota(jnp.int32, (tokens, LANES), 1)
        first, second = named(ids, lane)
        scale = lax.rsqrt(summed[:, experts_all : experts_all + 1] / width + epsilon)
        logits = summed * scale
        one = jnp.sum(jnp.where(first, logits, 0.0), axis=1, keepdims=True)
        two = jnp.sum(jnp.where(second, logits, 0.0), axis=1, keepdims=True)
        gate = jnp.where(first, 1.0 / (1.0 + jnp.exp(two - one)), 0.0)
        gate += jnp.where(second, 1.0 / (1.0 + jnp.exp(one - two)), 0.0)
        gate = jnp.where(lane == LANES - 1, scale, gate)
        for e, taken in enumerate(slot_maps(ids, experts, tok_dev)):
            row = lax.dot_general(
                taken, gate, (((0,), (0,)), ((), ())), preferred_element_type=jnp.float32,
                precision=lax.Precision.HIGHEST,
            )
            seat = row[:, e : e + 1].astype(jnp.bfloat16).astype(jnp.float32)
            s["seat"][e] = jnp.broadcast_to(seat, s["seat"].shape[1:])
            s["size"][e] = jnp.broadcast_to(row[:, LANES - 1 :], s["size"].shape[1:])

    def store(i, h, total):
        expert = lax.div(begin + i, red.per)
        column = lax.rem(begin + i, red.per) * wide + h * red.half
        size = s["size"][expert][:, :1]
        up = total[req:] * size
        hidden = s["seat"][expert][:, :1] * silu(total[:req] * size) * up
        at = pl.ds(pl.multiple_of(column, LANES), red.half)
        hid_ref[expert, :, at] = hidden.astype(jnp.bfloat16)

    def send_home():
        scatter_start(home_ref, homes_ref, s["hos"], count, me, tp_count)
        homes_ref[me] = home_ref[me]

    lags = (2, 5, 8, 11)
    extras = [(0, send_stats), (4, pass_stats), (lags[3] - 1, gates)]
    if extra:
        extras.append((2, send_home))
    red.run(s, left_of, store, lags, extras)
    if extra:
        for which in range(2):
            scatter_wait(homes_ref, s["hos"], which, count)
        slice_dev = homes_ref.shape[2]
        for k in range(count):
            mamba_ref[:, k * slice_dev : (k + 1) * slice_dev] = homes_ref[k]


def expert_scratch(red, depth, experts, stat, home):
    bf16, f32 = jnp.bfloat16, jnp.float32
    dma = pltpu.SemaphoreType.DMA
    rep_count, tp_count = red.z * red.x, red.y * red.c
    scratch = red.scratch(depth)
    scratch["left"] = pltpu.VMEM((experts, rep_count * red.rows, depth), bf16)
    scratch["sas"] = dma((2, rep_count - 1))
    scratch["sbs"] = dma((2, tp_count - 1))
    scratch["stats"] = pltpu.VMEM((rep_count,) + stat[1:], f32)
    scratch["stats_tp"] = pltpu.VMEM((tp_count,) + stat[1:], f32)
    scratch["own"] = pltpu.VMEM((1,) + stat[1:], f32)
    scratch["seat"] = pltpu.VMEM((experts, red.rows // 2, LANES), f32)
    scratch["size"] = pltpu.VMEM((experts, red.rows // 2, LANES), f32)
    if home is not None:
        scratch["hos"] = dma((2,))
        scratch["homes"] = pltpu.VMEM(home, bf16)
    return scratch


def last_stage(slots, home, stat, ids, w, experts_all, width, rep_count, tp_count, hidden_dev):
    bf16 = jnp.bfloat16
    experts, total_rows, slice_dev = slots.shape
    rows = 2 * total_rows // rep_count
    shape = jax.ShapeDtypeStruct
    full = Reduce(rep_count, tp_count, rows, hidden_dev, 0)
    total = full.per * experts
    most = max(1, ROOM // (full.chunk_bytes() + 2 * w.size // total))
    begin, ups = 0, None
    while begin < total:
        red = Reduce(rep_count, tp_count, rows, hidden_dev, min(most, total - begin))
        extra = begin == 0
        scratch = expert_scratch(
            red, 2 * slice_dev, experts, stat.shape, home.shape if extra else None
        )
        outs = [shape((experts, rows // 2, hidden_dev), bf16)]
        if extra:
            outs += [shape((home.shape[1], width), bf16)]
        got = pl.pallas_call(
            functools.partial(last_kernel, red, tuple(scratch), begin, extra, experts_all, width),
            out_shape=outs,
            in_specs=in_vmem(4) + [pl.BlockSpec(memory_space=pl.ANY)],
            out_specs=in_vmem(len(outs)),
            scratch_shapes=list(scratch.values()),
            compiler_params=pltpu.CompilerParams(
                collective_id=10 + begin, has_side_effects=True, vmem_limit_bytes=62 * 2**20
            ),
            name="last_stage",
        )(slots, home, stat, ids, w)
        if extra:
            ups, homes = got
        else:
            edge = begin // full.per
            column = (begin % full.per) * 2 * full.half
            at = lax.broadcasted_iota(jnp.int32, (experts, 1, hidden_dev), 2)
            order = lax.broadcasted_iota(jnp.int32, (experts, 1, hidden_dev), 0)
            older = (order < edge) | ((order == edge) & (at < column))
            ups = jnp.where(older, ups, got[0])
        begin += red.chunks
    return ups, homes


def finish_kernel(experts, *refs):
    sources, targets, held = refs[:4], refs[4:8], refs[8:12]
    moved, sems, state_sems = refs[12:]
    parts = state_sems.shape[1]
    size = sources[3].shape[0] // parts

    def load(k):
        return pltpu.make_async_copy(sources[k], held[k], sems.at[0, k])

    def save(k):
        return pltpu.make_async_copy(moved if k == 2 else held[k], targets[k], sems.at[1, k])

    def state(k, way):
        at = pl.ds(k * size, size)
        if way == 0:
            return pltpu.make_async_copy(sources[3].at[at], held[3].at[at], state_sems.at[0, k])
        return pltpu.make_async_copy(held[3].at[at], targets[3].at[at], state_sems.at[1, k])

    for k in range(parts):
        state(k, 0).start()
    for k in range(3):
        load(k).start()
    rows = moved.shape[0]
    to, source = column_iota((rows, rows), 0), column_iota((rows, rows), 1)
    block, seat = lax.div(to, experts * CAPACITY), lax.rem(to, CAPACITY)
    expert = lax.rem(lax.div(to, CAPACITY), experts)
    moves = source == expert * (rows // experts) + block * CAPACITY + seat
    for k in range(parts):
        state(k, 0).wait()
        state(k, 1).start()
    for k in range(2):
        load(k).wait()
        save(k).start()
    load(2).wait()
    moved[...] = jnp.dot(
        moves.astype(jnp.bfloat16), held[2][...], preferred_element_type=jnp.float32
    ).astype(jnp.bfloat16)
    save(2).start()
    for k in range(3):
        save(k).wait()
    for k in range(parts):
        state(k, 1).wait()


def finish(conv_next, mamba, hidden, state, experts):
    anywhere = pl.BlockSpec(memory_space=pl.ANY)
    arrays = (conv_next, mamba, hidden, state)
    dma = pltpu.SemaphoreType.DMA
    return pl.pallas_call(
        functools.partial(finish_kernel, experts),
        out_shape=[jax.ShapeDtypeStruct(array.shape, array.dtype) for array in arrays],
        in_specs=[anywhere] * 4,
        out_specs=[anywhere] * 4,
        scratch_shapes=[pltpu.VMEM(array.shape, array.dtype) for array in arrays]
        + [pltpu.VMEM(hidden.shape, hidden.dtype), dma((2, 3)), dma((2, 4))],
        name="finish",
    )(*arrays)


def shards(
    tokens,
    conv_state,
    ssm_state,
    norm_gains,
    conv_weight,
    conv_skip,
    step_bias,
    decay_log,
    input_proj,
    select_proj,
    step_proj,
    output_proj,
    router,
    expert_proj,
    expert_ids,
):
    tp_count = lax.axis_size("tp")
    rep_count = lax.axis_size("rep")
    args = (
        tokens, expert_ids, norm_gains, conv_weight, conv_skip, step_bias, decay_log,
        select_proj.T, conv_state, router.T, step_proj, input_proj, ssm_state, output_proj,
    )
    conv_next, ssm_next, hidden, mamba = mixer(
        args, expert_proj, router.shape[1], rep_count, tp_count
    )
    hidden = hidden.reshape(-1, hidden.shape[2])
    conv_next, mamba_out, expert_hidden, ssm_next = finish(
        conv_next, mamba, hidden, ssm_next, expert_proj.shape[1]
    )
    return (mamba_out, conv_next, ssm_next, expert_hidden)


def solution(mesh):
    in_specs = (
        P(("rep", "tp"), None),
        P(None, "rep", "tp"),
        P("rep", None, "tp"),
        P(None, ("rep", "tp")),
        P(None, ("rep", "tp")),
        P(None, ("rep", "tp")),
        P(("rep", "tp")),
        P(None, ("rep", "tp")),
        P(("rep", "tp"), None, None),
        P("tp", "rep"),
        P(("rep", "tp"), None),
        P(None, ("rep", "tp")),
        P(("rep", "tp"), None),
        P(("rep", "tp"), None, None, None),
        P(("rep", "tp"), None),
    )
    out_specs = (P(("rep", "tp"), None), P(None, "rep", "tp"), P("rep", None, "tp"), P("rep", "tp"))
    return jax.shard_map(shards, mesh=mesh, in_specs=in_specs, out_specs=out_specs, check_vma=False)
```
